32 devices in a mesh: seq: 8 (over z, y), tp: 4 (over x, core).
Axes of the slice: x: 2, y: 2, z: 4, core: 2. Of those that a mesh axis runs over, the one named last changes fastest.
Arguments:
- encoded: bfloat16 [8192, 1280], P(('seq', 'tp')), may hold values from -6 to 6
- starts: int32 [32, 32], replicated, may hold values from 0 to 256, as said below
- w_up: bfloat16 [1280, 4096], P(None, 'tp'), may hold values from -0.15625 to 0.15625
- norm_gain: float32 [4096], replicated, may hold values from 0.25 to 1.75
- w_query: bfloat16 [4096, 4096], P(None, 'tp'), may hold values from -8 to 8
- w_key: bfloat16 [4096, 4096], P(None, 'tp'), may hold values from -8 to 8
- w_value: bfloat16 [4096, 4096], P(None, 'tp'), may hold values from -0.09375 to 0.09375
- w_out: bfloat16 [4096, 4096], P('tp'), may hold values from -0.09375 to 0.09375
- cotangent: bfloat16 [1024, 4096], P('seq', 'tp'), may hold values from -6 to 6
Outputs:
- latent_out: bfloat16 [1024, 4096], P('seq', 'tp')
- latent_grad: float32 [1024, 4096], P('seq', 'tp')
The draws below stay inside these ranges and needn't reach their ends.
Inputs may be any that keep to these rules, and one draw needn't show every extreme that they name: `starts`: row i lists in increasing order the distinct offsets at which patches begin in byte shard i, followed by 256 in unused slots; every shard has at least one patch and at least 8, some shard exactly 32; shard 0 begins a patch at offset 0.
All inputs are finite; a program needn't handle non-finite values.
Results may differ from the reference program's by a relative error of at most 0.014.
Values may be sent and summed in bfloat16 or wider, within the bound.
A program may use at most 128 MiB of HBM per device.

```python
import jax
import jax.numpy as jnp
from jax import lax

E = 1280
D = 4096
HEADS = 32
HEAD_DIM = 128
B_DEV = 256
PATCH_CAP = 32
SHARDS = 32
PATCHES = 1024
BYTES = 8192


def shard_order(key):
    return jax.random.permutation(key, B_DEV)


def draw_starts(key, part):
    count_key, pick_key, full_key = jax.random.split(jax.random.fold_in(key, 3), 3)
    counts = jax.random.randint(count_key, (SHARDS,), max(PATCH_CAP // 4, 1), PATCH_CAP + 1)
    fullest = jax.random.randint(full_key, (), 0, SHARDS)
    counts = jnp.where(jnp.arange(SHARDS) == fullest, PATCH_CAP, counts)
    orders = jax.vmap(shard_order)(jax.random.split(pick_key, SHARDS))
    places = jnp.arange(B_DEV, dtype=jnp.int32)[None, :]
    chosen = jnp.where(orders < counts[:, None], places, B_DEV)
    ordered = jnp.sort(chosen, axis=1)[:, :PATCH_CAP]
    ordered = ordered.at[0, 0].set(0)
    return ordered.astype(jnp.int32)


def query_key_pair(key):
    first, second = jax.random.split(jax.random.fold_in(key, 17))
    query = jnp.clip(jax.random.normal(first, (D, D), jnp.float32), -5.0, 5.0) * D ** (-0.5)
    other = jnp.clip(jax.random.normal(second, (D, D), jnp.float32), -5.0, 5.0) * D ** (-0.5)
    keys = other
    return (query, keys)


def draw_w_query(key, part):
    return query_key_pair(key)[0].astype(jnp.bfloat16)


def draw_w_key(key, part):
    return query_key_pair(key)[1].astype(jnp.bfloat16)


def shard_levels(key, dims, cuts, least, high):
    def one(dim, parts):
        draws = jax.random.uniform(jax.random.fold_in(jax.random.fold_in(key, 6), dim), (parts,), jnp.float32, least / len(cuts), high / len(cuts))
        return jnp.repeat(jnp.exp(draws), dims[dim] // parts).reshape((-1,) + (1,) * (len(dims) - dim - 1))

    loudness = one(*cuts[0])
    for cut in cuts[1:]:
        loudness = loudness * one(*cut)
    return loudness


def bell_draw(rng, shape, spread, limit, cuts=(), kind=jnp.bfloat16):
    loudness = shard_levels(rng, shape, cuts, -0.22, 0.18) if cuts else 1.0
    drawn = jax.random.normal(rng, shape, jnp.float32) * spread * loudness
    return jnp.minimum(jnp.maximum(drawn, -limit), limit).astype(kind)


def setup_inputs(seed: int = 0) -> dict:
    key_list = jax.random.split(jax.random.key(seed), 10)
    encoded = bell_draw(key_list[0], (BYTES, E), 1.0, 6.0, ((0, 32),))
    starts = draw_starts(jax.random.fold_in(key_list[9], 71), 0)
    w_up = bell_draw(key_list[2], (E, D), E ** -0.5, 0.15625, ((1, 4),))
    norm_gain = jnp.clip(1.0 + 0.15 * jax.random.normal(key_list[3], (D,), jnp.float32), 0.25, 1.75)
    w_query = draw_w_query(jax.random.fold_in(key_list[9], 71), 0)
    w_key = draw_w_key(jax.random.fold_in(key_list[9], 71), 0)
    w_value = bell_draw(key_list[6], (D, D), D ** -0.5, 0.09375, ((1, 4),))
    w_out = bell_draw(key_list[7], (D, D), D ** -0.5, 0.09375, ((0, 4),))
    cotangent = bell_draw(key_list[8], (PATCHES, D), 1.0, 6.0, ((0, 8), (1, 4)))
    return {"encoded": encoded, "starts": starts, "w_up": w_up, "norm_gain": norm_gain, "w_query": w_query, "w_key": w_key, "w_value": w_value, "w_out": w_out, "cotangent": cotangent}


EPS = 1e-05
NEG = -1e+30
CONTRACT_LAST = (((1,), (1,)), ((), ()))

def pooled_patches(encoded, starts):
    shards = starts.shape[0]
    byte_blocks = encoded.reshape(shards, B_DEV, E).astype(jnp.float32)
    places = jnp.arange(B_DEV, dtype=jnp.int32)
    following = jnp.concatenate([starts[:, 1:], jnp.full((shards, 1), B_DEV, jnp.int32)], 1)
    member = ((places[None, None, :] >= starts[:, :, None]) & (places[None, None, :] < following[:, :, None])).astype(jnp.float32)
    sums = jnp.einsum('spb,sbe->spe', member, byte_blocks)
    sizes = lax.optimization_barrier(jnp.sum(member, 2))
    leading = (places[None, :] < starts[:, :1]).astype(jnp.float32)
    lead_sums = jnp.einsum('sb,sbe->se', leading, byte_blocks)
    lead_sizes = lax.optimization_barrier(jnp.sum(leading, 1))
    next_sums = jnp.concatenate([lead_sums[1:], jnp.zeros((1, E), jnp.float32)], 0)
    next_sizes = jnp.concatenate([lead_sizes[1:], jnp.zeros((1,), jnp.float32)], 0)
    counts = lax.optimization_barrier(jnp.sum((starts < B_DEV).astype(jnp.int32), 1))
    last_slot = (jnp.arange(PATCH_CAP, dtype=jnp.int32)[None, :] == (counts - 1)[:, None]).astype(jnp.float32)
    sums = sums + last_slot[:, :, None] * next_sums[:, None, :]
    sizes = sizes + last_slot * next_sizes[:, None]
    patches = sums / jnp.maximum(sizes, 1.0)[:, :, None]
    return patches.reshape(PATCHES, E).astype(jnp.bfloat16)

def split_heads(matrix):
    return matrix.reshape(PATCHES, HEADS, HEAD_DIM).transpose(1, 0, 2)

def join_heads(stacked):
    return stacked.transpose(1, 0, 2).reshape(PATCHES, D)

def reference(encoded, starts, w_up, norm_gain, w_query, w_key, w_value, w_out, cotangent):
    patches = pooled_patches(encoded, starts)
    valid = (starts < B_DEV).reshape(PATCHES)
    latent_in = jnp.dot(patches, w_up, preferred_element_type=jnp.float32).astype(jnp.bfloat16)
    wide = latent_in.astype(jnp.float32)
    rinv = lax.rsqrt(lax.optimization_barrier(jnp.sum(wide * wide, 1)) / D + EPS)
    scaled = (wide * norm_gain[None, :]).astype(jnp.bfloat16)
    query = (rinv[:, None] * jnp.dot(scaled, w_query, preferred_element_type=jnp.float32)).astype(jnp.bfloat16)
    keys = (rinv[:, None] * jnp.dot(scaled, w_key, preferred_element_type=jnp.float32)).astype(jnp.bfloat16)
    values = (rinv[:, None] * jnp.dot(scaled, w_value, preferred_element_type=jnp.float32)).astype(jnp.bfloat16)
    index = jnp.arange(PATCHES, dtype=jnp.int32)
    allowed = valid[None, :] & (index[None, :] <= index[:, None])
    scale = HEAD_DIM ** (-0.5)

    def head_forward(operands):
        head_query, head_key, head_value = operands
        scores = jnp.dot(head_query, head_key.T, preferred_element_type=jnp.float32) * scale
        peak = lax.optimization_barrier(jnp.max(jnp.where(allowed, scores, NEG), 1))
        expo = jnp.where(allowed, jnp.exp(scores - peak[:, None]), 0.0)
        total = lax.optimization_barrier(jnp.sum(expo, 1))
        mixed = jnp.dot(expo.astype(jnp.bfloat16), head_value, preferred_element_type=jnp.float32)
        return ((mixed / total[:, None]).astype(jnp.bfloat16), peak, total)
    heads_query = split_heads(query)
    heads_key = split_heads(keys)
    heads_value = split_heads(values)
    heads_attn, peaks, totals = lax.map(head_forward, (heads_query, heads_key, heads_value))
    attn = join_heads(heads_attn)
    result = wide + jnp.dot(attn, w_out, preferred_element_type=jnp.float32)
    latent_out = jnp.where(valid[:, None], result, 0.0).astype(jnp.bfloat16)
    grad_out = jnp.where(valid[:, None], cotangent, jnp.zeros_like(cotangent))
    d_attn = lax.dot_general(grad_out, w_out, CONTRACT_LAST, preferred_element_type=jnp.float32).astype(jnp.bfloat16)

    def head_backward(operands):
        head_query, head_key, head_value, head_out, head_grad, peak, total = operands
        scores = jnp.dot(head_query, head_key.T, preferred_element_type=jnp.float32) * scale
        probs = jnp.where(allowed, jnp.exp(scores - peak[:, None]), 0.0) / total[:, None]
        delta = lax.optimization_barrier(jnp.sum(head_grad.astype(jnp.float32) * head_out.astype(jnp.float32), 1))
        d_probs = jnp.dot(head_grad, head_value.T, preferred_element_type=jnp.float32)
        d_scores = (probs * (d_probs - delta[:, None])).astype(jnp.bfloat16)
        grad_query = (jnp.dot(d_scores, head_key, preferred_element_type=jnp.float32) * scale).astype(jnp.bfloat16)
        grad_key = (jnp.dot(d_scores.T, head_query, preferred_element_type=jnp.float32) * scale).astype(jnp.bfloat16)
        grad_value = jnp.dot(probs.astype(jnp.bfloat16).T, head_grad, preferred_element_type=jnp.float32).astype(jnp.bfloat16)
        return (grad_query, grad_key, grad_value)
    grads_query, grads_key, grads_value = lax.map(head_backward, (heads_query, heads_key, heads_value, heads_attn, split_heads(d_attn), peaks, totals))
    dnormed = lax.dot_general(join_heads(grads_query), w_query, CONTRACT_LAST, preferred_element_type=jnp.float32) + lax.dot_general(join_heads(grads_key), w_key, CONTRACT_LAST, preferred_element_type=jnp.float32) + lax.dot_general(join_heads(grads_value), w_value, CONTRACT_LAST, preferred_element_type=jnp.float32)
    dots = lax.optimization_barrier(jnp.sum(norm_gain[None, :] * dnormed * wide, 1))
    latent_grad = grad_out.astype(jnp.float32) + rinv[:, None] * norm_gain[None, :] * dnormed - wide * (rinv ** 3)[:, None] * dots[:, None] / D
    return (latent_out, latent_grad)
```

```python
import functools

import jax
import jax.numpy as jnp
from jax import lax
from jax.experimental import pallas as pl
from jax.experimental.pallas import tpu as pltpu
from jax.sharding import PartitionSpec as P

HEAD_DIM = 128


EPS = 1e-05
NEG = -1e30
CONTRACT_LAST = (((1,), (1,)), ((), ()))


def shifted(block, axis, distance):
    devices = range(lax.axis_size(axis))
    route = [(i - distance, i) for i in devices if i - distance in devices]
    return lax.ppermute(block, axis, route)


def per_device(encoded, starts, w_up, norm_gain, w_query, w_key, w_value, w_out, cotangent):
    byte_rows = encoded.shape[0]
    patch_cap = starts.shape[1]
    model_width = norm_gain.shape[0]
    shard = lax.axis_index(("seq", "tp"))
    own_starts = lax.dynamic_slice_in_dim(starts, shard, 1, 0)[0]
    places = jnp.arange(byte_rows, dtype=jnp.int32)
    following = jnp.concatenate([own_starts[1:], jnp.full((1,), byte_rows, jnp.int32)])
    inside = (places[None, :] >= own_starts[:, None]) & (places[None, :] < following[:, None])
    sums = jnp.dot(inside.astype(jnp.bfloat16), encoded, preferred_element_type=jnp.float32)
    sizes = jnp.sum(inside.astype(jnp.float32), 1)
    leading = places[None, :] < own_starts[:1, None]
    lead_sum = jnp.dot(leading.astype(jnp.bfloat16), encoded, preferred_element_type=jnp.float32)
    lead_size = jnp.sum(leading.astype(jnp.float32), 1)
    next_sum, next_size = shifted((lead_sum, lead_size), ("seq", "tp"), -1)
    count = jnp.sum((own_starts < byte_rows).astype(jnp.int32))
    last_slot = (jnp.arange(patch_cap, dtype=jnp.int32) == count - 1).astype(jnp.float32)
    sums = sums + last_slot[:, None] * next_sum
    sizes = sizes + last_slot * next_size
    patches = (sums / jnp.maximum(sizes, 1.0)[:, None]).astype(jnp.bfloat16)
    group = lax.all_gather(patches, "tp", axis=0, tiled=True)
    latent_in = jnp.dot(group, w_up, preferred_element_type=jnp.float32).astype(jnp.bfloat16)
    group_rows, columns = latent_in.shape
    head_count = columns // HEAD_DIM
    wide_piece = lax.all_gather(latent_in, "tp", axis=1, tiled=True).astype(jnp.float32)
    scaled = (wide_piece * norm_gain[None, :]).astype(jnp.bfloat16)
    acc_query = jnp.dot(scaled, w_query, preferred_element_type=jnp.float32)
    acc_key = jnp.dot(scaled, w_key, preferred_element_type=jnp.float32)
    acc_value = jnp.dot(scaled, w_value, preferred_element_type=jnp.float32)
    acc_query, acc_key, acc_value, square = (
        acc_query,
        acc_key,
        acc_value,
        jnp.sum(wide_piece * wide_piece, 1),
    )
    rinv = lax.rsqrt(square / model_width + EPS)
    query = (rinv[:, None] * acc_query).astype(jnp.bfloat16)
    key_rows = (rinv[:, None] * acc_key).astype(jnp.bfloat16)
    value_rows = (rinv[:, None] * acc_value).astype(jnp.bfloat16)
    keys_all, values_all = (
        lax.all_gather(key_rows, "seq", axis=0, tiled=True),
        lax.all_gather(value_rows, "seq", axis=0, tiled=True),
    )
    patches_total = keys_all.shape[0]
    valid_all = (starts < byte_rows).reshape(patches_total)
    row_base = lax.axis_index("seq") * group_rows
    query_index = row_base + jnp.arange(group_rows, dtype=jnp.int32)
    key_index = jnp.arange(patches_total, dtype=jnp.int32)
    query_valid = lax.dynamic_slice_in_dim(valid_all, row_base, group_rows, 0)
    allowed = valid_all[None, :] & (key_index[None, :] <= query_index[:, None])
    scale = HEAD_DIM ** (-0.5)
    query_heads = query.reshape(group_rows, head_count, HEAD_DIM)
    key_heads = keys_all.reshape(patches_total, head_count, HEAD_DIM)
    value_heads = values_all.reshape(patches_total, head_count, HEAD_DIM)
    scores = (
        jnp.einsum("rhd,khd->hrk", query_heads, key_heads, preferred_element_type=jnp.float32)
        * scale
    )
    peak = jnp.max(jnp.where(allowed[None], scores, NEG), 2)
    expo = jnp.where(allowed[None], jnp.exp(scores - peak[:, :, None]), 0.0)
    total = jnp.sum(expo, 2)
    mixed = jnp.einsum(
        "hrk,khd->rhd", expo.astype(jnp.bfloat16), value_heads, preferred_element_type=jnp.float32
    )
    attn = (mixed / total.T[:, :, None]).astype(jnp.bfloat16)
    partial_value = jnp.dot(
        attn.reshape(group_rows, columns), w_out, preferred_element_type=jnp.float32
    )
    head_sum = lax.psum_scatter(
        partial_value.astype(jnp.bfloat16), "tp", scatter_dimension=1, tiled=True
    ).astype(jnp.float32)
    wide_in = latent_in.astype(jnp.float32)
    latent_out = jnp.where(query_valid[:, None], wide_in + head_sum, 0.0).astype(jnp.bfloat16)
    grad_out = jnp.where(query_valid[:, None], cotangent, jnp.zeros_like(cotangent))
    d_attn = lax.dot_general(
        lax.all_gather(grad_out, "tp", axis=1, tiled=True),
        w_out,
        CONTRACT_LAST,
        preferred_element_type=jnp.float32,
    ).astype(jnp.bfloat16)
    grad_heads = d_attn.reshape(group_rows, head_count, HEAD_DIM)
    delta = jnp.sum(grad_heads.astype(jnp.float32) * attn.astype(jnp.float32), 2).T
    probs = expo / total[:, :, None]
    d_probs = jnp.einsum(
        "rhd,khd->hrk", grad_heads, value_heads, preferred_element_type=jnp.float32
    )
    d_scores = (probs * (d_probs - delta[:, :, None])).astype(jnp.bfloat16)
    grad_query = (
        (
            jnp.einsum("hrk,khd->rhd", d_scores, key_heads, preferred_element_type=jnp.float32)
            * scale
        )
        .astype(jnp.bfloat16)
        .reshape(group_rows, columns)
    )
    weights_low = probs.astype(jnp.bfloat16)
    count_rows = group_rows * lax.axis_size("seq")
    key_part = jnp.einsum("hrk,rhd->khd", d_scores, query_heads, preferred_element_type=jnp.float32)
    value_part = jnp.einsum(
        "hrk,rhd->khd", weights_low, grad_heads, preferred_element_type=jnp.float32
    )
    both = lax.psum_scatter(
        jnp.concatenate(
            [key_part.reshape(count_rows, columns), value_part.reshape(count_rows, columns)], 1
        ).astype(jnp.bfloat16),
        "seq",
        scatter_dimension=0,
        tiled=True,
    ).astype(jnp.float32)
    grad_key = (both[:, :columns] * scale).astype(jnp.bfloat16)
    grad_value = both[:, columns:].astype(jnp.bfloat16)
    dnormed = (
        lax.dot_general(grad_query, w_query, CONTRACT_LAST, preferred_element_type=jnp.float32)
        + lax.dot_general(grad_key, w_key, CONTRACT_LAST, preferred_element_type=jnp.float32)
        + lax.dot_general(grad_value, w_value, CONTRACT_LAST, preferred_element_type=jnp.float32)
    )
    normed_grad = lax.psum_scatter(
        dnormed.astype(jnp.bfloat16), "tp", scatter_dimension=1, tiled=True
    ).astype(jnp.float32)
    gain_own = lax.dynamic_slice_in_dim(norm_gain, lax.axis_index("tp") * columns, columns, 0)
    dots = lax.psum(jnp.sum(gain_own[None, :] * normed_grad * wide_in, 1), "tp")
    latent_grad = (
        grad_out.astype(jnp.float32)
        + rinv[:, None] * gain_own[None, :] * normed_grad
        - wide_in * (rinv**3)[:, None] * dots[:, None] / model_width
    )
    return (latent_out, latent_grad)


MESH = pl.DeviceIdType.MESH
LOW = jnp.bfloat16
WIDE = jnp.float32
ROWS_FIRST = (((0,), (0,)), ((), ()))


def tile_of(index, size):
    return pl.ds(pl.multiple_of(index * size, size), size)


def dot(a, b):
    return jnp.dot(a, b, preferred_element_type=WIDE)


def dot_last(a, b):
    return lax.dot_general(a, b, CONTRACT_LAST, preferred_element_type=WIDE)


def to_row(column):
    n = column.shape[0]
    down = lax.broadcasted_iota(jnp.int32, (n, n), 0)
    across = lax.broadcasted_iota(jnp.int32, (n, n), 1)
    return jnp.sum(jnp.where(down == across, column, 0.0), 0, keepdims=True)


def to_column(row, shift=0):
    n = row.shape[1]
    down = lax.broadcasted_iota(jnp.int32, (n, n), 0)
    across = lax.broadcasted_iota(jnp.int32, (n, n), 1)
    return jnp.sum(jnp.where(down + shift == across, row, 0.0), 1, keepdims=True)


def layer_kernel(
    seq_size,
    tp_size,
    encoded,
    starts,
    gain,
    cotangent,
    w_up_far,
    w_query_far,
    w_key_far,
    w_value_far,
    w_out_far,
    out_value,
    out_grad,
    w_up,
    w_query,
    w_key,
    w_value,
    w_out,
    lead_out,
    lead_in,
    group,
    wide,
    wide_grad,
    scaled,
    valid_column,
    rinv_column,
    outbox,
    heads,
    value_turned,
    key_turned,
    scores,
    d_probs,
    key_sum,
    value_sum,
    returns,
    back,
    grad_sum,
    partial,
    pair_in,
    cross_out,
    cross_in,
    dots_out,
    dots_in,
    weight_sem,
    lead_sem,
    gather_send,
    gather_recv,
    out_send,
    out_recv,
    back_send,
    back_recv,
    pair_send,
    pair_recv,
    cross_send,
    cross_recv,
    dots_send,
    dots_recv,
):
    byte_rows, byte_width = encoded.shape
    shards, cap = starts.shape
    rows, columns = cotangent.shape
    model_width = gain.shape[1]
    patches_total = shards * cap
    mine = lax.axis_index("seq")
    t = lax.axis_index("tp")
    chip, core = t // 2, lax.rem(t, 2)
    shard = mine * tp_size + t
    partner = t + 1 - 2 * core
    across = lax.rem(t + 2, tp_size)
    diagonal = lax.rem(partner + 2, tp_size)
    tile = 2 * HEAD_DIM
    tiles = columns // tile
    scale = HEAD_DIM ** (-0.5)

    def remote(src, dst, send, recv, device):
        return pltpu.make_async_remote_copy(
            src_ref=src,
            dst_ref=dst,
            send_sem=send,
            recv_sem=recv,
            device_id=device,
            device_id_type=MESH,
        )

    pieces = weight_sem.shape[1]

    def weight_copies(i, far, near):
        depth = far.shape[0] // pieces
        return [
            pltpu.make_async_copy(
                far.at[pl.ds(p * depth, depth)], near.at[pl.ds(p * depth, depth)], weight_sem.at[i, p]
            )
            for p in range(pieces)
        ]

    up_copies = weight_copies(0, w_up_far, w_up)
    out_copies = weight_copies(1, w_out_far, w_out)
    key_copies = weight_copies(2, w_key_far, w_key)
    query_copies = weight_copies(3, w_query_far, w_query)
    value_copies = weight_copies(4, w_value_far, w_value)
    for copies in (up_copies, out_copies, key_copies, query_copies, value_copies):
        for copy in copies:
            copy.start()

    barrier = pltpu.get_barrier_semaphore()
    for offset in range(1, tp_size):
        pl.semaphore_signal(
            barrier, inc=1, device_id={"tp": lax.rem(t + offset, tp_size)}, device_id_type=MESH
        )
    for offset in range(1, seq_size):
        pl.semaphore_signal(
            barrier, inc=1, device_id={"seq": lax.rem(mine + offset, seq_size)}, device_id_type=MESH
        )
    has_before = shard > 0
    has_after = shard < shards - 1
    group_first = jnp.logical_and(t == 0, has_before)
    group_last = jnp.logical_and(t == tp_size - 1, has_after)
    shard_before = {
        "seq": jnp.where(t == 0, lax.rem(mine + seq_size - 1, seq_size), mine),
        "tp": lax.rem(t + tp_size - 1, tp_size),
    }
    shard_after = {
        "seq": jnp.where(t == tp_size - 1, lax.rem(mine + 1, seq_size), mine),
        "tp": lax.rem(t + 1, tp_size),
    }

    @pl.when(group_first)
    def _():
        pl.semaphore_signal(barrier, inc=1, device_id=shard_before, device_id_type=MESH)

    @pl.when(group_last)
    def _():
        pl.semaphore_signal(barrier, inc=1, device_id=shard_after, device_id_type=MESH)

    limit = float(byte_rows)
    own = starts[pl.ds(shard, 1), :].astype(WIDE)
    after = starts[pl.ds(jnp.minimum(shard + 1, shards - 1), 1), :].astype(WIDE)
    first = to_column(own)
    slot = lax.broadcasted_iota(jnp.int32, (cap, 1), 0)
    following = to_column(own, 1) + jnp.where(slot == cap - 1, limit, 0.0)
    places = lax.broadcasted_iota(jnp.int32, (cap, byte_rows), 1).astype(WIDE)
    inside = jnp.where((places >= first) & (places < following), 1.0, 0.0).astype(LOW)
    lead_places = lax.broadcasted_iota(jnp.int32, (16, byte_rows), 1).astype(WIDE)
    leading = jnp.where(lead_places < own[:, :1], 1.0, 0.0).astype(LOW)
    lead_out[...] = dot(leading, encoded[...])[:1]

    index = lax.broadcasted_iota(jnp.int32, (patches_total, shards), 0)
    lane = lax.broadcasted_iota(jnp.int32, (patches_total, shards), 1)
    owner = jnp.where((index >= lane * cap) & (index < lane * cap + cap), 1.0, 0.0).astype(LOW)
    valid = jnp.where(starts[...].astype(WIDE) < limit, 1.0, 0.0).astype(LOW)
    spread = dot(owner, valid)
    slots = lax.broadcasted_iota(jnp.int32, (patches_total, cap), 1)
    places_in = lax.broadcasted_iota(jnp.int32, (patches_total, cap), 0)
    valid_column[...] = jnp.sum(
        jnp.where(jnp.bitwise_and(places_in, cap - 1) == slots, spread, 0.0), 1, keepdims=True
    )
    own_rows = tile_of(mine, rows)
    row_valid = valid_column[own_rows, :]
    wide_grad[t] = jnp.where(row_valid > 0.5, cotangent[...].astype(WIDE), 0.0).astype(LOW)
    sums = dot(inside, encoded[...])

    neighbours = group_first.astype(jnp.int32) + group_last.astype(jnp.int32)
    pl.semaphore_wait(barrier, tp_size + seq_size - 2 + neighbours)

    lead_copy = remote(lead_out, lead_in, lead_sem.at[0], lead_sem.at[1], shard_before)

    @pl.when(has_before)
    def _():
        lead_copy.start()

    def gather_start(k, view):
        piece = view(t)
        remote(
            piece, piece, gather_send.at[0, k], gather_recv.at[0, k], {"tp": across}
        ).start()
        remote(
            piece, piece, gather_send.at[1, k], gather_recv.at[1, k], {"tp": partner}
        ).start()

    def gather_relay(k, view):
        piece = view(across)
        remote(
            piece, piece, gather_send.at[0, k], gather_recv.at[0, k], {"tp": across}
        ).wait_recv()
        remote(
            piece, piece, gather_send.at[2, k], gather_recv.at[2, k], {"tp": partner}
        ).start()

    def gather_finish(k, view):
        for way, origin in ((1, partner), (2, diagonal)):
            piece = view(origin)
            remote(
                piece, piece, gather_send.at[way, k], gather_recv.at[way, k], {"tp": partner}
            ).wait_recv()

    def gather_drain(k, view):
        for way, origin, target in ((0, t, across), (1, t, partner), (2, across, partner)):
            piece = view(origin)
            remote(
                piece, piece, gather_send.at[way, k], gather_recv.at[way, k], {"tp": target}
            ).wait_send()

    half_rows = rows // 2
    grad_views = [
        lambda q, p=p: wide_grad.at[q, pl.ds(p * half_rows, half_rows)] for p in range(2)
    ]
    group_view = lambda q: group.at[tile_of(q, cap)]

    def wide_view(j):
        return lambda q: wide.at[q, :, tile_of(j, tile)]

    gather_start(1, grad_views[0])

    @pl.when(has_after)
    def _():
        lead_copy.wait_recv()

    joined = jnp.where(
        jnp.logical_and(first < limit, following >= limit), jnp.where(has_after, 1.0, 0.0), 0.0
    )
    sums = sums + joined * jnp.where(has_after, lead_in[...], 0.0)
    sizes = (following - first) * jnp.where(first < limit, 1.0, 0.0) + joined * after[:, :1]
    group[tile_of(t, cap), :] = (sums / jnp.maximum(sizes, 1.0)).astype(LOW)
    gather_start(0, group_view)
    gather_start(2, grad_views[1])
    gather_relay(0, group_view)
    for copy in up_copies:
        copy.wait()
    gather_finish(0, group_view)

    def up_step(j, carry):
        wide[t, :, tile_of(j, tile)] = dot(group[...], w_up[:, tile_of(j, tile)]).astype(LOW)
        gather_start(3 + j, wide_view(j))
        return carry

    lax.fori_loop(0, tiles, up_step, 0)

    far_half = 1 - mine // (seq_size // 2)

    def send_heads(a, j, block):
        for u in range(2):
            h = 2 * j + u
            part = block[:, u * HEAD_DIM : (u + 1) * HEAD_DIM]

            @pl.when(h == mine)
            def _():
                heads[a, own_rows, :] = part

            @pl.when(h != mine)
            def _():
                outbox[a, h] = part
                remote(
                    outbox.at[a, h],
                    heads.at[a, own_rows],
                    out_send.at[a, h],
                    out_recv.at[a, mine],
                    {"seq": h},
                ).start()

    def tile_order(jj):
        return lax.rem(far_half * (tiles // 2) + jj, tiles)

    for p in range(2):
        gather_relay(1 + p, grad_views[p])
    for copy in out_copies:
        copy.wait()
    for p in range(2):
        gather_finish(1 + p, grad_views[p])

    def d_attn_step(jj, carry):
        j = tile_order(jj)
        acc = jnp.zeros((rows, tile), WIDE)
        for q in range(tp_size):
            acc += dot_last(
                wide_grad[q], w_out[tile_of(j, tile), q * columns : (q + 1) * columns]
            )
        send_heads(3, j, acc.astype(LOW))
        return carry

    lax.fori_loop(0, tiles, d_attn_step, 0)

    def relay_step(j, carry):
        gather_relay(3 + j, wide_view(j))
        return carry

    def finish_step(j, carry):
        gather_finish(3 + j, wide_view(j))
        return carry

    lax.fori_loop(0, tiles, relay_step, 0)
    lax.fori_loop(0, tiles, finish_step, 0)

    def norm_step(q, square):
        piece = wide[q].astype(WIDE)
        scaled[q] = (piece * gain[:, tile_of(q, columns)]).astype(LOW)
        return square + jnp.sum(piece * piece, 1, keepdims=True)

    square = lax.fori_loop(0, tp_size, norm_step, jnp.zeros((rows, 1), WIDE))
    rinv_column[...] = lax.rsqrt(square / model_width + EPS)

    def project(a, weight, copies):
        for copy in copies:
            copy.wait()

        def step(jj, carry):
            j = tile_order(jj)
            acc = jnp.zeros((rows, tile), WIDE)
            for q in range(tp_size):
                acc += dot(scaled[q], weight[q * columns : (q + 1) * columns, tile_of(j, tile)])
            send_heads(a, j, (rinv_column[...] * acc).astype(LOW))
            return carry

        lax.fori_loop(0, tiles, step, 0)

    project(1, w_key, key_copies)
    project(0, w_query, query_copies)
    project(2, w_value, value_copies)

    def heads_arrived(a):
        for offset in range(1, seq_size):
            source = lax.rem(mine + offset, seq_size)
            place = heads.at[a, tile_of(source, rows)]
            remote(
                place, place, out_send.at[a, source], out_recv.at[a, source], {"seq": source}
            ).wait_recv()

    for a in (3, 1, 0, 2):
        heads_arrived(a)

    blocks = patches_total // tile

    def turn_step(j, carry):
        at = tile_of(j, tile)
        key_turned[:, at] = heads[1, at, :].astype(WIDE).T.astype(LOW)
        value_turned[:, at] = heads[2, at, :].astype(WIDE).T.astype(LOW)
        key_sum[at, :] = jnp.zeros((tile, HEAD_DIM), WIDE)
        value_sum[at, :] = jnp.zeros((tile, HEAD_DIM), WIDE)
        return carry

    lax.fori_loop(0, blocks, turn_step, 0)

    def attend(i):
        queries = pl.ds(i * tile, tile)

        def score_step(j, peak):
            at = tile_of(j, tile)
            score = dot_last(heads[1, at, :], heads[0, queries, :]) * scale
            key = lax.broadcasted_iota(jnp.int32, (tile, tile), 0) + j * tile
            query = lax.broadcasted_iota(jnp.int32, (tile, tile), 1) + i * tile
            score = jnp.where((valid_column[at, :] > 0.5) & (key <= query), score, NEG)
            scores[at, :] = score
            d_probs[at, :] = dot_last(heads[2, at, :], heads[3, queries, :])
            return jnp.maximum(peak, jnp.max(score, 0, keepdims=True))

        peak = lax.fori_loop(0, i + 1, score_step, jnp.full((1, tile), NEG, WIDE))

        def mix_step(j, carry):
            total, mixed = carry
            at = tile_of(j, tile)
            expo = jnp.exp(scores[at, :] - peak)
            scores[at, :] = expo
            total += jnp.sum(expo, 0, keepdims=True)
            mixed += dot(value_turned[:, at], expo.astype(LOW))
            return total, mixed

        total, mixed = lax.fori_loop(
            0,
            i + 1,
            mix_step,
            (jnp.zeros((1, tile), WIDE), jnp.zeros((HEAD_DIM, tile), WIDE)),
        )
        share = 1.0 / total
        attn = (mixed / total).astype(LOW).astype(WIDE)
        delta = jnp.sum(heads[3, queries, :].astype(WIDE).T * attn, 0, keepdims=True)
        returns[0, queries, :] = attn.T.astype(LOW)

        def grad_step(j, query_sum):
            at = tile_of(j, tile)
            probs = scores[at, :] * share
            d_scores = (probs * (d_probs[at, :] - delta)).astype(LOW)
            value_sum[at, :] += dot(probs.astype(LOW), heads[3, queries, :])
            key_sum[at, :] += dot(d_scores, heads[0, queries, :])
            return query_sum + dot(key_turned[:, at], d_scores)

        query_sum = lax.fori_loop(0, i + 1, grad_step, jnp.zeros((HEAD_DIM, tile), WIDE))
        returns[1, queries, :] = (query_sum * scale).T.astype(LOW)
        returns[2, queries, :] = value_sum[queries, :].astype(LOW)
        returns[3, queries, :] = (key_sum[queries, :] * scale).astype(LOW)

    own_columns = tile_of(mine, HEAD_DIM)

    def return_copy(a, peer):
        return remote(
            returns.at[a, pl.ds(peer * rows, rows)],
            back.at[a, :, own_columns],
            back_send.at[a, peer],
            back_recv.at[a, mine],
            {"seq": peer},
        )

    returned = returns.shape[0]
    for i in reversed(range(blocks)):
        attend(i)
        for a in range(returned):
            for peer in range(i * tile // rows, (i + 1) * tile // rows):

                @pl.when(peer != mine)
                def _():
                    return_copy(a, peer).start()

                @pl.when(peer == mine)
                def _():
                    back[a, :, own_columns] = returns[a, peer * rows : (peer + 1) * rows, :]

    def returns_arrived(a):
        for offset in range(1, seq_size):
            source = lax.rem(mine + offset, seq_size)
            place = back.at[a, :, tile_of(source, HEAD_DIM)]
            remote(
                place, place, back_send.at[a, source], back_recv.at[a, source], {"seq": source}
            ).wait_recv()

    order = (
        (1 - chip) * 2 + (1 - core),
        (1 - chip) * 2 + core,
        chip * 2 + (1 - core),
        chip * 2 + core,
    )

    def pair_copy(a, k):
        return remote(
            partial.at[a, order[2 * k]],
            pair_in.at[a, k],
            pair_send.at[a, k],
            pair_recv.at[a, k],
            {"tp": partner},
        )

    def cross_copy(a):
        return remote(
            cross_out.at[a], cross_in.at[a], cross_send.at[a], cross_recv.at[a], {"tp": across}
        )

    returns_arrived(0)
    for k in range(tp_size):
        quarter = order[k]

        def value_step(j, carry):
            at = tile_of(quarter * tiles + j, tile)
            partial[0, quarter, :, tile_of(j, tile)] = dot(back[0], w_out[:, at]).astype(LOW)
            return carry

        lax.fori_loop(0, tiles, value_step, 0)
        if k % 2 == 0:
            pair_copy(0, k // 2).start()
    pair_copy(0, 0).wait_recv()
    cross_out[0] = (partial[0, order[1]].astype(WIDE) + pair_in[0, 0].astype(WIDE)).astype(LOW)
    cross_copy(0).start()

    for a, weight in ((1, w_query), (2, w_value)):
        returns_arrived(a)
        for quarter in range(tp_size):

            def grad_in_step(j, carry):
                at = tile_of(quarter * tiles + j, tile)
                more = dot_last(back[a], weight[at, :])
                here = tile_of(j, tile)
                if a == 1:
                    grad_sum[quarter, :, here] = more
                else:
                    grad_sum[quarter, :, here] += more
                return carry

            lax.fori_loop(0, tiles, grad_in_step, 0)
    returns_arrived(3)
    dots = jnp.zeros((rows, 1), WIDE)
    for k in range(tp_size):
        quarter = order[k]

        def last_step(j, dots):
            at = tile_of(quarter * tiles + j, tile)
            here = tile_of(j, tile)
            whole = grad_sum[quarter, :, here] + dot_last(back[3], w_key[at, :])
            partial[1, quarter, :, here] = whole.astype(LOW)
            inner = gain[:, at] * whole * wide[quarter, :, here].astype(WIDE)
            return dots + jnp.sum(inner, 1, keepdims=True)

        dots = lax.fori_loop(0, tiles, last_step, dots)
        if k % 2 == 0:
            pair_copy(1, k // 2).start()
        if k == 1:
            pair_copy(1, 0).wait_recv()
            cross_out[1] = (
                partial[1, order[1]].astype(WIDE) + pair_in[1, 0].astype(WIDE)
            ).astype(LOW)
            cross_copy(1).start()

    def dots_copy(offset):
        return remote(
            dots_out,
            dots_in.at[offset],
            dots_send.at[offset],
            dots_recv.at[offset],
            {"tp": lax.rem(t + offset, tp_size)},
        )

    dots_out[...] = jnp.broadcast_to(to_row(dots), dots_out.shape)
    for offset in range(1, tp_size):
        dots_copy(offset).start()

    wide_in = wide[t].astype(WIDE)
    rinv = rinv_column[...]
    pair_copy(0, 1).wait_recv()
    cross_copy(0).wait_recv()
    total_value = (
        partial[0, t].astype(WIDE) + pair_in[0, 1].astype(WIDE) + cross_in[0].astype(WIDE)
    )
    out_value[...] = jnp.where(row_valid > 0.5, wide_in + total_value, 0.0).astype(LOW)
    for offset in range(1, tp_size):
        dots_copy(offset).wait_recv()
        dots += to_column(dots_in[offset][:1])
    pair_copy(1, 1).wait_recv()
    cross_copy(1).wait_recv()
    total_grad = (
        partial[1, t].astype(WIDE) + pair_in[1, 1].astype(WIDE) + cross_in[1].astype(WIDE)
    )
    out_grad[...] = (
        wide_grad[t].astype(WIDE)
        + rinv * gain[:, tile_of(t, columns)] * total_grad
        - wide_in * (rinv**3 * dots / model_width)
    )

    @pl.when(has_before)
    def _():
        lead_copy.wait_send()

    gather_drain(0, group_view)
    for p in range(2):
        gather_drain(1 + p, grad_views[p])

    def drain_step(j, carry):
        gather_drain(3 + j, wide_view(j))
        return carry

    lax.fori_loop(0, tiles, drain_step, 0)
    for offset in range(1, seq_size):
        peer = lax.rem(mine + offset, seq_size)
        for a in range(heads.shape[0]):
            remote(
                outbox.at[a, peer],
                heads.at[a, own_rows],
                out_send.at[a, peer],
                out_recv.at[a, mine],
                {"seq": peer},
            ).wait_send()
        for a in range(returned):
            remote(
                returns.at[a, tile_of(peer, rows)],
                back.at[a, :, own_columns],
                back_send.at[a, peer],
                back_recv.at[a, mine],
                {"seq": peer},
            ).wait_send()
    for a in range(2):
        for k in range(2):
            pair_copy(a, k).wait_send()
        cross_copy(a).wait_send()
    for offset in range(1, tp_size):
        dots_copy(offset).wait_send()


def per_device_whole(encoded, starts, w_up, norm_gain, w_query, w_key, w_value, w_out, cotangent):
    seq_size, tp_size = lax.axis_size("seq"), lax.axis_size("tp")
    rows, columns = cotangent.shape
    model_width = norm_gain.shape[0]
    byte_width = encoded.shape[1]
    cap = starts.shape[1]
    total = starts.size
    tile = 2 * HEAD_DIM
    chunks = 3 + columns // tile
    dma = pltpu.SemaphoreType.DMA
    scratch = [
        pltpu.VMEM(w_up.shape, LOW),
        pltpu.VMEM(w_query.shape, LOW),
        pltpu.VMEM(w_key.shape, LOW),
        pltpu.VMEM(w_value.shape, LOW),
        pltpu.VMEM(w_out.shape, LOW),
        pltpu.VMEM((1, byte_width), WIDE),
        pltpu.VMEM((1, byte_width), WIDE),
        pltpu.VMEM((rows, byte_width), LOW),
        pltpu.VMEM((tp_size, rows, columns), LOW),
        pltpu.VMEM((tp_size, rows, columns), LOW),
        pltpu.VMEM((tp_size, rows, columns), LOW),
        pltpu.VMEM((total, 1), WIDE),
        pltpu.VMEM((rows, 1), WIDE),
        pltpu.VMEM((4, seq_size, rows, HEAD_DIM), LOW),
        pltpu.VMEM((4, total, HEAD_DIM), LOW),
        pltpu.VMEM((HEAD_DIM, total), LOW),
        pltpu.VMEM((HEAD_DIM, total), LOW),
        pltpu.VMEM((total, tile), WIDE),
        pltpu.VMEM((total, tile), WIDE),
        pltpu.VMEM((total, HEAD_DIM), WIDE),
        pltpu.VMEM((total, HEAD_DIM), WIDE),
        pltpu.VMEM((4, total, HEAD_DIM), LOW),
        pltpu.VMEM((4, rows, columns), LOW),
        pltpu.VMEM((tp_size, rows, columns), WIDE),
        pltpu.VMEM((2, tp_size, rows, columns), LOW),
        pltpu.VMEM((2, 2, rows, columns), LOW),
        pltpu.VMEM((2, rows, columns), LOW),
        pltpu.VMEM((2, rows, columns), LOW),
        pltpu.VMEM((8, rows), WIDE),
        pltpu.VMEM((tp_size, 8, rows), WIDE),
        dma((5, 4)),
        dma((2,)),
        dma((3, chunks)),
        dma((3, chunks)),
        dma((4, seq_size)),
        dma((4, seq_size)),
        dma((4, seq_size)),
        dma((4, seq_size)),
            dma((2, 2)),
        dma((2, 2)),
        dma((2,)),
        dma((2,)),
        dma((tp_size,)),
        dma((tp_size,)),
    ]
    near = pl.BlockSpec(memory_space=pltpu.VMEM)
    far = pl.BlockSpec(memory_space=pl.ANY)
    return tuple(
        pl.pallas_call(
            functools.partial(layer_kernel, seq_size, tp_size),
            out_shape=[
                jax.ShapeDtypeStruct((rows, columns), LOW),
                jax.ShapeDtypeStruct((rows, columns), WIDE),
            ],
            in_specs=[near] * 4 + [far] * 5,
            out_specs=[near] * 2,
            scratch_shapes=scratch,
            compiler_params=pltpu.CompilerParams(
                collective_id=0, has_side_effects=True, vmem_limit_bytes=67043328
            ),
        )(
            encoded,
            starts,
            norm_gain.reshape(1, model_width),
            cotangent,
            w_up,
            w_query,
            w_key,
            w_value,
            w_out,
        )
    )


def fits_one_kernel(arrays):
    encoded, starts, w_up, norm_gain, w_query, w_key, w_value, w_out, cotangent = arrays
    seq_size, tp_size = lax.axis_size("seq"), lax.axis_size("tp")
    rows, columns = cotangent.shape
    cap = starts.shape[1]
    return (
        tp_size == 4
        and seq_size % 2 == 0
        and columns == seq_size * HEAD_DIM
        and rows == HEAD_DIM
        and rows == tp_size * cap
        and cap & (cap - 1) == 0
        and cap % 16 == 0
        and columns % (4 * HEAD_DIM) == 0
        and norm_gain.shape[0] == tp_size * columns
        and starts.shape[0] == seq_size * tp_size
        and starts.size % (2 * HEAD_DIM) == 0
    )


def solution(mesh):
    in_specs = (
        P(("seq", "tp"), None),
        P(),
        P(None, "tp"),
        P(),
        P(None, "tp"),
        P(None, "tp"),
        P(None, "tp"),
        P("tp", None),
        P("seq", "tp"),
    )
    out_specs = (P("seq", "tp"), P("seq", "tp"))

    def choose(*arrays):
        return (per_device_whole if fits_one_kernel(arrays) else per_device)(*arrays)

    return jax.shard_map(
        choose, mesh=mesh, in_specs=in_specs, out_specs=out_specs, check_vma=False
    )
```

```python
import functools

import jax
import jax.numpy as jnp
from jax import lax
from jax.experimental import pallas as pl
from jax.experimental.pallas import tpu as pltpu
from jax.sharding import PartitionSpec as P

HEAD_DIM = 128


EPS = 1e-05
NEG = -1e30
CONTRACT_LAST = (((1,), (1,)), ((), ()))


def shifted(block, axis, distance):
    devices = range(lax.axis_size(axis))
    route = [(i - distance, i) for i in devices if i - distance in devices]
    return lax.ppermute(block, axis, route)


def per_device(encoded, starts, w_up, norm_gain, w_query, w_key, w_value, w_out, cotangent):
    byte_rows = encoded.shape[0]
    patch_cap = starts.shape[1]
    model_width = norm_gain.shape[0]
    shard = lax.axis_index(("seq", "tp"))
    own_starts = lax.dynamic_slice_in_dim(starts, shard, 1, 0)[0]
    places = jnp.arange(byte_rows, dtype=jnp.int32)
    following = jnp.concatenate([own_starts[1:], jnp.full((1,), byte_rows, jnp.int32)])
    inside = (places[None, :] >= own_starts[:, None]) & (places[None, :] < following[:, None])
    sums = jnp.dot(inside.astype(jnp.bfloat16), encoded, preferred_element_type=jnp.float32)
    sizes = jnp.sum(inside.astype(jnp.float32), 1)
    leading = places[None, :] < own_starts[:1, None]
    lead_sum = jnp.dot(leading.astype(jnp.bfloat16), encoded, preferred_element_type=jnp.float32)
    lead_size = jnp.sum(leading.astype(jnp.float32), 1)
    next_sum, next_size = shifted((lead_sum, lead_size), ("seq", "tp"), -1)
    count = jnp.sum((own_starts < byte_rows).astype(jnp.int32))
    last_slot = (jnp.arange(patch_cap, dtype=jnp.int32) == count - 1).astype(jnp.float32)
    sums = sums + last_slot[:, None] * next_sum
    sizes = sizes + last_slot * next_size
    patches = (sums / jnp.maximum(sizes, 1.0)[:, None]).astype(jnp.bfloat16)
    group = lax.all_gather(patches, "tp", axis=0, tiled=True)
    latent_in = jnp.dot(group, w_up, preferred_element_type=jnp.float32).astype(jnp.bfloat16)
    group_rows, columns = latent_in.shape
    head_count = columns // HEAD_DIM
    wide_piece = lax.all_gather(latent_in, "tp", axis=1, tiled=True).astype(jnp.float32)
    scaled = (wide_piece * norm_gain[None, :]).astype(jnp.bfloat16)
    acc_query = jnp.dot(scaled, w_query, preferred_element_type=jnp.float32)
    acc_key = jnp.dot(scaled, w_key, preferred_element_type=jnp.float32)
    acc_value = jnp.dot(scaled, w_value, preferred_element_type=jnp.float32)
    acc_query, acc_key, acc_value, square = (
        acc_query,
        acc_key,
        acc_value,
        jnp.sum(wide_piece * wide_piece, 1),
    )
    rinv = lax.rsqrt(square / model_width + EPS)
    query = (rinv[:, None] * acc_query).astype(jnp.bfloat16)
    key_rows = (rinv[:, None] * acc_key).astype(jnp.bfloat16)
    value_rows = (rinv[:, None] * acc_value).astype(jnp.bfloat16)
    keys_all, values_all = (
        lax.all_gather(key_rows, "seq", axis=0, tiled=True),
        lax.all_gather(value_rows, "seq", axis=0, tiled=True),
    )
    patches_total = keys_all.shape[0]
    valid_all = (starts < byte_rows).reshape(patches_total)
    row_base = lax.axis_index("seq") * group_rows
    query_index = row_base + jnp.arange(group_rows, dtype=jnp.int32)
    key_index = jnp.arange(patches_total, dtype=jnp.int32)
    query_valid = lax.dynamic_slice_in_dim(valid_all, row_base, group_rows, 0)
    allowed = valid_all[None, :] & (key_index[None, :] <= query_index[:, None])
    scale = HEAD_DIM ** (-0.5)
    query_heads = query.reshape(group_rows, head_count, HEAD_DIM)
    key_heads = keys_all.reshape(patches_total, head_count, HEAD_DIM)
    value_heads = values_all.reshape(patches_total, head_count, HEAD_DIM)
    scores = (
        jnp.einsum("rhd,khd->hrk", query_heads, key_heads, preferred_element_type=jnp.float32)
        * scale
    )
    peak = jnp.max(jnp.where(allowed[None], scores, NEG), 2)
    expo = jnp.where(allowed[None], jnp.exp(scores - peak[:, :, None]), 0.0)
    total = jnp.sum(expo, 2)
    mixed = jnp.einsum(
        "hrk,khd->rhd", expo.astype(jnp.bfloat16), value_heads, preferred_element_type=jnp.float32
    )
    attn = (mixed / total.T[:, :, None]).astype(jnp.bfloat16)
    partial_value = jnp.dot(
        attn.reshape(group_rows, columns), w_out, preferred_element_type=jnp.float32
    )
    head_sum = lax.psum_scatter(
        partial_value.astype(jnp.bfloat16), "tp", scatter_dimension=1, tiled=True
    ).astype(jnp.float32)
    wide_in = latent_in.astype(jnp.float32)
    latent_out = jnp.where(query_valid[:, None], wide_in + head_sum, 0.0).astype(jnp.bfloat16)
    grad_out = jnp.where(query_valid[:, None], cotangent, jnp.zeros_like(cotangent))
    d_attn = lax.dot_general(
        lax.all_gather(grad_out, "tp", axis=1, tiled=True),
        w_out,
        CONTRACT_LAST,
        preferred_element_type=jnp.float32,
    ).astype(jnp.bfloat16)
    grad_heads = d_attn.reshape(group_rows, head_count, HEAD_DIM)
    delta = jnp.sum(grad_heads.astype(jnp.float32) * attn.astype(jnp.float32), 2).T
    probs = expo / total[:, :, None]
    d_probs = jnp.einsum(
        "rhd,khd->hrk", grad_heads, value_heads, preferred_element_type=jnp.float32
    )
    d_scores = (probs * (d_probs - delta[:, :, None])).astype(jnp.bfloat16)
    grad_query = (
        (
            jnp.einsum("hrk,khd->rhd", d_scores, key_heads, preferred_element_type=jnp.float32)
            * scale
        )
        .astype(jnp.bfloat16)
        .reshape(group_rows, columns)
    )
    weights_low = probs.astype(jnp.bfloat16)
    count_rows = group_rows * lax.axis_size("seq")
    key_part = jnp.einsum("hrk,rhd->khd", d_scores, query_heads, preferred_element_type=jnp.float32)
    value_part = jnp.einsum(
        "hrk,rhd->khd", weights_low, grad_heads, preferred_element_type=jnp.float32
    )
    both = lax.psum_scatter(
        jnp.concatenate(
            [key_part.reshape(count_rows, columns), value_part.reshape(count_rows, columns)], 1
        ).astype(jnp.bfloat16),
        "seq",
        scatter_dimension=0,
        tiled=True,
    ).astype(jnp.float32)
    grad_key = (both[:, :columns] * scale).astype(jnp.bfloat16)
    grad_value = both[:, columns:].astype(jnp.bfloat16)
    dnormed = (
        lax.dot_general(grad_query, w_query, CONTRACT_LAST, preferred_element_type=jnp.float32)
        + lax.dot_general(grad_key, w_key, CONTRACT_LAST, preferred_element_type=jnp.float32)
        + lax.dot_general(grad_value, w_value, CONTRACT_LAST, preferred_element_type=jnp.float32)
    )
    normed_grad = lax.psum_scatter(
        dnormed.astype(jnp.bfloat16), "tp", scatter_dimension=1, tiled=True
    ).astype(jnp.float32)
    gain_own = lax.dynamic_slice_in_dim(norm_gain, lax.axis_index("tp") * columns, columns, 0)
    dots = lax.psum(jnp.sum(gain_own[None, :] * normed_grad * wide_in, 1), "tp")
    latent_grad = (
        grad_out.astype(jnp.float32)
        + rinv[:, None] * gain_own[None, :] * normed_grad
        - wide_in * (rinv**3)[:, None] * dots[:, None] / model_width
    )
    return (latent_out, latent_grad)


MESH = pl.DeviceIdType.MESH
LOW = jnp.bfloat16
WIDE = jnp.float32
ROWS_FIRST = (((0,), (0,)), ((), ()))


def tile_of(index, size):
    return pl.ds(pl.multiple_of(index * size, size), size)


def dot(a, b):
    return jnp.dot(a, b, preferred_element_type=WIDE)


def dot_last(a, b):
    return lax.dot_general(a, b, CONTRACT_LAST, preferred_element_type=WIDE)


def to_row(column, lanes):
    n = column.shape[0]
    down = lax.broadcasted_iota(jnp.int32, (n, lanes), 0)
    across = lax.broadcasted_iota(jnp.int32, (n, lanes), 1)
    return jnp.sum(jnp.where(down == across, column, 0.0), 0, keepdims=True)


def to_column(row, n, shift=0):
    lanes = row.shape[1]
    down = lax.broadcasted_iota(jnp.int32, (n, lanes), 0)
    across = lax.broadcasted_iota(jnp.int32, (n, lanes), 1)
    return jnp.sum(jnp.where(down + shift == across, row, 0.0), 1, keepdims=True)


def layer_kernel(
    seq_size,
    tp_size,
    starts_far,
    gain_far,
    encoded_far,
    cotangent_far,
    w_up_far,
    w_query_far,
    w_key_far,
    w_value_far,
    w_out_far,
    out_value,
    out_grad,
    starts,
    gain,
    encoded,
    cotangent,
    w_up,
    w_query,
    w_key,
    w_value,
    w_out,
    lead_out,
    lead_in,
    group,
    wide,
    wide_grad,
    scaled,
    valid_column,
    key_bias,
    rinv_column,
    outbox,
    heads,
    value_turned,
    key_turned,
    scores,
    attn_turned,
    share_row,
    key_sum,
    value_sum,
    returns,
    back,
    grad_sum,
    partial,
    pair_in,
    cross_out,
    cross_in,
    dots_out,
    dots_in,
    weight_sem,
    near_sem,
    lead_sem,
    gather_send,
    gather_recv,
    out_send,
    out_recv,
    back_send,
    back_recv,
    pair_send,
    pair_recv,
    cross_send,
    cross_recv,
    dots_send,
    dots_recv,
):
    byte_rows, byte_width = encoded.shape
    shards, cap = starts.shape
    rows, columns = cotangent.shape
    model_width = gain.shape[1]
    patches_total = shards * cap
    mine = lax.axis_index("seq")
    t = lax.axis_index("tp")
    chip, core = t // 2, lax.rem(t, 2)
    shard = mine * tp_size + t
    partner = t + 1 - 2 * core
    across = lax.rem(t + 2, tp_size)
    diagonal = lax.rem(partner + 2, tp_size)
    tile = 2 * HEAD_DIM
    tiles = columns // tile
    scale = HEAD_DIM ** (-0.5)

    def remote(src, dst, send, recv, device):
        return pltpu.make_async_remote_copy(
            src_ref=src,
            dst_ref=dst,
            send_sem=send,
            recv_sem=recv,
            device_id=device,
            device_id_type=MESH,
        )

    barrier = pltpu.get_barrier_semaphore()
    for offset in range(1, tp_size):
        pl.semaphore_signal(
            barrier, inc=1, device_id={"tp": lax.rem(t + offset, tp_size)}, device_id_type=MESH
        )
    for offset in range(1, seq_size):
        pl.semaphore_signal(
            barrier, inc=1, device_id={"seq": lax.rem(mine + offset, seq_size)}, device_id_type=MESH
        )
    has_before = shard > 0
    has_after = shard < shards - 1
    group_first = jnp.logical_and(t == 0, has_before)
    group_last = jnp.logical_and(t == tp_size - 1, has_after)
    shard_before = {
        "seq": jnp.where(t == 0, lax.rem(mine + seq_size - 1, seq_size), mine),
        "tp": lax.rem(t + tp_size - 1, tp_size),
    }
    shard_after = {
        "seq": jnp.where(t == tp_size - 1, lax.rem(mine + 1, seq_size), mine),
        "tp": lax.rem(t + 1, tp_size),
    }

    @pl.when(group_first)
    def _():
        pl.semaphore_signal(barrier, inc=1, device_id=shard_before, device_id_type=MESH)

    @pl.when(group_last)
    def _():
        pl.semaphore_signal(barrier, inc=1, device_id=shard_after, device_id_type=MESH)

    near_copies = [
        pltpu.make_async_copy(starts_far, starts, near_sem.at[0]),
        pltpu.make_async_copy(encoded_far, encoded, near_sem.at[1]),
        pltpu.make_async_copy(cotangent_far, cotangent, near_sem.at[2]),
        pltpu.make_async_copy(gain_far, gain, near_sem.at[3]),
    ]
    for copy in near_copies:
        copy.start()
    pieces = weight_sem.shape[1]

    def weight_copies(i, far, near):
        depth = far.shape[0] // pieces
        return [
            pltpu.make_async_copy(
                far.at[pl.ds(p * depth, depth)], near.at[pl.ds(p * depth, depth)], weight_sem.at[i, p]
            )
            for p in range(pieces)
        ]

    up_copies = weight_copies(0, w_up_far, w_up)
    out_copies = weight_copies(1, w_out_far, w_out)
    key_copies = weight_copies(2, w_key_far, w_key)
    query_copies = weight_copies(3, w_query_far, w_query)
    value_copies = weight_copies(4, w_value_far, w_value)
    near_copies[0].wait()
    limit = float(byte_rows)
    own = starts[pl.ds(shard, 1), :].astype(WIDE)
    after = starts[pl.ds(jnp.minimum(shard + 1, shards - 1), 1), :].astype(WIDE)
    first = to_column(own, cap)
    slot = lax.broadcasted_iota(jnp.int32, (cap, 1), 0)
    following = to_column(own, cap, 1) + jnp.where(slot == cap - 1, limit, 0.0)
    places = lax.broadcasted_iota(jnp.int32, (cap, byte_rows), 1).astype(WIDE)
    inside = jnp.where((places >= first) & (places < following), 1.0, 0.0).astype(LOW)
    lead_places = lax.broadcasted_iota(jnp.int32, (16, byte_rows), 1).astype(WIDE)
    leading = jnp.where(lead_places < own[:, :1], 1.0, 0.0).astype(LOW)
    near_copies[1].wait()
    for copy in up_copies:
        copy.start()
    lead_out[...] = dot(leading, encoded[...])[:1]
    sums = dot(inside, encoded[...])

    index = lax.broadcasted_iota(jnp.int32, (patches_total, shards), 0)
    lane = lax.broadcasted_iota(jnp.int32, (patches_total, shards), 1)
    owner = jnp.where((index >= lane * cap) & (index < lane * cap + cap), 1.0, 0.0).astype(LOW)
    valid = jnp.where(starts[...].astype(WIDE) < limit, 1.0, 0.0).astype(LOW)
    spread = dot(owner, valid)
    slots = lax.broadcasted_iota(jnp.int32, (patches_total, cap), 1)
    places_in = lax.broadcasted_iota(jnp.int32, (patches_total, cap), 0)
    valid_column[...] = jnp.sum(
        jnp.where(jnp.bitwise_and(places_in, cap - 1) == slots, spread, 0.0), 1, keepdims=True
    )
    own_rows = tile_of(mine, rows)
    row_valid = valid_column[own_rows, :]
    key_bias[...] = jnp.broadcast_to((valid_column[...] - 1.0) * -NEG, key_bias.shape)
    near_copies[2].wait()
    wide_grad[t] = jnp.where(row_valid > 0.5, cotangent[...].astype(WIDE), 0.0).astype(LOW)
    near_copies[3].wait()

    neighbours = group_first.astype(jnp.int32) + group_last.astype(jnp.int32)
    pl.semaphore_wait(barrier, tp_size + seq_size - 2 + neighbours)

    lead_copy = remote(lead_out, lead_in, lead_sem.at[0], lead_sem.at[1], shard_before)

    @pl.when(has_before)
    def _():
        lead_copy.start()

    def gather_start(k, view):
        piece = view(t)
        remote(
            piece, piece, gather_send.at[0, k], gather_recv.at[0, k], {"tp": across}
        ).start()
        remote(
            piece, piece, gather_send.at[1, k], gather_recv.at[1, k], {"tp": partner}
        ).start()

    def gather_relay(k, view):
        piece = view(across)
        remote(
            piece, piece, gather_send.at[0, k], gather_recv.at[0, k], {"tp": across}
        ).wait_recv()
        remote(
            piece, piece, gather_send.at[2, k], gather_recv.at[2, k], {"tp": partner}
        ).start()

    def gather_finish(k, view, ways=(1, 2)):
        for way in ways:
            piece = view(partner if way == 1 else diagonal)
            remote(
                piece, piece, gather_send.at[way, k], gather_recv.at[way, k], {"tp": partner}
            ).wait_recv()

    def gather_drain(k, view):
        for way, origin, target in ((0, t, across), (1, t, partner), (2, across, partner)):
            piece = view(origin)
            remote(
                piece, piece, gather_send.at[way, k], gather_recv.at[way, k], {"tp": target}
            ).wait_send()

    grad_pieces = 4
    piece_rows = rows // grad_pieces
    grad_views = [
        lambda q, p=p: wide_grad.at[q, pl.ds(p * piece_rows, piece_rows)]
        for p in range(grad_pieces)
    ]
    group_view = lambda q: group.at[tile_of(q, cap)]
    half_rows = rows // 2
    wide_tile = columns // 2

    def wide_view(batch, j):
        def view(q):
            of_chip = q // 2
            place = of_chip if batch == 0 else 1 - of_chip
            return wide.at[
                q, tile_of(place, half_rows), j * wide_tile : (j + 1) * wide_tile
            ]

        return view

    def wide_chunk(batch, j):
        return 1 + grad_pieces + 2 * batch + j

    @pl.when(has_after)
    def _():
        lead_copy.wait_recv()

    joined = jnp.where(
        jnp.logical_and(first < limit, following >= limit), jnp.where(has_after, 1.0, 0.0), 0.0
    )
    sums = sums + joined * jnp.where(has_after, lead_in[...], 0.0)
    sizes = (following - first) * jnp.where(first < limit, 1.0, 0.0) + joined * after[:, :1]
    group[tile_of(t, cap), :] = (sums / jnp.maximum(sizes, 1.0)).astype(LOW)
    gather_start(0, group_view)
    for copies in (key_copies, query_copies, value_copies, out_copies):
        for copy in copies:
            copy.start()

    def raise_rows(batch):
        place = tile_of(chip if batch == 0 else 1 - chip, half_rows)
        for j in range(2):
            cut = slice(j * wide_tile, (j + 1) * wide_tile)
            wide[t, place, cut] = dot(group[place, :], w_up[:, cut]).astype(LOW)
            gather_start(wide_chunk(batch, j), wide_view(batch, j))

    gather_finish(0, group_view, (1,))
    for copy in up_copies:
        copy.wait()
    raise_rows(0)
    gather_relay(0, group_view)
    gather_finish(0, group_view, (2,))
    raise_rows(1)

    far_half = 1 - mine // (seq_size // 2)

    def head_copy(k, h):
        if k == 6:
            src, place = outbox.at[3, h], own_rows
        else:
            a, batch = k // 2, k % 2
            piece = 1 - chip if batch == 0 else chip
            src = outbox.at[a, h, tile_of(piece, half_rows)]
            place = tile_of(2 * mine + piece, half_rows)
        return remote(
            src,
            heads.at[3 if k == 6 else k // 2, place],
            out_send.at[k, h],
            out_recv.at[k, mine],
            {"seq": h},
        )

    def start_head(k, h):
        @pl.when(h != mine)
        def _():
            head_copy(k, h).start()

    def keep_heads(a, j, block, start, size):
        for u in range(2):
            h = 2 * j + u
            part = block[:, u * HEAD_DIM : (u + 1) * HEAD_DIM]

            @pl.when(h == mine)
            def _():
                heads[a, pl.ds(pl.multiple_of(mine * rows + start, size), size), :] = part

            @pl.when(h != mine)
            def _():
                outbox[a, h, pl.ds(pl.multiple_of(start, size), size), :] = part

    def tile_order(jj):
        return lax.rem(far_half * (tiles // 2) + jj, tiles)

    def relay_rows(batch):
        for j in range(2):
            gather_relay(wide_chunk(batch, j), wide_view(batch, j))

    def norm_rows(batch):
        place = tile_of(1 - chip if batch == 0 else chip, half_rows)

        def norm_step(q, square):
            piece = wide[q, place].astype(WIDE)
            scaled[q, place] = (piece * gain[:, tile_of(q, columns)]).astype(LOW)
            return square + jnp.sum(piece * piece, 1, keepdims=True)

        square = lax.fori_loop(0, tp_size, norm_step, jnp.zeros((half_rows, 1), WIDE))
        rinv_column[place, :] = lax.rsqrt(square / model_width + EPS)

    def project(a, weight, batch):
        piece = 1 - chip if batch == 0 else chip
        place = tile_of(piece, half_rows)

        def step(jj, carry):
            j = tile_order(jj)
            acc = jnp.zeros((half_rows, tile), WIDE)
            for q in range(tp_size):
                acc += dot(
                    scaled[q, place], weight[q * columns : (q + 1) * columns, tile_of(j, tile)]
                )
            block = (rinv_column[place, :] * acc).astype(LOW)
            keep_heads(a, j, block, piece * half_rows, half_rows)
            for u in range(2):
                start_head(2 * a + batch, 2 * j + u)
            return carry

        lax.fori_loop(0, tiles, step, 0)

    relay_rows(0)
    for j in range(2):
        gather_finish(wide_chunk(0, j), wide_view(0, j), (2,))
        gather_finish(wide_chunk(1, j), wide_view(1, j), (1,))
    norm_rows(0)
    for copy in key_copies:
        copy.wait()
    project(1, w_key, 0)
    relay_rows(1)
    for p in range(grad_pieces):
        gather_start(1 + p, grad_views[p])
    for copy in query_copies:
        copy.wait()
    project(0, w_query, 0)
    for copy in value_copies:
        copy.wait()
    project(2, w_value, 0)
    for j in range(2):
        gather_finish(wide_chunk(0, j), wide_view(0, j), (1,))
        gather_finish(wide_chunk(1, j), wide_view(1, j), (2,))
    norm_rows(1)
    project(1, w_key, 1)
    project(0, w_query, 1)
    for p in range(grad_pieces):
        gather_relay(1 + p, grad_views[p])
    project(2, w_value, 1)
    for copy in out_copies:
        copy.wait()
    for p in range(grad_pieces):
        gather_finish(1 + p, grad_views[p])

    def d_attn_step(jj, carry):
        j = tile_order(jj)
        acc = jnp.zeros((rows, tile), WIDE)
        for q in range(tp_size):
            acc += dot_last(
                wide_grad[q], w_out[tile_of(j, tile), q * columns : (q + 1) * columns]
            )
        keep_heads(3, j, acc.astype(LOW), 0, rows)
        return carry

    lax.fori_loop(0, tiles, d_attn_step, 0)


    def heads_arrived(k):
        for offset in range(1, seq_size):
            source = lax.rem(mine + offset, seq_size)
            if k == 6:
                place = heads.at[3, tile_of(source, rows)]
            else:
                piece = 1 - chip if k % 2 == 0 else chip
                place = heads.at[k // 2, tile_of(2 * source + piece, half_rows)]
            remote(
                place, place, out_send.at[k, source], out_recv.at[k, source], {"seq": source}
            ).wait_recv()

    for k in (2, 0, 4, 3, 1):
        heads_arrived(k)
    for step in range(seq_size):
        start_head(6, lax.rem(far_half * (seq_size // 2) + step, seq_size))
    heads_arrived(5)

    blocks = patches_total // tile
    own_columns = tile_of(mine, HEAD_DIM)

    def piece_of(k):
        if k < 3:
            return k, 0, rows
        return 3, half_rows * (k - 3), half_rows

    def return_copy(k, peer):
        a, start, size = piece_of(k)
        return remote(
            returns.at[a, pl.ds(peer * rows + start, size)],
            back.at[a, start : start + size, own_columns],
            back_send.at[k, peer],
            back_recv.at[k, mine],
            {"seq": peer},
        )

    def send_back(k, i):
        a, start, size = piece_of(k)
        for peer in range(i * tile // rows, (i + 1) * tile // rows):

            @pl.when(peer != mine)
            def _():
                return_copy(k, peer).start()

            @pl.when(peer == mine)
            def _():
                first = peer * rows + start
                back[a, start : start + size, own_columns] = returns[a, first : first + size, :]

    def sent_back(k):
        for peer in range(seq_size):

            @pl.when(peer != mine)
            def _():
                return_copy(k, peer).wait_send()

    def cut_of(i):
        return slice(i * tile, (i + 1) * tile)

    def score_cut(i, j):
        return cut_of(i * (i + 1) // 2 + j)

    for j in range(blocks):
        key_turned[:, cut_of(j)] = heads[1, cut_of(j), :].astype(WIDE).T.astype(LOW)
        value_turned[:, cut_of(j)] = heads[2, cut_of(j), :].astype(WIDE).T.astype(LOW)

    def attend(i):
        peak = jnp.full((1, tile), NEG, WIDE)
        for j in range(i + 1):
            score = dot_last(heads[1, cut_of(j), :], heads[0, cut_of(i), :]) * scale
            bias = key_bias[cut_of(j), :]
            score += jnp.concatenate([bias] * (tile // bias.shape[1]), 1)
            if i == j:
                key = lax.broadcasted_iota(jnp.int32, (tile, tile), 0)
                query = lax.broadcasted_iota(jnp.int32, (tile, tile), 1)
                score = jnp.where(key <= query, score, NEG)
            scores[score_cut(i, j), :] = score
            peak = jnp.maximum(peak, jnp.max(score, 0, keepdims=True))
        total = jnp.zeros((1, tile), WIDE)
        mixed = jnp.zeros((HEAD_DIM, tile), WIDE)
        for j in range(i + 1):
            expo = jnp.exp(scores[score_cut(i, j), :] - peak)
            scores[score_cut(i, j), :] = expo
            total += jnp.sum(expo, 0, keepdims=True)
            mixed += dot(value_turned[:, cut_of(j)], expo.astype(LOW))
        share_row[:, cut_of(i)] = 1.0 / total
        attn = (mixed / total).astype(LOW).astype(WIDE)
        attn_turned[:, cut_of(i)] = attn
        returns[0, cut_of(i), :] = attn.T.astype(LOW)

    def attend_back(i):
        grad = heads[3, cut_of(i), :]
        delta = jnp.sum(grad.astype(WIDE).T * attn_turned[:, cut_of(i)], 0, keepdims=True)
        share = share_row[:, cut_of(i)]
        query_sum = jnp.zeros((HEAD_DIM, tile), WIDE)
        for j in range(i + 1):
            d_probs = dot_last(heads[2, cut_of(j), :], grad)
            probs = scores[score_cut(i, j), :] * share
            d_scores = (probs * (d_probs - delta)).astype(LOW)
            value_part = dot(probs.astype(LOW), grad)
            key_part = dot(d_scores, heads[0, cut_of(i), :])
            query_sum += dot(key_turned[:, cut_of(j)], d_scores)
            if i < blocks - 1:
                value_part += value_sum[cut_of(j), :]
                key_part += key_sum[cut_of(j), :]
            if i == j:
                returns[2, cut_of(j), :] = value_part.astype(LOW)
                returns[3, cut_of(j), :] = (key_part * scale).astype(LOW)
            else:
                value_sum[cut_of(j), :] = value_part
                key_sum[cut_of(j), :] = key_part
        returns[1, cut_of(i), :] = (query_sum * scale).T.astype(LOW)

    ends = [0] + list(reversed(range(1, blocks)))
    for i in ends:
        attend(i)
        send_back(0, i)
    heads_arrived(6)
    for i in reversed(range(blocks)):
        attend_back(i)
        send_back(1, i)
    sent_back(0)
    for i in reversed(range(blocks)):
        send_back(2, i)

    def returns_arrived(k):
        a, start, size = piece_of(k)
        for step in range(1, seq_size):
            source = lax.rem(mine + step, seq_size)
            place = back.at[a, start : start + size, tile_of(source, HEAD_DIM)]
            remote(
                place, place, back_send.at[k, source], back_recv.at[k, source], {"seq": source}
            ).wait_recv()

    order = (
        (1 - chip) * 2 + (1 - core),
        (1 - chip) * 2 + core,
        chip * 2 + (1 - core),
        chip * 2 + core,
    )
    stages = ((0, slice(0, rows)), (1, slice(0, half_rows)), (1, slice(half_rows, rows)))

    def pair_copy(stage, k):
        a, part = stages[stage]
        return remote(
            partial.at[a, order[2 * k], part],
            pair_in.at[a, k, part],
            pair_send.at[stage, k],
            pair_recv.at[stage, k],
            {"tp": partner},
        )

    def cross_copy(stage):
        a, part = stages[stage]
        return remote(
            cross_out.at[a, part],
            cross_in.at[a, part],
            cross_send.at[stage],
            cross_recv.at[stage],
            {"tp": across},
        )

    def cross_over(stage):
        a, part = stages[stage]
        pair_copy(stage, 0).wait_recv()
        cross_out[a, part] = (
            partial[a, order[1], part].astype(WIDE) + pair_in[a, 0, part].astype(WIDE)
        ).astype(LOW)
        cross_copy(stage).start()

    def summed(stage):
        a, part = stages[stage]
        pair_copy(stage, 1).wait_recv()
        cross_copy(stage).wait_recv()
        return (
            partial[a, t, part].astype(WIDE)
            + pair_in[a, 1, part].astype(WIDE)
            + cross_in[a, part].astype(WIDE)
        )

    returns_arrived(0)
    for k in range(tp_size):
        quarter = order[k]

        def value_step(j, carry):
            at = tile_of(quarter * tiles + j, tile)
            partial[0, quarter, :, tile_of(j, tile)] = dot(back[0], w_out[:, at]).astype(LOW)
            return carry

        lax.fori_loop(0, tiles, value_step, 0, unroll=True)
        if k % 2 == 0:
            pair_copy(0, k // 2).start()
    cross_over(0)
    sent_back(1)
    for i in reversed(range(blocks)):
        send_back(3, i)

    weights = {1: w_query, 2: w_value, 3: w_key}

    def dots_copy(half, offset):
        return remote(
            dots_out.at[half],
            dots_in.at[half, offset],
            dots_send.at[half, offset],
            dots_recv.at[half, offset],
            {"tp": lax.rem(t + offset, tp_size)},
        )

    def share_gradient(half, product):
        stage = 1 + half
        part = stages[stage][1]
        dots = jnp.zeros((half_rows, 1), WIDE)
        for k in range(tp_size):
            quarter = order[k]
            for j in range(tiles):
                at = tile_of(quarter * tiles + j, tile)
                here = tile_of(j, tile)
                whole = product(quarter, at, here)
                partial[1, quarter, part, here] = whole.astype(LOW)
                inner = gain[:, at] * whole * wide[quarter, part, here].astype(WIDE)
                dots += jnp.sum(inner, 1, keepdims=True)
            if k % 2 == 0:
                pair_copy(stage, k // 2).start()
            if k == 2:
                cross_over(stage)
        dots_out[half] = jnp.broadcast_to(to_row(dots, rows), dots_out.shape[1:])
        for offset in range(1, tp_size):
            dots_copy(half, offset).start()
        return dots

    def finish_gradient(half, dots):
        stage = 1 + half
        part = stages[stage][1]
        for offset in range(1, tp_size):
            dots_copy(half, offset).wait_recv()
            dots += to_column(dots_in[half, offset, :1], half_rows)
        rinv = rinv_column[part, :]
        out_grad[part, :] = (
            wide_grad[t, part].astype(WIDE)
            + rinv * gain[:, tile_of(t, columns)] * summed(stage)
            - wide[t, part].astype(WIDE) * (rinv**3 * dots / model_width)
        )

    for a in (1, 2):
        returns_arrived(a)

        def quarter_step(quarter, carry):
            for j in range(tiles):
                at = tile_of(quarter * tiles + j, tile)
                here = tile_of(j, tile)
                more = dot_last(back[a], weights[a][at, :])
                if a == 1:
                    grad_sum[quarter, :, here] = more
                else:
                    grad_sum[quarter, :, here] += more
            return carry

        lax.fori_loop(0, tp_size, quarter_step, 0)
        if a == 1:
            sent_back(2)
            for i in reversed(range(blocks)):
                send_back(4, i)
    out_value[...] = jnp.where(
        row_valid > 0.5, wide[t].astype(WIDE) + summed(0), 0.0
    ).astype(LOW)

    def product_of(half):
        part = stages[1 + half][1]

        def product(quarter, at, here):
            return grad_sum[quarter, part, here] + dot_last(back[3, part], w_key[at, :])

        return product

    returns_arrived(3)
    upper_dots = share_gradient(0, product_of(0))
    returns_arrived(4)
    lower_dots = share_gradient(1, product_of(1))
    finish_gradient(0, upper_dots)
    finish_gradient(1, lower_dots)

    @pl.when(has_before)
    def _():
        lead_copy.wait_send()

    gather_drain(0, group_view)
    for p in range(grad_pieces):
        gather_drain(1 + p, grad_views[p])

    for batch in range(2):
        for j in range(2):
            gather_drain(wide_chunk(batch, j), wide_view(batch, j))
    for offset in range(1, seq_size):
        peer = lax.rem(mine + offset, seq_size)
        for k in range(7):
            head_copy(k, peer).wait_send()
    for k in (3, 4):
        sent_back(k)
    for stage in range(len(stages)):
        for k in range(2):
            pair_copy(stage, k).wait_send()
        cross_copy(stage).wait_send()
    for half in range(2):
        for offset in range(1, tp_size):
            dots_copy(half, offset).wait_send()


def per_device_whole(encoded, starts, w_up, norm_gain, w_query, w_key, w_value, w_out, cotangent):
    seq_size, tp_size = lax.axis_size("seq"), lax.axis_size("tp")
    rows, columns = cotangent.shape
    model_width = norm_gain.shape[0]
    byte_width = encoded.shape[1]
    cap = starts.shape[1]
    total = starts.size
    tile = 2 * HEAD_DIM
    chunks = 9
    blocks = total // tile
    dma = pltpu.SemaphoreType.DMA
    scratch = [
        pltpu.VMEM(starts.shape, jnp.int32),
        pltpu.VMEM((1, model_width), WIDE),
        pltpu.VMEM(encoded.shape, LOW),
        pltpu.VMEM(cotangent.shape, LOW),
        pltpu.VMEM(w_up.shape, LOW),
        pltpu.VMEM(w_query.shape, LOW),
        pltpu.VMEM(w_key.shape, LOW),
        pltpu.VMEM(w_value.shape, LOW),
        pltpu.VMEM(w_out.shape, LOW),
        pltpu.VMEM((1, byte_width), WIDE),
        pltpu.VMEM((1, byte_width), WIDE),
        pltpu.VMEM((rows, byte_width), LOW),
        pltpu.VMEM((tp_size, rows, columns), LOW),
        pltpu.VMEM((tp_size, rows, columns), LOW),
        pltpu.VMEM((tp_size, rows, columns), LOW),
        pltpu.VMEM((total, 1), WIDE),
        pltpu.VMEM((total, 128), WIDE),
        pltpu.VMEM((rows, 1), WIDE),
        pltpu.VMEM((4, seq_size, rows, HEAD_DIM), LOW),
        pltpu.VMEM((4, total, HEAD_DIM), LOW),
        pltpu.VMEM((HEAD_DIM, total), LOW),
        pltpu.VMEM((HEAD_DIM, total), LOW),
        pltpu.VMEM((blocks * (blocks + 1) // 2 * tile, tile), WIDE),
        pltpu.VMEM((HEAD_DIM, total), WIDE),
        pltpu.VMEM((1, total), WIDE),
        pltpu.VMEM((total, HEAD_DIM), WIDE),
        pltpu.VMEM((total, HEAD_DIM), WIDE),
        pltpu.VMEM((4, total, HEAD_DIM), LOW),
        pltpu.VMEM((4, rows, columns), LOW),
        pltpu.VMEM((tp_size, rows, columns), WIDE),
        pltpu.VMEM((2, tp_size, rows, columns), LOW),
        pltpu.VMEM((2, 2, rows, columns), LOW),
        pltpu.VMEM((2, rows, columns), LOW),
        pltpu.VMEM((2, rows, columns), LOW),
        pltpu.VMEM((2, 8, rows), WIDE),
        pltpu.VMEM((2, tp_size, 8, rows), WIDE),
        dma((5, 4)),
        dma((4,)),
        dma((2,)),
        dma((3, chunks)),
        dma((3, chunks)),
        dma((7, seq_size)),
        dma((7, seq_size)),
        dma((5, seq_size)),
        dma((5, seq_size)),
        dma((3, 2)),
        dma((3, 2)),
        dma((3,)),
        dma((3,)),
        dma((2, tp_size)),
        dma((2, tp_size)),
    ]
    near = pl.BlockSpec(memory_space=pltpu.VMEM)
    far = pl.BlockSpec(memory_space=pl.ANY)
    return tuple(
        pl.pallas_call(
            functools.partial(layer_kernel, seq_size, tp_size),
            out_shape=[
                jax.ShapeDtypeStruct((rows, columns), LOW),
                jax.ShapeDtypeStruct((rows, columns), WIDE),
            ],
            in_specs=[far] * 9,
            out_specs=[near] * 2,
            scratch_shapes=scratch,
            compiler_params=pltpu.CompilerParams(
                collective_id=0, has_side_effects=True, vmem_limit_bytes=67043328
            ),
        )(
            starts,
            norm_gain.reshape(1, model_width),
            encoded,
            cotangent,
            w_up,
            w_query,
            w_key,
            w_value,
            w_out,
        )
    )


def fits_one_kernel(arrays):
    encoded, starts, w_up, norm_gain, w_query, w_key, w_value, w_out, cotangent = arrays
    seq_size, tp_size = lax.axis_size("seq"), lax.axis_size("tp")
    rows, columns = cotangent.shape
    cap = starts.shape[1]
    return (
        tp_size == 4
        and seq_size % 2 == 0
        and columns == seq_size * HEAD_DIM
        and rows == HEAD_DIM
        and rows == tp_size * cap
        and cap & (cap - 1) == 0
        and cap % 16 == 0
        and columns % (4 * HEAD_DIM) == 0
        and norm_gain.shape[0] == tp_size * columns
        and starts.shape[0] == seq_size * tp_size
        and starts.size % (2 * HEAD_DIM) == 0
    )


def solution(mesh):
    in_specs = (
        P(("seq", "tp"), None),
        P(),
        P(None, "tp"),
        P(),
        P(None, "tp"),
        P(None, "tp"),
        P(None, "tp"),
        P("tp", None),
        P("seq", "tp"),
    )
    out_specs = (P("seq", "tp"), P("seq", "tp"))

    def choose(*arrays):
        return (per_device_whole if fits_one_kernel(arrays) else per_device)(*arrays)

    return jax.shard_map(
        choose, mesh=mesh, in_specs=in_specs, out_specs=out_specs, check_vma=False
    )
```

```python
import functools

import jax
import jax.numpy as jnp
from jax import lax
from jax.experimental import pallas as pl
from jax.experimental.pallas import tpu as pltpu
from jax.sharding import PartitionSpec as P

HEAD_DIM = 128


EPS = 1e-05
NEG = -1e30
CONTRACT_LAST = (((1,), (1,)), ((), ()))


def shifted(block, axis, distance):
    devices = range(lax.axis_size(axis))
    route = [(i - distance, i) for i in devices if i - distance in devices]
    return lax.ppermute(block, axis, route)


def per_device(encoded, starts, w_up, norm_gain, w_query, w_key, w_value, w_out, cotangent):
    byte_rows = encoded.shape[0]
    patch_cap = starts.shape[1]
    model_width = norm_gain.shape[0]
    shard = lax.axis_index(("seq", "tp"))
    own_starts = lax.dynamic_slice_in_dim(starts, shard, 1, 0)[0]
    places = jnp.arange(byte_rows, dtype=jnp.int32)
    following = jnp.concatenate([own_starts[1:], jnp.full((1,), byte_rows, jnp.int32)])
    inside = (places[None, :] >= own_starts[:, None]) & (places[None, :] < following[:, None])
    sums = jnp.dot(inside.astype(jnp.bfloat16), encoded, preferred_element_type=jnp.float32)
    sizes = jnp.sum(inside.astype(jnp.float32), 1)
    leading = places[None, :] < own_starts[:1, None]
    lead_sum = jnp.dot(leading.astype(jnp.bfloat16), encoded, preferred_element_type=jnp.float32)
    lead_size = jnp.sum(leading.astype(jnp.float32), 1)
    next_sum, next_size = shifted((lead_sum, lead_size), ("seq", "tp"), -1)
    count = jnp.sum((own_starts < byte_rows).astype(jnp.int32))
    last_slot = (jnp.arange(patch_cap, dtype=jnp.int32) == count - 1).astype(jnp.float32)
    sums = sums + last_slot[:, None] * next_sum
    sizes = sizes + last_slot * next_size
    patches = (sums / jnp.maximum(sizes, 1.0)[:, None]).astype(jnp.bfloat16)
    group = lax.all_gather(patches, "tp", axis=0, tiled=True)
    latent_in = jnp.dot(group, w_up, preferred_element_type=jnp.float32).astype(jnp.bfloat16)
    group_rows, columns = latent_in.shape
    head_count = columns // HEAD_DIM
    wide_piece = lax.all_gather(latent_in, "tp", axis=1, tiled=True).astype(jnp.float32)
    scaled = (wide_piece * norm_gain[None, :]).astype(jnp.bfloat16)
    acc_query = jnp.dot(scaled, w_query, preferred_element_type=jnp.float32)
    acc_key = jnp.dot(scaled, w_key, preferred_element_type=jnp.float32)
    acc_value = jnp.dot(scaled, w_value, preferred_element_type=jnp.float32)
    acc_query, acc_key, acc_value, square = (
        acc_query,
        acc_key,
        acc_value,
        jnp.sum(wide_piece * wide_piece, 1),
    )
    rinv = lax.rsqrt(square / model_width + EPS)
    query = (rinv[:, None] * acc_query).astype(jnp.bfloat16)
    key_rows = (rinv[:, None] * acc_key).astype(jnp.bfloat16)
    value_rows = (rinv[:, None] * acc_value).astype(jnp.bfloat16)
    keys_all, values_all = (
        lax.all_gather(key_rows, "seq", axis=0, tiled=True),
        lax.all_gather(value_rows, "seq", axis=0, tiled=True),
    )
    patches_total = keys_all.shape[0]
    valid_all = (starts < byte_rows).reshape(patches_total)
    row_base = lax.axis_index("seq") * group_rows
    query_index = row_base + jnp.arange(group_rows, dtype=jnp.int32)
    key_index = jnp.arange(patches_total, dtype=jnp.int32)
    query_valid = lax.dynamic_slice_in_dim(valid_all, row_base, group_rows, 0)
    allowed = valid_all[None, :] & (key_index[None, :] <= query_index[:, None])
    scale = HEAD_DIM ** (-0.5)
    query_heads = query.reshape(group_rows, head_count, HEAD_DIM)
    key_heads = keys_all.reshape(patches_total, head_count, HEAD_DIM)
    value_heads = values_all.reshape(patches_total, head_count, HEAD_DIM)
    scores = (
        jnp.einsum("rhd,khd->hrk", query_heads, key_heads, preferred_element_type=jnp.float32)
        * scale
    )
    peak = jnp.max(jnp.where(allowed[None], scores, NEG), 2)
    expo = jnp.where(allowed[None], jnp.exp(scores - peak[:, :, None]), 0.0)
    total = jnp.sum(expo, 2)
    mixed = jnp.einsum(
        "hrk,khd->rhd", expo.astype(jnp.bfloat16), value_heads, preferred_element_type=jnp.float32
    )
    attn = (mixed / total.T[:, :, None]).astype(jnp.bfloat16)
    partial_value = jnp.dot(
        attn.reshape(group_rows, columns), w_out, preferred_element_type=jnp.float32
    )
    head_sum = lax.psum_scatter(
        partial_value.astype(jnp.bfloat16), "tp", scatter_dimension=1, tiled=True
    ).astype(jnp.float32)
    wide_in = latent_in.astype(jnp.float32)
    latent_out = jnp.where(query_valid[:, None], wide_in + head_sum, 0.0).astype(jnp.bfloat16)
    grad_out = jnp.where(query_valid[:, None], cotangent, jnp.zeros_like(cotangent))
    d_attn = lax.dot_general(
        lax.all_gather(grad_out, "tp", axis=1, tiled=True),
        w_out,
        CONTRACT_LAST,
        preferred_element_type=jnp.float32,
    ).astype(jnp.bfloat16)
    grad_heads = d_attn.reshape(group_rows, head_count, HEAD_DIM)
    delta = jnp.sum(grad_heads.astype(jnp.float32) * attn.astype(jnp.float32), 2).T
    probs = expo / total[:, :, None]
    d_probs = jnp.einsum(
        "rhd,khd->hrk", grad_heads, value_heads, preferred_element_type=jnp.float32
    )
    d_scores = (probs * (d_probs - delta[:, :, None])).astype(jnp.bfloat16)
    grad_query = (
        (
            jnp.einsum("hrk,khd->rhd", d_scores, key_heads, preferred_element_type=jnp.float32)
            * scale
        )
        .astype(jnp.bfloat16)
        .reshape(group_rows, columns)
    )
    weights_low = probs.astype(jnp.bfloat16)
    count_rows = group_rows * lax.axis_size("seq")
    key_part = jnp.einsum("hrk,rhd->khd", d_scores, query_heads, preferred_element_type=jnp.float32)
    value_part = jnp.einsum(
        "hrk,rhd->khd", weights_low, grad_heads, preferred_element_type=jnp.float32
    )
    both = lax.psum_scatter(
        jnp.concatenate(
            [key_part.reshape(count_rows, columns), value_part.reshape(count_rows, columns)], 1
        ).astype(jnp.bfloat16),
        "seq",
        scatter_dimension=0,
        tiled=True,
    ).astype(jnp.float32)
    grad_key = (both[:, :columns] * scale).astype(jnp.bfloat16)
    grad_value = both[:, columns:].astype(jnp.bfloat16)
    dnormed = (
        lax.dot_general(grad_query, w_query, CONTRACT_LAST, preferred_element_type=jnp.float32)
        + lax.dot_general(grad_key, w_key, CONTRACT_LAST, preferred_element_type=jnp.float32)
        + lax.dot_general(grad_value, w_value, CONTRACT_LAST, preferred_element_type=jnp.float32)
    )
    normed_grad = lax.psum_scatter(
        dnormed.astype(jnp.bfloat16), "tp", scatter_dimension=1, tiled=True
    ).astype(jnp.float32)
    gain_own = lax.dynamic_slice_in_dim(norm_gain, lax.axis_index("tp") * columns, columns, 0)
    dots = lax.psum(jnp.sum(gain_own[None, :] * normed_grad * wide_in, 1), "tp")
    latent_grad = (
        grad_out.astype(jnp.float32)
        + rinv[:, None] * gain_own[None, :] * normed_grad
        - wide_in * (rinv**3)[:, None] * dots[:, None] / model_width
    )
    return (latent_out, latent_grad)


MESH = pl.DeviceIdType.MESH
LOW = jnp.bfloat16
WIDE = jnp.float32
ROWS_FIRST = (((0,), (0,)), ((), ()))


def tile_of(index, size):
    return pl.ds(pl.multiple_of(index * size, size), size)


def dot(a, b):
    return jnp.dot(a, b, preferred_element_type=WIDE)


def dot_last(a, b):
    return lax.dot_general(a, b, CONTRACT_LAST, preferred_element_type=WIDE)


def to_row(column, lanes):
    n = column.shape[0]
    down = lax.broadcasted_iota(jnp.int32, (n, lanes), 0)
    across = lax.broadcasted_iota(jnp.int32, (n, lanes), 1)
    return jnp.sum(jnp.where(down == across, column, 0.0), 0, keepdims=True)


def to_column(row, n, shift=0):
    lanes = row.shape[1]
    down = lax.broadcasted_iota(jnp.int32, (n, lanes), 0)
    across = lax.broadcasted_iota(jnp.int32, (n, lanes), 1)
    return jnp.sum(jnp.where(down + shift == across, row, 0.0), 1, keepdims=True)


def layer_kernel(
    seq_size,
    tp_size,
    starts_far,
    gain_far,
    encoded_far,
    cotangent_far,
    w_up_far,
    w_query_far,
    w_key_far,
    w_value_far,
    w_out_far,
    out_value,
    out_grad,
    starts,
    gain,
    encoded,
    cotangent,
    w_up,
    w_query,
    w_key,
    w_value,
    w_out,
    lead_out,
    lead_in,
    group,
    wide,
    wide_grad,
    scaled,
    valid_column,
    key_bias,
    rinv_column,
    outbox,
    heads,
    value_turned,
    key_turned,
    scores,
    attn_turned,
    share_row,
    key_sum,
    value_sum,
    returns,
    back,
    grad_sum,
    partial,
    pair_in,
    cross_out,
    cross_in,
    dots_out,
    dots_in,
    weight_sem,
    near_sem,
    lead_sem,
    gather_send,
    gather_recv,
    out_send,
    out_recv,
    back_send,
    back_recv,
    pair_send,
    pair_recv,
    cross_send,
    cross_recv,
    dots_send,
    dots_recv,
):
    byte_rows, byte_width = encoded.shape
    shards, cap = starts.shape
    rows, columns = cotangent.shape
    model_width = gain.shape[1]
    patches_total = shards * cap
    mine = lax.axis_index("seq")
    t = lax.axis_index("tp")
    chip, core = t // 2, lax.rem(t, 2)
    shard = mine * tp_size + t
    partner = t + 1 - 2 * core
    across = lax.rem(t + 2, tp_size)
    diagonal = lax.rem(partner + 2, tp_size)
    tile = 2 * HEAD_DIM
    tiles = columns // tile
    scale = HEAD_DIM ** (-0.5)

    def remote(src, dst, send, recv, device):
        return pltpu.make_async_remote_copy(
            src_ref=src,
            dst_ref=dst,
            send_sem=send,
            recv_sem=recv,
            device_id=device,
            device_id_type=MESH,
        )

    barrier = pltpu.get_barrier_semaphore()
    for offset in range(1, tp_size):
        pl.semaphore_signal(
            barrier, inc=1, device_id={"tp": lax.rem(t + offset, tp_size)}, device_id_type=MESH
        )
    for offset in range(1, seq_size):
        pl.semaphore_signal(
            barrier, inc=1, device_id={"seq": lax.rem(mine + offset, seq_size)}, device_id_type=MESH
        )
    has_before = shard > 0
    has_after = shard < shards - 1
    group_first = jnp.logical_and(t == 0, has_before)
    group_last = jnp.logical_and(t == tp_size - 1, has_after)
    shard_before = {
        "seq": jnp.where(t == 0, lax.rem(mine + seq_size - 1, seq_size), mine),
        "tp": lax.rem(t + tp_size - 1, tp_size),
    }
    shard_after = {
        "seq": jnp.where(t == tp_size - 1, lax.rem(mine + 1, seq_size), mine),
        "tp": lax.rem(t + 1, tp_size),
    }

    @pl.when(group_first)
    def _():
        pl.semaphore_signal(barrier, inc=1, device_id=shard_before, device_id_type=MESH)

    @pl.when(group_last)
    def _():
        pl.semaphore_signal(barrier, inc=1, device_id=shard_after, device_id_type=MESH)

    near_copies = [
        pltpu.make_async_copy(starts_far, starts, near_sem.at[0]),
        pltpu.make_async_copy(encoded_far, encoded, near_sem.at[1]),
        pltpu.make_async_copy(cotangent_far, cotangent, near_sem.at[2]),
        pltpu.make_async_copy(gain_far, gain, near_sem.at[3]),
    ]
    for copy in near_copies:
        copy.start()
    pieces = 4

    def weight_copies(i, far, near):
        depth = far.shape[0] // pieces
        for p in range(pieces):
            part = pl.ds(p * depth, depth)
            pltpu.make_async_copy(far.at[part], near.at[part], weight_sem.at[i]).start()

    def weight_wait(i, far, near):
        pltpu.make_async_copy(far, near, weight_sem.at[i]).wait()

    near_copies[0].wait()
    limit = float(byte_rows)
    own = starts[pl.ds(shard, 1), :].astype(WIDE)
    after = starts[pl.ds(jnp.minimum(shard + 1, shards - 1), 1), :].astype(WIDE)
    first = to_column(own, cap)
    slot = lax.broadcasted_iota(jnp.int32, (cap, 1), 0)
    following = to_column(own, cap, 1) + jnp.where(slot == cap - 1, limit, 0.0)
    places = lax.broadcasted_iota(jnp.int32, (cap, byte_rows), 1).astype(WIDE)
    inside = jnp.where((places >= first) & (places < following), 1.0, 0.0).astype(LOW)
    lead_places = lax.broadcasted_iota(jnp.int32, (16, byte_rows), 1).astype(WIDE)
    leading = jnp.where(lead_places < own[:, :1], 1.0, 0.0).astype(LOW)
    near_copies[1].wait()
    weight_copies(0, w_up_far, w_up)
    lead_out[...] = dot(leading, encoded[...])[:1]
    sums = dot(inside, encoded[...])

    neighbours = group_first.astype(jnp.int32) + group_last.astype(jnp.int32)
    pl.semaphore_wait(barrier, tp_size + seq_size - 2 + neighbours)

    lead_copy = remote(lead_out, lead_in, lead_sem.at[0], lead_sem.at[1], shard_before)

    @pl.when(has_before)
    def _():
        lead_copy.start()

    def gather_copy(way, k, kind, piece):
        target = across if way == 0 else partner
        return remote(
            piece, piece, gather_send.at[kind], gather_recv.at[way, k], {"tp": target}
        )

    def gather_start(k, kind, view):
        gather_copy(0, k, kind, view(t)).start()
        gather_copy(1, k, kind, view(t)).start()

    def gather_relay(k, kind, view):
        gather_copy(0, k, kind, view(across)).wait_recv()
        gather_copy(2, k, kind, view(across)).start()

    def gather_finish(k, kind, view, ways=(1, 2)):
        for way in ways:
            gather_copy(way, k, kind, view(partner if way == 1 else diagonal)).wait_recv()

    grad_view = lambda q: wide_grad.at[q]
    group_view = lambda q: group.at[tile_of(q, cap)]
    half_rows = rows // 2
    wide_tile = columns // 2

    def wide_view(batch, j):
        def view(q):
            of_chip = q // 2
            place = of_chip if batch == 0 else 1 - of_chip
            return wide.at[
                q, tile_of(place, half_rows), j * wide_tile : (j + 1) * wide_tile
            ]

        return view

    def wide_chunk(batch, j):
        return 2 + 2 * batch + j

    @pl.when(has_after)
    def _():
        lead_copy.wait_recv()

    joined = jnp.where(
        jnp.logical_and(first < limit, following >= limit), jnp.where(has_after, 1.0, 0.0), 0.0
    )
    sums = sums + joined * jnp.where(has_after, lead_in[...], 0.0)
    sizes = (following - first) * jnp.where(first < limit, 1.0, 0.0) + joined * after[:, :1]
    group[tile_of(t, cap), :] = (sums / jnp.maximum(sizes, 1.0)).astype(LOW)
    gather_start(0, 0, group_view)
    weight_copies(1, w_key_far, w_key)
    weight_copies(2, w_query_far, w_query)
    weight_copies(3, w_value_far, w_value)
    weight_copies(4, w_out_far, w_out)

    index = lax.broadcasted_iota(jnp.int32, (patches_total, shards), 0)
    lane = lax.broadcasted_iota(jnp.int32, (patches_total, shards), 1)
    owner = jnp.where((index >= lane * cap) & (index < lane * cap + cap), 1.0, 0.0).astype(LOW)
    valid = jnp.where(starts[...].astype(WIDE) < limit, 1.0, 0.0).astype(LOW)
    spread = dot(owner, valid)
    slots = lax.broadcasted_iota(jnp.int32, (patches_total, cap), 1)
    places_in = lax.broadcasted_iota(jnp.int32, (patches_total, cap), 0)
    valid_column[...] = jnp.sum(
        jnp.where(jnp.bitwise_and(places_in, cap - 1) == slots, spread, 0.0), 1, keepdims=True
    )
    own_rows = tile_of(mine, rows)
    row_valid = valid_column[own_rows, :]
    key_bias[...] = jnp.broadcast_to((valid_column[...] - 1.0) * -NEG, key_bias.shape)
    near_copies[2].wait()
    wide_grad[t] = jnp.where(row_valid > 0.5, cotangent[...].astype(WIDE), 0.0).astype(LOW)

    def raise_rows(batch):
        place = tile_of(chip if batch == 0 else 1 - chip, half_rows)
        for j in range(2):
            cut = slice(j * wide_tile, (j + 1) * wide_tile)
            wide[t, place, cut] = dot(group[place, :], w_up[:, cut]).astype(LOW)
            gather_start(wide_chunk(batch, j), 2, wide_view(batch, j))

    gather_finish(0, 0, group_view, (1,))
    weight_wait(0, w_up_far, w_up)
    raise_rows(0)
    gather_relay(0, 0, group_view)
    gather_finish(0, 0, group_view, (2,))
    raise_rows(1)

    far_half = 1 - mine // (seq_size // 2)

    def head_copy(k, h):
        if k == 6:
            src, place = outbox.at[3, h], own_rows
        else:
            a, batch = k // 2, k % 2
            piece = 1 - chip if batch == 0 else chip
            src = outbox.at[a, h, tile_of(piece, half_rows)]
            place = tile_of(2 * mine + piece, half_rows)
        return remote(
            src,
            heads.at[3 if k == 6 else k // 2, place],
            out_send.at[k],
            out_recv.at[k],
            {"seq": h},
        )

    def start_head(k, h):
        @pl.when(h != mine)
        def _():
            head_copy(k, h).start()

    def keep_heads(a, h_first, block, start, size):
        for u in range(block.shape[1] // HEAD_DIM):
            h = h_first + u
            part = block[:, u * HEAD_DIM : (u + 1) * HEAD_DIM]

            @pl.when(h == mine)
            def _():
                heads[a, pl.ds(pl.multiple_of(mine * rows + start, size), size), :] = part

            @pl.when(h != mine)
            def _():
                outbox[a, h, pl.ds(pl.multiple_of(start, size), size), :] = part

    def tile_order(jj):
        return lax.rem(far_half * (tiles // 2) + jj, tiles)

    def relay_rows(batch):
        for j in range(2):
            gather_relay(wide_chunk(batch, j), 2, wide_view(batch, j))

    def norm_rows(batch):
        place = tile_of(1 - chip if batch == 0 else chip, half_rows)

        def norm_step(q, square):
            piece = wide[q, place].astype(WIDE)
            scaled[q, place] = (piece * gain[:, tile_of(q, columns)]).astype(LOW)
            return square + jnp.sum(piece * piece, 1, keepdims=True)

        square = lax.fori_loop(0, tp_size, norm_step, jnp.zeros((half_rows, 1), WIDE))
        rinv_column[place, :] = lax.rsqrt(square / model_width + EPS)

    def project(a, weight, batch, width):
        piece = 1 - chip if batch == 0 else chip
        place = tile_of(piece, half_rows)
        steps = columns // width
        held = width // HEAD_DIM

        def step(jj, carry):
            j = lax.rem(far_half * (steps // 2) + jj, steps)
            acc = jnp.zeros((half_rows, width), WIDE)
            for q in range(tp_size):
                acc += dot(
                    scaled[q, place], weight[q * columns : (q + 1) * columns, tile_of(j, width)]
                )
            block = (rinv_column[place, :] * acc).astype(LOW)
            keep_heads(a, j * held, block, piece * half_rows, half_rows)
            for u in range(held):
                start_head(2 * a + batch, j * held + u)
            return carry

        lax.fori_loop(0, steps, step, 0)

    near_copies[3].wait()
    relay_rows(0)
    for j in range(2):
        gather_finish(wide_chunk(0, j), 2, wide_view(0, j), (2,))
        gather_finish(wide_chunk(1, j), 2, wide_view(1, j), (1,))
    norm_rows(0)
    weight_wait(1, w_key_far, w_key)
    project(1, w_key, 0, tile)
    relay_rows(1)
    gather_start(1, 1, grad_view)
    weight_wait(2, w_query_far, w_query)
    project(0, w_query, 0, wide_tile)
    weight_wait(3, w_value_far, w_value)
    project(2, w_value, 0, wide_tile)
    for j in range(2):
        gather_finish(wide_chunk(0, j), 2, wide_view(0, j), (1,))
        gather_finish(wide_chunk(1, j), 2, wide_view(1, j), (2,))
    norm_rows(1)
    project(1, w_key, 1, wide_tile)
    project(0, w_query, 1, wide_tile)
    gather_relay(1, 1, grad_view)
    project(2, w_value, 1, wide_tile)
    weight_wait(4, w_out_far, w_out)
    gather_finish(1, 1, grad_view)

    def d_attn_step(jj, carry):
        j = tile_order(jj)
        acc = jnp.zeros((rows, tile), WIDE)
        for q in range(tp_size):
            acc += dot_last(
                wide_grad[q], w_out[tile_of(j, tile), q * columns : (q + 1) * columns]
            )
        keep_heads(3, 2 * j, acc.astype(LOW), 0, rows)
        for u in range(2):
            start_head(6, 2 * j + u)
        return carry

    lax.fori_loop(0, tiles, d_attn_step, 0)


    def heads_arrived(k):
        size = (rows if k == 6 else half_rows) * (seq_size - 1)
        place = heads.at[3 if k == 6 else k // 2, :size]
        remote(place, place, out_send.at[k], out_recv.at[k], {"seq": mine}).wait_recv()

    def turn_square(q, carry):
        steps = columns // tile
        for i in range(steps):
            for j in range(i, steps):
                upper = w_key.at[tile_of(q * steps + i, tile), j * tile : (j + 1) * tile]
                lower = w_key.at[tile_of(q * steps + j, tile), i * tile : (i + 1) * tile]
                turned = upper[...].T
                if i != j:
                    upper[...] = lower[...].T
                lower[...] = turned
        return carry

    lax.fori_loop(0, tp_size, turn_square, 0)
    for k in range(4):
        heads_arrived(k)

    blocks = patches_total // tile
    own_columns = tile_of(mine, HEAD_DIM)

    def piece_of(k):
        if k < 3:
            return k, 0, rows
        return 3, half_rows * (k - 3), half_rows

    half_seq = seq_size // 2
    near_half = mine // half_seq

    def return_copy(k, peer):
        a, start, size = piece_of(k)
        return remote(
            returns.at[a, pl.ds(peer * rows + start, size)],
            back.at[a, start : start + size, own_columns],
            back_send.at[k],
            back_recv.at[k, jnp.where(peer // half_seq == near_half, 0, 1)],
            {"seq": peer},
        )

    def send_back(k, i):
        a, start, size = piece_of(k)
        for peer in range(i * tile // rows, (i + 1) * tile // rows):

            @pl.when(peer != mine)
            def _():
                return_copy(k, peer).start()

            @pl.when(peer == mine)
            def _():
                first = peer * rows + start
                back[a, start : start + size, own_columns] = returns[a, first : first + size, :]

    def sent_back(k):
        a, start, size = piece_of(k)
        sent = returns.at[a, : size * (seq_size - 1)]
        remote(sent, sent, back_send.at[k], back_recv.at[k, 0], {"seq": mine}).wait_send()

    def cut_of(i):
        return slice(i * tile, (i + 1) * tile)

    def score_cut(i, j):
        return cut_of(i * (i + 1) // 2 + j)

    for j in range(blocks):
        key_turned[:, cut_of(j)] = heads[1, cut_of(j), :].astype(WIDE).T.astype(LOW)

    def attend(i):
        peak = jnp.full((1, tile), NEG, WIDE)
        for j in range(i + 1):
            score = dot_last(heads[1, cut_of(j), :], heads[0, cut_of(i), :]) * scale
            bias = key_bias[cut_of(j), :]
            score += jnp.concatenate([bias] * (tile // bias.shape[1]), 1)
            if i == j:
                key = lax.broadcasted_iota(jnp.int32, (tile, tile), 0)
                query = lax.broadcasted_iota(jnp.int32, (tile, tile), 1)
                score = jnp.where(key <= query, score, NEG)
            scores[score_cut(i, j), :] = score
            peak = jnp.maximum(peak, jnp.max(score, 0, keepdims=True))
        total = jnp.zeros((1, tile), WIDE)
        for j in range(i + 1):
            expo = jnp.exp(scores[score_cut(i, j), :] - peak)
            scores[score_cut(i, j), :] = expo
            total += jnp.sum(expo, 0, keepdims=True)
        share_row[:, cut_of(i)] = 1.0 / total

    def mix(i):
        mixed = jnp.zeros((HEAD_DIM, tile), WIDE)
        for j in range(i + 1):
            mixed += dot(value_turned[:, cut_of(j)], scores[score_cut(i, j), :].astype(LOW))
        attn = (mixed * share_row[:, cut_of(i)]).astype(LOW).astype(WIDE)
        attn_turned[:, cut_of(i)] = attn
        returns[0, cut_of(i), :] = attn.T.astype(LOW)

    def attend_back(i):
        grad = heads[3, cut_of(i), :]
        delta = jnp.sum(grad.astype(WIDE).T * attn_turned[:, cut_of(i)], 0, keepdims=True)
        share = share_row[:, cut_of(i)]
        query_sum = jnp.zeros((HEAD_DIM, tile), WIDE)
        for j in range(i + 1):
            d_probs = dot_last(heads[2, cut_of(j), :], grad)
            probs = scores[score_cut(i, j), :] * share
            d_scores = (probs * (d_probs - delta)).astype(LOW)
            value_part = dot(probs.astype(LOW), grad)
            key_part = dot(d_scores, heads[0, cut_of(i), :])
            query_sum += dot(key_turned[:, cut_of(j)], d_scores)
            if i < blocks - 1:
                value_part += value_sum[cut_of(j), :]
                key_part += key_sum[cut_of(j), :]
            if i == j:
                returns[2, cut_of(j), :] = value_part.astype(LOW)
                returns[3, cut_of(j), :] = (key_part * scale).astype(LOW)
            else:
                value_sum[cut_of(j), :] = value_part
                key_sum[cut_of(j), :] = key_part
        returns[1, cut_of(i), :] = (query_sum * scale).T.astype(LOW)

    ends = [0] + list(reversed(range(1, blocks)))
    for i in range(blocks):
        attend(i)
    for k in (4, 5):
        heads_arrived(k)
    for j in range(blocks):
        value_turned[:, cut_of(j)] = heads[2, cut_of(j), :].astype(WIDE).T.astype(LOW)
    for i in ends:
        mix(i)
        send_back(0, i)
    heads_arrived(6)
    for i in reversed(range(blocks)):
        attend_back(i)
        send_back(1, i)
    sent_back(0)
    for i in reversed(range(blocks)):
        send_back(2, i)

    def returns_arrived(k, sides=(0, 1)):
        a, start, size = piece_of(k)
        for side in sides:
            place = returns.at[a, : size * (half_seq - 1 + side)]
            remote(
                place, place, back_send.at[k], back_recv.at[k, side], {"seq": mine}
            ).wait_recv()

    order = (
        (1 - chip) * 2 + (1 - core),
        (1 - chip) * 2 + core,
        chip * 2 + (1 - core),
        chip * 2 + core,
    )
    stages = ((0, slice(0, rows)), (1, slice(0, half_rows)), (1, slice(half_rows, rows)))

    def pair_copy(stage, k):
        a, part = stages[stage]
        return remote(
            partial.at[a, order[2 * k], part],
            pair_in.at[a, k, part],
            pair_send.at[stage],
            pair_recv.at[stage, k],
            {"tp": partner},
        )

    def cross_copy(stage):
        a, part = stages[stage]
        return remote(
            cross_out.at[a, part],
            cross_in.at[a, part],
            cross_send.at[stage],
            cross_recv.at[stage],
            {"tp": across},
        )

    def cross_over(stage):
        a, part = stages[stage]
        pair_copy(stage, 0).wait_recv()
        cross_out[a, part] = (
            partial[a, order[1], part].astype(WIDE) + pair_in[a, 0, part].astype(WIDE)
        ).astype(LOW)
        cross_copy(stage).start()

    def summed(stage):
        a, part = stages[stage]
        pair_copy(stage, 1).wait_recv()
        cross_copy(stage).wait_recv()
        return (
            partial[a, t, part].astype(WIDE)
            + pair_in[a, 1, part].astype(WIDE)
            + cross_in[a, part].astype(WIDE)
        )

    returns_arrived(0)
    for k in range(tp_size):
        quarter = order[k]

        for j in range(2):
            at = tile_of(quarter * 2 + j, wide_tile)
            here = slice(j * wide_tile, (j + 1) * wide_tile)
            partial[0, quarter, :, here] = dot(back[0], w_out[:, at]).astype(LOW)
        if k % 2 == 0:
            pair_copy(0, k // 2).start()
    weights = {1: w_query, 2: w_value, 3: w_key}

    def dots_copy(half, offset):
        return remote(
            dots_out.at[half],
            dots_in.at[half, offset],
            dots_send.at[half],
            dots_recv.at[half],
            {"tp": lax.rem(t + offset, tp_size)},
        )

    def share_gradient(half, product):
        stage = 1 + half
        part = stages[stage][1]
        dots = jnp.zeros((half_rows, 1), WIDE)
        for k in range(tp_size):
            quarter = order[k]
            for j in range(2):
                at = tile_of(quarter * 2 + j, wide_tile)
                here = slice(j * wide_tile, (j + 1) * wide_tile)
                whole = product(quarter, here)
                partial[1, quarter, part, here] = whole.astype(LOW)
                inner = gain[:, at] * whole * wide[quarter, part, here].astype(WIDE)
                dots += jnp.sum(inner, 1, keepdims=True)
            if k % 2 == 0:
                pair_copy(stage, k // 2).start()
            if k == 2:
                cross_over(stage)
        dots_out[half] = jnp.broadcast_to(to_row(dots, rows), dots_out.shape[1:])
        for offset in range(1, tp_size):
            dots_copy(half, offset).start()
        return dots

    def finish_gradient(half, dots):
        stage = 1 + half
        part = stages[stage][1]
        place = dots_in.at[half, 1:]
        remote(place, place, dots_send.at[half], dots_recv.at[half], {"tp": t}).wait_recv()
        for offset in range(1, tp_size):
            dots += to_column(dots_in[half, offset, :1], half_rows)
        rinv = rinv_column[part, :]
        out_grad[part, :] = (
            wide_grad[t, part].astype(WIDE)
            + rinv * gain[:, tile_of(t, columns)] * summed(stage)
            - wide[t, part].astype(WIDE) * (rinv**3 * dots / model_width)
        )

    half_columns = columns // 2
    for a, side in ((1, 0), (1, 1), (2, 0), (2, 1)):
        returns_arrived(a, (side,))
        sources = tile_of(near_half if side == 0 else 1 - near_half, half_columns)

        def quarter_step(quarter, carry):
            for j in range(tiles):
                at = tile_of(quarter * tiles + j, tile)
                here = tile_of(j, tile)
                more = dot_last(back[a, :, sources], weights[a][at, sources])
                if a == 1 and side == 0:
                    grad_sum[quarter, :, here] = more
                else:
                    grad_sum[quarter, :, here] += more
            return carry

        lax.fori_loop(0, tp_size, quarter_step, 0, unroll=2)
        if a == 1 and side == 0:
            sent_back(1)
            for i in reversed(range(blocks)):
                send_back(3, i)
            cross_over(0)
        if a == 1 and side == 1:
            sent_back(2)
            for i in reversed(range(blocks)):
                send_back(4, i)
    out_value[...] = jnp.where(
        row_valid > 0.5, wide[t].astype(WIDE) + summed(0), 0.0
    ).astype(LOW)

    def product_of(half):
        part = stages[1 + half][1]

        def product(quarter, here):
            turned = w_key[tile_of(quarter, columns), here]
            return grad_sum[quarter, part, here] + dot(back[3, part], turned)

        return product

    returns_arrived(3)
    upper_dots = share_gradient(0, product_of(0))
    returns_arrived(4)
    lower_dots = share_gradient(1, product_of(1))
    finish_gradient(0, upper_dots)
    finish_gradient(1, lower_dots)

    @pl.when(has_before)
    def _():
        lead_copy.wait_send()

    for kind, sent in ((0, group.at[: 3 * cap]), (1, wide_grad.at[:3]), (2, wide.at[:3])):
        gather_copy(0, 0, kind, sent).wait_send()
    for k in range(7):
        sent = outbox.at[3, 1:] if k == 6 else outbox.at[k // 2, 1:, :half_rows]
        remote(sent, sent, out_send.at[k], out_recv.at[k], {"seq": mine}).wait_send()
    for k in (3, 4):
        sent_back(k)
    for stage in range(len(stages)):
        a, part = stages[stage]
        sent = pair_in.at[a, :, part]
        remote(
            sent, sent, pair_send.at[stage], pair_recv.at[stage, 0], {"tp": partner}
        ).wait_send()
        cross_copy(stage).wait_send()
    for half in range(2):
        sent = dots_in.at[half, 1:]
        remote(sent, sent, dots_send.at[half], dots_recv.at[half], {"tp": t}).wait_send()


def per_device_whole(encoded, starts, w_up, norm_gain, w_query, w_key, w_value, w_out, cotangent):
    seq_size, tp_size = lax.axis_size("seq"), lax.axis_size("tp")
    rows, columns = cotangent.shape
    model_width = norm_gain.shape[0]
    byte_width = encoded.shape[1]
    cap = starts.shape[1]
    total = starts.size
    tile = 2 * HEAD_DIM
    blocks = total // tile
    dma = pltpu.SemaphoreType.DMA
    scratch = [
        pltpu.VMEM(starts.shape, jnp.int32),
        pltpu.VMEM((1, model_width), WIDE),
        pltpu.VMEM(encoded.shape, LOW),
        pltpu.VMEM(cotangent.shape, LOW),
        pltpu.VMEM(w_up.shape, LOW),
        pltpu.VMEM(w_query.shape, LOW),
        pltpu.VMEM(w_key.shape, LOW),
        pltpu.VMEM(w_value.shape, LOW),
        pltpu.VMEM(w_out.shape, LOW),
        pltpu.VMEM((1, byte_width), WIDE),
        pltpu.VMEM((1, byte_width), WIDE),
        pltpu.VMEM((rows, byte_width), LOW),
        pltpu.VMEM((tp_size, rows, columns), LOW),
        pltpu.VMEM((tp_size, rows, columns), LOW),
        pltpu.VMEM((tp_size, rows, columns), LOW),
        pltpu.VMEM((total, 1), WIDE),
        pltpu.VMEM((total, 128), WIDE),
        pltpu.VMEM((rows, 1), WIDE),
        pltpu.VMEM((4, seq_size, rows, HEAD_DIM), LOW),
        pltpu.VMEM((4, total, HEAD_DIM), LOW),
        pltpu.VMEM((HEAD_DIM, total), LOW),
        pltpu.VMEM((HEAD_DIM, total), LOW),
        pltpu.VMEM((blocks * (blocks + 1) // 2 * tile, tile), WIDE),
        pltpu.VMEM((HEAD_DIM, total), WIDE),
        pltpu.VMEM((1, total), WIDE),
        pltpu.VMEM((total, HEAD_DIM), WIDE),
        pltpu.VMEM((total, HEAD_DIM), WIDE),
        pltpu.VMEM((4, total, HEAD_DIM), LOW),
        pltpu.VMEM((4, rows, columns), LOW),
        pltpu.VMEM((tp_size, rows, columns), WIDE),
        pltpu.VMEM((2, tp_size, rows, columns), LOW),
        pltpu.VMEM((2, 2, rows, columns), LOW),
        pltpu.VMEM((2, rows, columns), LOW),
        pltpu.VMEM((2, rows, columns), LOW),
        pltpu.VMEM((2, 8, rows), WIDE),
        pltpu.VMEM((2, tp_size, 8, rows), WIDE),
        dma((5,)),
        dma((4,)),
        dma((2,)),
        dma((3,)),
        dma((3, 6)),
        dma((7,)),
        dma((7,)),
        dma((5,)),
        dma((5, 2)),
        dma((3,)),
        dma((3, 2)),
        dma((3,)),
        dma((3,)),
        dma((2,)),
        dma((2,)),
    ]
    near = pl.BlockSpec(memory_space=pltpu.VMEM)
    far = pl.BlockSpec(memory_space=pl.ANY)
    return tuple(
        pl.pallas_call(
            functools.partial(layer_kernel, seq_size, tp_size),
            out_shape=[
                pltpu.VMEM((rows, columns), LOW),
                pltpu.VMEM((rows, columns), WIDE),
            ],
            in_specs=[far] * 9,
            out_specs=[near] * 2,
            scratch_shapes=scratch,
            compiler_params=pltpu.CompilerParams(
                collective_id=0, has_side_effects=True, vmem_limit_bytes=60 * 1024 * 1024
            ),
        )(
            starts,
            norm_gain.reshape(1, model_width),
            encoded,
            cotangent,
            w_up,
            w_query,
            w_key,
            w_value,
            w_out,
        )
    )


def fits_one_kernel(arrays):
    encoded, starts, w_up, norm_gain, w_query, w_key, w_value, w_out, cotangent = arrays
    seq_size, tp_size = lax.axis_size("seq"), lax.axis_size("tp")
    rows, columns = cotangent.shape
    cap = starts.shape[1]
    return (
        tp_size == 4
        and seq_size % 2 == 0
        and columns == seq_size * HEAD_DIM
        and rows == HEAD_DIM
        and rows == tp_size * cap
        and cap & (cap - 1) == 0
        and cap % 16 == 0
        and columns % (4 * HEAD_DIM) == 0
        and norm_gain.shape[0] == tp_size * columns
        and starts.shape[0] == seq_size * tp_size
        and starts.size % (2 * HEAD_DIM) == 0
    )


def solution(mesh):
    in_specs = (
        P(("seq", "tp"), None),
        P(),
        P(None, "tp"),
        P(),
        P(None, "tp"),
        P(None, "tp"),
        P(None, "tp"),
        P("tp", None),
        P("seq", "tp"),
    )
    out_specs = (P("seq", "tp"), P("seq", "tp"))

    def choose(*arrays):
        return (per_device_whole if fits_one_kernel(arrays) else per_device)(*arrays)

    return jax.shard_map(
        choose, mesh=mesh, in_specs=in_specs, out_specs=out_specs, check_vma=False
    )
```

```python
import functools

import jax
import jax.numpy as jnp
from jax import lax
from jax.experimental import pallas as pl
from jax.experimental.pallas import tpu as pltpu
from jax.sharding import PartitionSpec as P

HEAD_DIM = 128


EPS = 1e-05
NEG = -1e30
CONTRACT_LAST = (((1,), (1,)), ((), ()))


def shifted(block, axis, distance):
    devices = range(lax.axis_size(axis))
    route = [(i - distance, i) for i in devices if i - distance in devices]
    return lax.ppermute(block, axis, route)


def per_device(encoded, starts, w_up, norm_gain, w_query, w_key, w_value, w_out, cotangent):
    byte_rows = encoded.shape[0]
    patch_cap = starts.shape[1]
    model_width = norm_gain.shape[0]
    shard = lax.axis_index(("seq", "tp"))
    own_starts = lax.dynamic_slice_in_dim(starts, shard, 1, 0)[0]
    places = jnp.arange(byte_rows, dtype=jnp.int32)
    following = jnp.concatenate([own_starts[1:], jnp.full((1,), byte_rows, jnp.int32)])
    inside = (places[None, :] >= own_starts[:, None]) & (places[None, :] < following[:, None])
    sums = jnp.dot(inside.astype(jnp.bfloat16), encoded, preferred_element_type=jnp.float32)
    sizes = jnp.sum(inside.astype(jnp.float32), 1)
    leading = places[None, :] < own_starts[:1, None]
    lead_sum = jnp.dot(leading.astype(jnp.bfloat16), encoded, preferred_element_type=jnp.float32)
    lead_size = jnp.sum(leading.astype(jnp.float32), 1)
    next_sum, next_size = shifted((lead_sum, lead_size), ("seq", "tp"), -1)
    count = jnp.sum((own_starts < byte_rows).astype(jnp.int32))
    last_slot = (jnp.arange(patch_cap, dtype=jnp.int32) == count - 1).astype(jnp.float32)
    sums = sums + last_slot[:, None] * next_sum
    sizes = sizes + last_slot * next_size
    patches = (sums / jnp.maximum(sizes, 1.0)[:, None]).astype(jnp.bfloat16)
    group = lax.all_gather(patches, "tp", axis=0, tiled=True)
    latent_in = jnp.dot(group, w_up, preferred_element_type=jnp.float32).astype(jnp.bfloat16)
    group_rows, columns = latent_in.shape
    head_count = columns // HEAD_DIM
    wide_piece = lax.all_gather(latent_in, "tp", axis=1, tiled=True).astype(jnp.float32)
    scaled = (wide_piece * norm_gain[None, :]).astype(jnp.bfloat16)
    acc_query = jnp.dot(scaled, w_query, preferred_element_type=jnp.float32)
    acc_key = jnp.dot(scaled, w_key, preferred_element_type=jnp.float32)
    acc_value = jnp.dot(scaled, w_value, preferred_element_type=jnp.float32)
    acc_query, acc_key, acc_value, square = (
        acc_query,
        acc_key,
        acc_value,
        jnp.sum(wide_piece * wide_piece, 1),
    )
    rinv = lax.rsqrt(square / model_width + EPS)
    query = (rinv[:, None] * acc_query).astype(jnp.bfloat16)
    key_rows = (rinv[:, None] * acc_key).astype(jnp.bfloat16)
    value_rows = (rinv[:, None] * acc_value).astype(jnp.bfloat16)
    keys_all, values_all = (
        lax.all_gather(key_rows, "seq", axis=0, tiled=True),
        lax.all_gather(value_rows, "seq", axis=0, tiled=True),
    )
    patches_total = keys_all.shape[0]
    valid_all = (starts < byte_rows).reshape(patches_total)
    row_base = lax.axis_index("seq") * group_rows
    query_index = row_base + jnp.arange(group_rows, dtype=jnp.int32)
    key_index = jnp.arange(patches_total, dtype=jnp.int32)
    query_valid = lax.dynamic_slice_in_dim(valid_all, row_base, group_rows, 0)
    allowed = valid_all[None, :] & (key_index[None, :] <= query_index[:, None])
    scale = HEAD_DIM ** (-0.5)
    query_heads = query.reshape(group_rows, head_count, HEAD_DIM)
    key_heads = keys_all.reshape(patches_total, head_count, HEAD_DIM)
    value_heads = values_all.reshape(patches_total, head_count, HEAD_DIM)
    scores = (
        jnp.einsum("rhd,khd->hrk", query_heads, key_heads, preferred_element_type=jnp.float32)
        * scale
    )
    peak = jnp.max(jnp.where(allowed[None], scores, NEG), 2)
    expo = jnp.where(allowed[None], jnp.exp(scores - peak[:, :, None]), 0.0)
    total = jnp.sum(expo, 2)
    mixed = jnp.einsum(
        "hrk,khd->rhd", expo.astype(jnp.bfloat16), value_heads, preferred_element_type=jnp.float32
    )
    attn = (mixed / total.T[:, :, None]).astype(jnp.bfloat16)
    partial_value = jnp.dot(
        attn.reshape(group_rows, columns), w_out, preferred_element_type=jnp.float32
    )
    head_sum = lax.psum_scatter(
        partial_value.astype(jnp.bfloat16), "tp", scatter_dimension=1, tiled=True
    ).astype(jnp.float32)
    wide_in = latent_in.astype(jnp.float32)
    latent_out = jnp.where(query_valid[:, None], wide_in + head_sum, 0.0).astype(jnp.bfloat16)
    grad_out = jnp.where(query_valid[:, None], cotangent, jnp.zeros_like(cotangent))
    d_attn = lax.dot_general(
        lax.all_gather(grad_out, "tp", axis=1, tiled=True),
        w_out,
        CONTRACT_LAST,
        preferred_element_type=jnp.float32,
    ).astype(jnp.bfloat16)
    grad_heads = d_attn.reshape(group_rows, head_count, HEAD_DIM)
    delta = jnp.sum(grad_heads.astype(jnp.float32) * attn.astype(jnp.float32), 2).T
    probs = expo / total[:, :, None]
    d_probs = jnp.einsum(
        "rhd,khd->hrk", grad_heads, value_heads, preferred_element_type=jnp.float32
    )
    d_scores = (probs * (d_probs - delta[:, :, None])).astype(jnp.bfloat16)
    grad_query = (
        (
            jnp.einsum("hrk,khd->rhd", d_scores, key_heads, preferred_element_type=jnp.float32)
            * scale
        )
        .astype(jnp.bfloat16)
        .reshape(group_rows, columns)
    )
    weights_low = probs.astype(jnp.bfloat16)
    count_rows = group_rows * lax.axis_size("seq")
    key_part = jnp.einsum("hrk,rhd->khd", d_scores, query_heads, preferred_element_type=jnp.float32)
    value_part = jnp.einsum(
        "hrk,rhd->khd", weights_low, grad_heads, preferred_element_type=jnp.float32
    )
    both = lax.psum_scatter(
        jnp.concatenate(
            [key_part.reshape(count_rows, columns), value_part.reshape(count_rows, columns)], 1
        ).astype(jnp.bfloat16),
        "seq",
        scatter_dimension=0,
        tiled=True,
    ).astype(jnp.float32)
    grad_key = (both[:, :columns] * scale).astype(jnp.bfloat16)
    grad_value = both[:, columns:].astype(jnp.bfloat16)
    dnormed = (
        lax.dot_general(grad_query, w_query, CONTRACT_LAST, preferred_element_type=jnp.float32)
        + lax.dot_general(grad_key, w_key, CONTRACT_LAST, preferred_element_type=jnp.float32)
        + lax.dot_general(grad_value, w_value, CONTRACT_LAST, preferred_element_type=jnp.float32)
    )
    normed_grad = lax.psum_scatter(
        dnormed.astype(jnp.bfloat16), "tp", scatter_dimension=1, tiled=True
    ).astype(jnp.float32)
    gain_own = lax.dynamic_slice_in_dim(norm_gain, lax.axis_index("tp") * columns, columns, 0)
    dots = lax.psum(jnp.sum(gain_own[None, :] * normed_grad * wide_in, 1), "tp")
    latent_grad = (
        grad_out.astype(jnp.float32)
        + rinv[:, None] * gain_own[None, :] * normed_grad
        - wide_in * (rinv**3)[:, None] * dots[:, None] / model_width
    )
    return (latent_out, latent_grad)


MESH = pl.DeviceIdType.MESH
LOW = jnp.bfloat16
WIDE = jnp.float32
ROWS_FIRST = (((0,), (0,)), ((), ()))


def tile_of(index, size):
    return pl.ds(pl.multiple_of(index * size, size), size)


def dot(a, b):
    return jnp.dot(a, b, preferred_element_type=WIDE)


def dot_last(a, b):
    return lax.dot_general(a, b, CONTRACT_LAST, preferred_element_type=WIDE)


def to_row(column, lanes):
    n = column.shape[0]
    down = lax.broadcasted_iota(jnp.int32, (n, lanes), 0)
    across = lax.broadcasted_iota(jnp.int32, (n, lanes), 1)
    return jnp.sum(jnp.where(down == across, column, 0.0), 0, keepdims=True)


def to_column(row, n, shift=0):
    lanes = row.shape[1]
    down = lax.broadcasted_iota(jnp.int32, (n, lanes), 0)
    across = lax.broadcasted_iota(jnp.int32, (n, lanes), 1)
    return jnp.sum(jnp.where(down + shift == across, row, 0.0), 1, keepdims=True)


def layer_kernel(
    seq_size,
    tp_size,
    starts_far,
    gain_far,
    encoded_far,
    cotangent_far,
    w_up_far,
    w_query_far,
    w_key_far,
    w_value_far,
    w_out_far,
    out_value,
    out_grad,
    starts,
    gain,
    encoded,
    cotangent,
    w_up,
    w_query,
    w_key,
    w_value,
    w_out,
    lead_out,
    lead_in,
    group,
    wide,
    wide_grad,
    scaled,
    key_bias,
    rinv_column,
    outbox,
    heads,
    value_turned,
    key_turned,
    scores,
    attn_turned,
    share_row,
    key_sum,
    value_sum,
    returns,
    back,
    grad_sum,
    partial,
    pair_in,
    cross_out,
    cross_in,
    dots_out,
    dots_in,
    weight_sem,
    near_sem,
    lead_sem,
    gather_send,
    gather_recv,
    out_send,
    out_recv,
    back_send,
    back_recv,
    pair_send,
    pair_recv,
    cross_send,
    cross_recv,
    dots_send,
    dots_recv,
):
    byte_rows, byte_width = encoded.shape
    shards, cap = starts.shape
    rows, columns = cotangent.shape
    model_width = gain.shape[1]
    patches_total = shards * cap
    mine = lax.axis_index("seq")
    t = lax.axis_index("tp")
    chip, core = t // 2, lax.rem(t, 2)
    shard = mine * tp_size + t
    partner = t + 1 - 2 * core
    across = lax.rem(t + 2, tp_size)
    diagonal = lax.rem(partner + 2, tp_size)
    tile = 2 * HEAD_DIM
    tiles = columns // tile
    scale = HEAD_DIM ** (-0.5)

    def remote(src, dst, send, recv, device):
        return pltpu.make_async_remote_copy(
            src_ref=src,
            dst_ref=dst,
            send_sem=send,
            recv_sem=recv,
            device_id=device,
            device_id_type=MESH,
        )

    barrier = pltpu.get_barrier_semaphore()
    for offset in range(1, tp_size):
        pl.semaphore_signal(
            barrier, inc=1, device_id={"tp": lax.rem(t + offset, tp_size)}, device_id_type=MESH
        )
    for offset in range(1, seq_size):
        pl.semaphore_signal(
            barrier, inc=1, device_id={"seq": lax.rem(mine + offset, seq_size)}, device_id_type=MESH
        )
    has_before = shard > 0
    has_after = shard < shards - 1
    group_first = jnp.logical_and(t == 0, has_before)
    group_last = jnp.logical_and(t == tp_size - 1, has_after)
    shard_before = {
        "seq": jnp.where(t == 0, lax.rem(mine + seq_size - 1, seq_size), mine),
        "tp": lax.rem(t + tp_size - 1, tp_size),
    }
    shard_after = {
        "seq": jnp.where(t == tp_size - 1, lax.rem(mine + 1, seq_size), mine),
        "tp": lax.rem(t + 1, tp_size),
    }

    @pl.when(group_first)
    def _():
        pl.semaphore_signal(barrier, inc=1, device_id=shard_before, device_id_type=MESH)

    @pl.when(group_last)
    def _():
        pl.semaphore_signal(barrier, inc=1, device_id=shard_after, device_id_type=MESH)

    near_copies = [
        pltpu.make_async_copy(starts_far, starts, near_sem.at[0]),
        pltpu.make_async_copy(encoded_far, encoded, near_sem.at[1]),
        pltpu.make_async_copy(cotangent_far, cotangent, near_sem.at[2]),
        pltpu.make_async_copy(gain_far, gain, near_sem.at[3]),
    ]
    for copy in near_copies:
        copy.start()
    pieces = 4

    def weight_copies(i, far, near):
        depth = far.shape[0] // pieces
        for p in range(pieces):
            part = pl.ds(p * depth, depth)
            pltpu.make_async_copy(far.at[part], near.at[part], weight_sem.at[i]).start()

    def weight_wait(i, far, near):
        pltpu.make_async_copy(far, near, weight_sem.at[i]).wait()

    near_copies[0].wait()
    limit = float(byte_rows)
    own = starts[pl.ds(shard, 1), :].astype(WIDE)
    after = starts[pl.ds(jnp.minimum(shard + 1, shards - 1), 1), :].astype(WIDE)
    first = to_column(own, cap)
    slot = lax.broadcasted_iota(jnp.int32, (cap, 1), 0)
    following = to_column(own, cap, 1) + jnp.where(slot == cap - 1, limit, 0.0)
    places = lax.broadcasted_iota(jnp.int32, (cap, byte_rows), 1).astype(WIDE)
    inside = jnp.where((places >= first) & (places < following), 1.0, 0.0).astype(LOW)
    lead_places = lax.broadcasted_iota(jnp.int32, (16, byte_rows), 1).astype(WIDE)
    leading = jnp.where(lead_places < own[:, :1], 1.0, 0.0).astype(LOW)
    near_copies[1].wait()
    weight_copies(0, w_up_far, w_up)
    weight_copies(4, w_out_far, w_out)
    lead_out[...] = dot(leading, encoded[...])[:1]
    sums = dot(inside, encoded[...])

    own_rows = tile_of(mine, rows)
    own_starts = [
        to_column(starts[pl.ds(mine * tp_size + u, 1), :].astype(WIDE), cap)
        for u in range(tp_size)
    ]
    row_valid = jnp.where(jnp.concatenate(own_starts, 0) < limit, 1.0, 0.0)
    near_copies[2].wait()
    wide_grad[t] = jnp.where(row_valid > 0.5, cotangent[...].astype(WIDE), 0.0).astype(LOW)

    neighbours = group_first.astype(jnp.int32) + group_last.astype(jnp.int32)
    pl.semaphore_wait(barrier, tp_size + seq_size - 2 + neighbours)

    lead_copy = remote(lead_out, lead_in, lead_sem.at[0], lead_sem.at[1], shard_before)

    @pl.when(has_before)
    def _():
        lead_copy.start()

    def gather_copy(way, k, kind, piece):
        target = across if way == 0 else partner
        return remote(
            piece, piece, gather_send.at[kind], gather_recv.at[way, k], {"tp": target}
        )

    def gather_start(k, kind, view):
        gather_copy(0, k, kind, view(t)).start()
        gather_copy(1, k, kind, view(t)).start()

    def gather_relay(k, kind, view):
        gather_copy(0, k, kind, view(across)).wait_recv()
        gather_copy(2, k, kind, view(across)).start()

    def gather_finish(k, kind, view, ways=(1, 2)):
        for way in ways:
            gather_copy(way, k, kind, view(partner if way == 1 else diagonal)).wait_recv()

    half_rows = rows // 2
    grad_views = (
        lambda q: wide_grad.at[q, :half_rows],
        lambda q: wide_grad.at[q, half_rows:],
    )
    gather_start(1, 1, grad_views[0])

    group_view = lambda q: group.at[tile_of(q, cap)]
    wide_tile = columns // 2

    def wide_view(batch, j):
        def view(q):
            of_chip = q // 2
            place = of_chip if batch == 0 else 1 - of_chip
            return wide.at[
                q, tile_of(place, half_rows), j * wide_tile : (j + 1) * wide_tile
            ]

        return view

    def wide_chunk(batch, j):
        return 2 + 2 * batch + j

    @pl.when(has_after)
    def _():
        lead_copy.wait_recv()

    joined = jnp.where(
        jnp.logical_and(first < limit, following >= limit), jnp.where(has_after, 1.0, 0.0), 0.0
    )
    sums = sums + joined * jnp.where(has_after, lead_in[...], 0.0)
    sizes = (following - first) * jnp.where(first < limit, 1.0, 0.0) + joined * after[:, :1]
    group[tile_of(t, cap), :] = (sums / jnp.maximum(sizes, 1.0)).astype(LOW)
    gather_start(0, 0, group_view)
    weight_copies(1, w_key_far, w_key)
    weight_copies(2, w_query_far, w_query)
    weight_copies(3, w_value_far, w_value)

    def raise_rows(batch):
        place = tile_of(chip if batch == 0 else 1 - chip, half_rows)
        for j in range(2):
            cut = slice(j * wide_tile, (j + 1) * wide_tile)
            wide[t, place, cut] = dot(group[place, :], w_up[:, cut]).astype(LOW)
            gather_start(wide_chunk(batch, j), 2, wide_view(batch, j))

    gather_finish(0, 0, group_view, (1,))
    weight_wait(0, w_up_far, w_up)
    raise_rows(0)

    far_half = 1 - mine // (seq_size // 2)

    def head_copy(k, h):
        if k >= 6:
            start = half_rows * (7 - k)
            src = outbox.at[3, h, start : start + half_rows]
            place = tile_of(2 * mine + 7 - k, half_rows)
        else:
            a, batch = k // 2, k % 2
            piece = 1 - chip if batch == 0 else chip
            src = outbox.at[a, h, tile_of(piece, half_rows)]
            place = tile_of(2 * mine + piece, half_rows)
        return remote(
            src,
            heads.at[min(k // 2, 3), place],
            out_send.at[k],
            out_recv.at[k],
            {"seq": h},
        )

    def start_head(k, h):
        @pl.when(h != mine)
        def _():
            head_copy(k, h).start()

    def keep_heads(a, h_first, block, start, size):
        for u in range(block.shape[1] // HEAD_DIM):
            h = h_first + u
            part = block[:, u * HEAD_DIM : (u + 1) * HEAD_DIM]

            @pl.when(h == mine)
            def _():
                heads[a, pl.ds(pl.multiple_of(mine * rows + start, size), size), :] = part

            @pl.when(h != mine)
            def _():
                outbox[a, h, pl.ds(pl.multiple_of(start, size), size), :] = part

    def d_attn_tile(upper, jj):
        j = far_half if jj == 0 else 1 - far_half
        start = 0 if upper else half_rows
        acc = jnp.zeros((half_rows, wide_tile), WIDE)
        for q in range(tp_size):
            acc += dot_last(
                wide_grad[q, start : start + half_rows],
                w_out[tile_of(j, wide_tile), q * columns : (q + 1) * columns],
            )
        held = wide_tile // HEAD_DIM
        keep_heads(3, j * held, acc.astype(LOW), start, half_rows)
        if upper:
            for u in range(held):
                start_head(7, j * held + u)

    def d_attn_rows(upper):
        for jj in range(2):
            d_attn_tile(upper, jj)

    def relay_rows(batch):
        for j in range(2):
            gather_relay(wide_chunk(batch, j), 2, wide_view(batch, j))

    def norm_rows(batch):
        place = tile_of(1 - chip if batch == 0 else chip, half_rows)

        def norm_step(q, square):
            piece = wide[q, place].astype(WIDE)
            scaled[q, place] = (piece * gain[:, tile_of(q, columns)]).astype(LOW)
            return square + jnp.sum(piece * piece, 1, keepdims=True)

        square = lax.fori_loop(0, tp_size, norm_step, jnp.zeros((half_rows, 1), WIDE))
        rinv_column[place, :] = lax.rsqrt(square / model_width + EPS)

    def project(a, weight, batch, width):
        piece = 1 - chip if batch == 0 else chip
        place = tile_of(piece, half_rows)
        steps = columns // width
        held = width // HEAD_DIM

        def step(jj, carry):
            j = lax.rem(far_half * (steps // 2) + jj, steps)
            acc = jnp.zeros((half_rows, width), WIDE)
            for q in range(tp_size):
                acc += dot(
                    scaled[q, place], weight[q * columns : (q + 1) * columns, tile_of(j, width)]
                )
            block = (rinv_column[place, :] * acc).astype(LOW)
            keep_heads(a, j * held, block, piece * half_rows, half_rows)
            for u in range(held):
                start_head(2 * a + batch, j * held + u)
            return carry

        lax.fori_loop(0, steps, step, 0)

    gather_relay(1, 1, grad_views[0])
    gather_relay(0, 0, group_view)
    weight_wait(4, w_out_far, w_out)
    gather_finish(1, 1, grad_views[0])
    d_attn_tile(1, 0)
    gather_finish(0, 0, group_view, (2,))
    raise_rows(1)
    near_copies[3].wait()
    relay_rows(0)
    for j in range(2):
        gather_finish(wide_chunk(0, j), 2, wide_view(0, j), (2,))
        gather_finish(wide_chunk(1, j), 2, wide_view(1, j), (1,))
    norm_rows(0)
    weight_wait(1, w_key_far, w_key)
    project(1, w_key, 0, tile)
    d_attn_tile(1, 1)
    relay_rows(1)
    gather_start(6, 1, grad_views[1])
    weight_wait(2, w_query_far, w_query)
    project(0, w_query, 0, wide_tile)
    weight_wait(3, w_value_far, w_value)
    project(2, w_value, 0, wide_tile)
    for j in range(2):
        gather_finish(wide_chunk(0, j), 2, wide_view(0, j), (1,))
        gather_finish(wide_chunk(1, j), 2, wide_view(1, j), (2,))
    norm_rows(1)
    project(1, w_key, 1, wide_tile)
    project(0, w_query, 1, wide_tile)
    gather_relay(6, 1, grad_views[1])
    project(2, w_value, 1, wide_tile)
    gather_finish(6, 1, grad_views[1])

    d_attn_rows(0)

    def heads_arrived(k):
        place = heads.at[min(k // 2, 3), : half_rows * (seq_size - 1)]
        remote(place, place, out_send.at[k], out_recv.at[k], {"seq": mine}).wait_recv()

    def turn(weight):
        def turn_square(q, carry):
            square = weight.at[tile_of(q, columns)]
            square[...] = square[...].T
            return carry

        lax.fori_loop(0, tp_size, turn_square, 0)

    index = lax.broadcasted_iota(jnp.int32, (patches_total, shards), 0)
    lane = lax.broadcasted_iota(jnp.int32, (patches_total, shards), 1)
    owner = jnp.where((index >= lane * cap) & (index < lane * cap + cap), 1.0, 0.0).astype(LOW)
    valid = jnp.where(starts[...].astype(WIDE) < limit, 1.0, 0.0).astype(LOW)
    spread = dot(owner, valid)
    slots = lax.broadcasted_iota(jnp.int32, (patches_total, cap), 1)
    places_in = lax.broadcasted_iota(jnp.int32, (patches_total, cap), 0)
    valid_column = jnp.sum(
        jnp.where(jnp.bitwise_and(places_in, cap - 1) == slots, spread, 0.0), 1, keepdims=True
    )
    key_bias[...] = jnp.broadcast_to((valid_column - 1.0) * -NEG, key_bias.shape)
    turn(w_key)
    for k in range(4):
        heads_arrived(k)
    for step in range(seq_size):
        start_head(6, lax.rem(far_half * (seq_size // 2) + step, seq_size))

    blocks = patches_total // tile
    own_columns = tile_of(mine, HEAD_DIM)

    def piece_of(k):
        if k < 2:
            return k, 0, rows
        return 2 + k % 2, half_rows * (k // 2 - 1), half_rows

    half_seq = seq_size // 2
    near_half = mine // half_seq

    def return_copy(k, peer):
        a, start, size = piece_of(k)
        return remote(
            returns.at[a, pl.ds(peer * rows + start, size)],
            back.at[a, start : start + size, own_columns],
            back_send.at[k],
            back_recv.at[k, jnp.where(peer // half_seq == near_half, 0, 1)],
            {"seq": peer},
        )

    def send_back(k, i):
        a, start, size = piece_of(k)
        for peer in range(i * tile // rows, (i + 1) * tile // rows):

            @pl.when(peer != mine)
            def _():
                return_copy(k, peer).start()

            @pl.when(peer == mine)
            def _():
                first = peer * rows + start
                back[a, start : start + size, own_columns] = returns[a, first : first + size, :]

    def sent_back(k):
        a, start, size = piece_of(k)
        sent = returns.at[a, : size * (seq_size - 1)]
        remote(sent, sent, back_send.at[k], back_recv.at[k, 0], {"seq": mine}).wait_send()

    def cut_of(i):
        return slice(i * tile, (i + 1) * tile)

    def score_cut(i, j):
        return cut_of(i * (i + 1) // 2 + j)

    for j in range(blocks):
        key_turned[:, cut_of(j)] = heads[1, cut_of(j), :].astype(WIDE).T.astype(LOW)

    def attend(i):
        peak = jnp.full((1, tile), NEG, WIDE)
        for j in range(i + 1):
            score = dot_last(heads[1, cut_of(j), :], heads[0, cut_of(i), :]) * scale
            bias = key_bias[cut_of(j), :]
            score += jnp.concatenate([bias] * (tile // bias.shape[1]), 1)
            if i == j:
                key = lax.broadcasted_iota(jnp.int32, (tile, tile), 0)
                query = lax.broadcasted_iota(jnp.int32, (tile, tile), 1)
                score = jnp.where(key <= query, score, NEG)
            scores[score_cut(i, j), :] = score
            peak = jnp.maximum(peak, jnp.max(score, 0, keepdims=True))
        total = jnp.zeros((1, tile), WIDE)
        for j in range(i + 1):
            expo = jnp.exp(scores[score_cut(i, j), :] - peak)
            scores[score_cut(i, j), :] = expo
            total += jnp.sum(expo, 0, keepdims=True)
        share_row[:, cut_of(i)] = 1.0 / total

    def mix(i):
        mixed = jnp.zeros((HEAD_DIM, tile), WIDE)
        for j in range(i + 1):
            mixed += dot(value_turned[:, cut_of(j)], scores[score_cut(i, j), :].astype(LOW))
        attn = (mixed * share_row[:, cut_of(i)]).astype(LOW).astype(WIDE)
        attn_turned[:, cut_of(i)] = attn
        returns[0, cut_of(i), :] = attn.T.astype(LOW)

    def attend_back(i):
        grad = heads[3, cut_of(i), :]
        delta = jnp.sum(grad.astype(WIDE).T * attn_turned[:, cut_of(i)], 0, keepdims=True)
        share = share_row[:, cut_of(i)]
        query_sum = jnp.zeros((HEAD_DIM, tile), WIDE)
        for j in range(i + 1):
            d_probs = dot_last(heads[2, cut_of(j), :], grad)
            probs = scores[score_cut(i, j), :] * share
            d_scores = (probs * (d_probs - delta)).astype(LOW)
            value_part = dot(probs.astype(LOW), grad)
            key_part = dot(d_scores, heads[0, cut_of(i), :])
            query_sum += dot(key_turned[:, cut_of(j)], d_scores)
            if i < blocks - 1:
                value_part += value_sum[cut_of(j), :]
                key_part += key_sum[cut_of(j), :]
            if i == j:
                returns[2, cut_of(j), :] = value_part.astype(LOW)
                returns[3, cut_of(j), :] = (key_part * scale).astype(LOW)
            else:
                value_sum[cut_of(j), :] = value_part
                key_sum[cut_of(j), :] = key_part
        returns[1, cut_of(i), :] = (query_sum * scale).T.astype(LOW)

    ends = [0] + list(reversed(range(1, blocks)))
    for i in range(blocks):
        attend(i)
    for k in (4, 5):
        heads_arrived(k)
    for j in range(blocks):
        value_turned[:, cut_of(j)] = heads[2, cut_of(j), :].astype(WIDE).T.astype(LOW)
    for i in ends:
        mix(i)
        send_back(0, i)
    turn(w_query)
    heads_arrived(7)
    heads_arrived(6)
    for i in reversed(range(blocks)):
        attend_back(i)
        send_back(1, i)
    turn(w_value)
    sent_back(0)
    for k in (2, 3):
        for i in range(blocks):
            send_back(k, i)

    def returns_arrived(k, sides=(0, 1)):
        a, start, size = piece_of(k)
        for side in sides:
            place = returns.at[a, : size * (half_seq - 1 + side)]
            remote(
                place, place, back_send.at[k], back_recv.at[k, side], {"seq": mine}
            ).wait_recv()

    order = (
        (1 - chip) * 2 + (1 - core),
        (1 - chip) * 2 + core,
        chip * 2 + (1 - core),
        chip * 2 + core,
    )
    stages = ((0, slice(0, rows)), (1, slice(0, half_rows)), (1, slice(half_rows, rows)))

    def pair_copy(stage, k):
        a, part = stages[stage]
        return remote(
            partial.at[a, order[2 * k], part],
            pair_in.at[a, k, part],
            pair_send.at[stage],
            pair_recv.at[stage, k],
            {"tp": partner},
        )

    def cross_copy(stage):
        a, part = stages[stage]
        return remote(
            cross_out.at[a, part],
            cross_in.at[a, part],
            cross_send.at[stage],
            cross_recv.at[stage],
            {"tp": across},
        )

    def cross_over(stage):
        a, part = stages[stage]
        pair_copy(stage, 0).wait_recv()
        cross_out[a, part] = (
            partial[a, order[1], part].astype(WIDE) + pair_in[a, 0, part].astype(WIDE)
        ).astype(LOW)
        cross_copy(stage).start()

    def summed(stage):
        a, part = stages[stage]
        pair_copy(stage, 1).wait_recv()
        cross_copy(stage).wait_recv()
        return (
            partial[a, t, part].astype(WIDE)
            + pair_in[a, 1, part].astype(WIDE)
            + cross_in[a, part].astype(WIDE)
        )

    returns_arrived(0)
    for k in range(tp_size):
        quarter = order[k]

        for j in range(2):
            at = tile_of(quarter * 2 + j, wide_tile)
            here = slice(j * wide_tile, (j + 1) * wide_tile)
            partial[0, quarter, :, here] = dot(back[0], w_out[:, at]).astype(LOW)
        if k % 2 == 0:
            pair_copy(0, k // 2).start()
    def dots_copy(half, offset):
        return remote(
            dots_out.at[half],
            dots_in.at[half, offset],
            dots_send.at[half],
            dots_recv.at[half],
            {"tp": lax.rem(t + offset, tp_size)},
        )

    def share_gradient(half, product):
        stage = 1 + half
        part = stages[stage][1]
        dots = jnp.zeros((half_rows, 1), WIDE)
        for k in range(tp_size):
            quarter = order[k]
            for j in range(2):
                at = tile_of(quarter * 2 + j, wide_tile)
                here = slice(j * wide_tile, (j + 1) * wide_tile)
                whole = product(quarter, here)
                partial[1, quarter, part, here] = whole.astype(LOW)
                inner = gain[:, at] * whole * wide[quarter, part, here].astype(WIDE)
                dots += jnp.sum(inner, 1, keepdims=True)
            if k % 2 == 0:
                pair_copy(stage, k // 2).start()
            if k == 2:
                cross_over(stage)
        dots_out[half] = jnp.broadcast_to(to_row(dots, rows), dots_out.shape[1:])
        for offset in range(1, tp_size):
            dots_copy(half, offset).start()
        return dots

    def finish_gradient(half, dots):
        stage = 1 + half
        part = stages[stage][1]
        place = dots_in.at[half, 1:]
        remote(place, place, dots_send.at[half], dots_recv.at[half], {"tp": t}).wait_recv()
        for offset in range(1, tp_size):
            dots += to_column(dots_in[half, offset, :1], half_rows)
        rinv = rinv_column[part, :]
        out_grad[part, :] = (
            wide_grad[t, part].astype(WIDE)
            + rinv * gain[:, tile_of(t, columns)] * summed(stage)
            - wide[t, part].astype(WIDE) * (rinv**3 * dots / model_width)
        )

    half_columns = columns // 2
    for side in range(2):
        returns_arrived(1, (side,))
        which = near_half if side == 0 else 1 - near_half

        def query_step(quarter, carry):
            at = tile_of(quarter * 2 + which, half_columns)
            for j in range(2):
                here = slice(j * wide_tile, (j + 1) * wide_tile)
                more = dot(back[1, :, tile_of(which, half_columns)], w_query[at, here])
                if side == 0:
                    grad_sum[quarter, :, here] = more
                else:
                    grad_sum[quarter, :, here] += more
            return carry

        lax.fori_loop(0, tp_size, query_step, 0, unroll=2)
        sent_back(1 + side)
        for i in range(blocks):
            send_back(4 + side, i)
        if side == 0:
            cross_over(0)

    def half_gradient(half):
        part = stages[1 + half][1]

        def value_step(quarter, carry):
            for j in range(2):
                here = slice(j * wide_tile, (j + 1) * wide_tile)
                turned = w_value[tile_of(quarter, columns), here]
                grad_sum[quarter, part, here] += dot(back[2, part], turned)
            return carry

        def product(quarter, here):
            turned = w_key[tile_of(quarter, columns), here]
            return grad_sum[quarter, part, here] + dot(back[3, part], turned)

        returns_arrived(2 + 2 * half)
        lax.fori_loop(0, tp_size, value_step, 0, unroll=2)
        returns_arrived(3 + 2 * half)
        return share_gradient(half, product)

    upper_dots = half_gradient(0)
    lower_dots = half_gradient(1)
    out_value[...] = jnp.where(
        row_valid > 0.5, wide[t].astype(WIDE) + summed(0), 0.0
    ).astype(LOW)
    finish_gradient(0, upper_dots)
    finish_gradient(1, lower_dots)

    @pl.when(has_before)
    def _():
        lead_copy.wait_send()

    for kind, sent in ((0, group.at[: 3 * cap]), (1, wide_grad.at[:3]), (2, wide.at[:3])):
        gather_copy(0, 0, kind, sent).wait_send()
    for k in range(8):
        sent = outbox.at[min(k // 2, 3), 1:, :half_rows]
        remote(sent, sent, out_send.at[k], out_recv.at[k], {"seq": mine}).wait_send()
    for k in (3, 4, 5):
        sent_back(k)
    for stage in range(len(stages)):
        a, part = stages[stage]
        sent = pair_in.at[a, :, part]
        remote(
            sent, sent, pair_send.at[stage], pair_recv.at[stage, 0], {"tp": partner}
        ).wait_send()
        cross_copy(stage).wait_send()
    for half in range(2):
        sent = dots_in.at[half, 1:]
        remote(sent, sent, dots_send.at[half], dots_recv.at[half], {"tp": t}).wait_send()


def per_device_whole(encoded, starts, w_up, norm_gain, w_query, w_key, w_value, w_out, cotangent):
    seq_size, tp_size = lax.axis_size("seq"), lax.axis_size("tp")
    rows, columns = cotangent.shape
    model_width = norm_gain.shape[0]
    byte_width = encoded.shape[1]
    cap = starts.shape[1]
    total = starts.size
    tile = 2 * HEAD_DIM
    blocks = total // tile
    dma = pltpu.SemaphoreType.DMA
    scratch = [
        pltpu.VMEM(starts.shape, jnp.int32),
        pltpu.VMEM((1, model_width), WIDE),
        pltpu.VMEM(encoded.shape, LOW),
        pltpu.VMEM(cotangent.shape, LOW),
        pltpu.VMEM(w_up.shape, LOW),
        pltpu.VMEM(w_query.shape, LOW),
        pltpu.VMEM(w_key.shape, LOW),
        pltpu.VMEM(w_value.shape, LOW),
        pltpu.VMEM(w_out.shape, LOW),
        pltpu.VMEM((1, byte_width), WIDE),
        pltpu.VMEM((1, byte_width), WIDE),
        pltpu.VMEM((rows, byte_width), LOW),
        pltpu.VMEM((tp_size, rows, columns), LOW),
        pltpu.VMEM((tp_size, rows, columns), LOW),
        pltpu.VMEM((tp_size, rows, columns), LOW),
        pltpu.VMEM((total, 128), WIDE),
        pltpu.VMEM((rows, 1), WIDE),
        pltpu.VMEM((4, seq_size, rows, HEAD_DIM), LOW),
        pltpu.VMEM((4, total, HEAD_DIM), LOW),
        pltpu.VMEM((HEAD_DIM, total), LOW),
        pltpu.VMEM((HEAD_DIM, total), LOW),
        pltpu.VMEM((blocks * (blocks + 1) // 2 * tile, tile), WIDE),
        pltpu.VMEM((HEAD_DIM, total), WIDE),
        pltpu.VMEM((1, total), WIDE),
        pltpu.VMEM((total, HEAD_DIM), WIDE),
        pltpu.VMEM((total, HEAD_DIM), WIDE),
        pltpu.VMEM((4, total, HEAD_DIM), LOW),
        pltpu.VMEM((4, rows, columns), LOW),
        pltpu.VMEM((tp_size, rows, columns), WIDE),
        pltpu.VMEM((2, tp_size, rows, columns), LOW),
        pltpu.VMEM((2, 2, rows, columns), LOW),
        pltpu.VMEM((2, rows, columns), LOW),
        pltpu.VMEM((2, rows, columns), LOW),
        pltpu.VMEM((2, 8, rows), WIDE),
        pltpu.VMEM((2, tp_size, 8, rows), WIDE),
        dma((5,)),
        dma((4,)),
        dma((2,)),
        dma((3,)),
        dma((3, 7)),
        dma((8,)),
        dma((8,)),
        dma((6,)),
        dma((6, 2)),
        dma((3,)),
        dma((3, 2)),
        dma((3,)),
        dma((3,)),
        dma((2,)),
        dma((2,)),
    ]
    near = pl.BlockSpec(memory_space=pltpu.VMEM)
    far = pl.BlockSpec(memory_space=pl.ANY)
    return tuple(
        pl.pallas_call(
            functools.partial(layer_kernel, seq_size, tp_size),
            out_shape=[
                pltpu.VMEM((rows, columns), LOW),
                pltpu.VMEM((rows, columns), WIDE),
            ],
            in_specs=[far] * 9,
            out_specs=[near] * 2,
            scratch_shapes=scratch,
            compiler_params=pltpu.CompilerParams(
                collective_id=0, has_side_effects=True, vmem_limit_bytes=60 * 1024 * 1024
            ),
        )(
            starts,
            norm_gain.reshape(1, model_width),
            encoded,
            cotangent,
            w_up,
            w_query,
            w_key,
            w_value,
            w_out,
        )
    )


def fits_one_kernel(arrays):
    encoded, starts, w_up, norm_gain, w_query, w_key, w_value, w_out, cotangent = arrays
    seq_size, tp_size = lax.axis_size("seq"), lax.axis_size("tp")
    rows, columns = cotangent.shape
    cap = starts.shape[1]
    return (
        tp_size == 4
        and seq_size % 2 == 0
        and columns == seq_size * HEAD_DIM
        and rows == HEAD_DIM
        and rows == tp_size * cap
        and cap & (cap - 1) == 0
        and cap % 16 == 0
        and columns % (4 * HEAD_DIM) == 0
        and norm_gain.shape[0] == tp_size * columns
        and starts.shape[0] == seq_size * tp_size
        and starts.size % (2 * HEAD_DIM) == 0
    )


def solution(mesh):
    in_specs = (
        P(("seq", "tp"), None),
        P(),
        P(None, "tp"),
        P(),
        P(None, "tp"),
        P(None, "tp"),
        P(None, "tp"),
        P("tp", None),
        P("seq", "tp"),
    )
    out_specs = (P("seq", "tp"), P("seq", "tp"))

    def choose(*arrays):
        return (per_device_whole if fits_one_kernel(arrays) else per_device)(*arrays)

    return jax.shard_map(
        choose, mesh=mesh, in_specs=in_specs, out_specs=out_specs, check_vma=False
    )
```

```python
import functools

import jax
import jax.numpy as jnp
from jax import lax
from jax.experimental import pallas as pl
from jax.experimental.pallas import tpu as pltpu
from jax.sharding import PartitionSpec as P

HEAD_DIM = 128


EPS = 1e-05
NEG = -1e30
CONTRACT_LAST = (((1,), (1,)), ((), ()))


def shifted(block, axis, distance):
    devices = range(lax.axis_size(axis))
    route = [(i - distance, i) for i in devices if i - distance in devices]
    return lax.ppermute(block, axis, route)


def per_device(encoded, starts, w_up, norm_gain, w_query, w_key, w_value, w_out, cotangent):
    byte_rows = encoded.shape[0]
    patch_cap = starts.shape[1]
    model_width = norm_gain.shape[0]
    shard = lax.axis_index(("seq", "tp"))
    own_starts = lax.dynamic_slice_in_dim(starts, shard, 1, 0)[0]
    places = jnp.arange(byte_rows, dtype=jnp.int32)
    following = jnp.concatenate([own_starts[1:], jnp.full((1,), byte_rows, jnp.int32)])
    inside = (places[None, :] >= own_starts[:, None]) & (places[None, :] < following[:, None])
    sums = jnp.dot(inside.astype(jnp.bfloat16), encoded, preferred_element_type=jnp.float32)
    sizes = jnp.sum(inside.astype(jnp.float32), 1)
    leading = places[None, :] < own_starts[:1, None]
    lead_sum = jnp.dot(leading.astype(jnp.bfloat16), encoded, preferred_element_type=jnp.float32)
    lead_size = jnp.sum(leading.astype(jnp.float32), 1)
    next_sum, next_size = shifted((lead_sum, lead_size), ("seq", "tp"), -1)
    count = jnp.sum((own_starts < byte_rows).astype(jnp.int32))
    last_slot = (jnp.arange(patch_cap, dtype=jnp.int32) == count - 1).astype(jnp.float32)
    sums = sums + last_slot[:, None] * next_sum
    sizes = sizes + last_slot * next_size
    patches = (sums / jnp.maximum(sizes, 1.0)[:, None]).astype(jnp.bfloat16)
    group = lax.all_gather(patches, "tp", axis=0, tiled=True)
    latent_in = jnp.dot(group, w_up, preferred_element_type=jnp.float32).astype(jnp.bfloat16)
    group_rows, columns = latent_in.shape
    head_count = columns // HEAD_DIM
    wide_piece = lax.all_gather(latent_in, "tp", axis=1, tiled=True).astype(jnp.float32)
    scaled = (wide_piece * norm_gain[None, :]).astype(jnp.bfloat16)
    acc_query = jnp.dot(scaled, w_query, preferred_element_type=jnp.float32)
    acc_key = jnp.dot(scaled, w_key, preferred_element_type=jnp.float32)
    acc_value = jnp.dot(scaled, w_value, preferred_element_type=jnp.float32)
    acc_query, acc_key, acc_value, square = (
        acc_query,
        acc_key,
        acc_value,
        jnp.sum(wide_piece * wide_piece, 1),
    )
    rinv = lax.rsqrt(square / model_width + EPS)
    query = (rinv[:, None] * acc_query).astype(jnp.bfloat16)
    key_rows = (rinv[:, None] * acc_key).astype(jnp.bfloat16)
    value_rows = (rinv[:, None] * acc_value).astype(jnp.bfloat16)
    keys_all, values_all = (
        lax.all_gather(key_rows, "seq", axis=0, tiled=True),
        lax.all_gather(value_rows, "seq", axis=0, tiled=True),
    )
    patches_total = keys_all.shape[0]
    valid_all = (starts < byte_rows).reshape(patches_total)
    row_base = lax.axis_index("seq") * group_rows
    query_index = row_base + jnp.arange(group_rows, dtype=jnp.int32)
    key_index = jnp.arange(patches_total, dtype=jnp.int32)
    query_valid = lax.dynamic_slice_in_dim(valid_all, row_base, group_rows, 0)
    allowed = valid_all[None, :] & (key_index[None, :] <= query_index[:, None])
    scale = HEAD_DIM ** (-0.5)
    query_heads = query.reshape(group_rows, head_count, HEAD_DIM)
    key_heads = keys_all.reshape(patches_total, head_count, HEAD_DIM)
    value_heads = values_all.reshape(patches_total, head_count, HEAD_DIM)
    scores = (
        jnp.einsum("rhd,khd->hrk", query_heads, key_heads, preferred_element_type=jnp.float32)
        * scale
    )
    peak = jnp.max(jnp.where(allowed[None], scores, NEG), 2)
    expo = jnp.where(allowed[None], jnp.exp(scores - peak[:, :, None]), 0.0)
    total = jnp.sum(expo, 2)
    mixed = jnp.einsum(
        "hrk,khd->rhd", expo.astype(jnp.bfloat16), value_heads, preferred_element_type=jnp.float32
    )
    attn = (mixed / total.T[:, :, None]).astype(jnp.bfloat16)
    partial_value = jnp.dot(
        attn.reshape(group_rows, columns), w_out, preferred_element_type=jnp.float32
    )
    head_sum = lax.psum_scatter(
        partial_value.astype(jnp.bfloat16), "tp", scatter_dimension=1, tiled=True
    ).astype(jnp.float32)
    wide_in = latent_in.astype(jnp.float32)
    latent_out = jnp.where(query_valid[:, None], wide_in + head_sum, 0.0).astype(jnp.bfloat16)
    grad_out = jnp.where(query_valid[:, None], cotangent, jnp.zeros_like(cotangent))
    d_attn = lax.dot_general(
        lax.all_gather(grad_out, "tp", axis=1, tiled=True),
        w_out,
        CONTRACT_LAST,
        preferred_element_type=jnp.float32,
    ).astype(jnp.bfloat16)
    grad_heads = d_attn.reshape(group_rows, head_count, HEAD_DIM)
    delta = jnp.sum(grad_heads.astype(jnp.float32) * attn.astype(jnp.float32), 2).T
    probs = expo / total[:, :, None]
    d_probs = jnp.einsum(
        "rhd,khd->hrk", grad_heads, value_heads, preferred_element_type=jnp.float32
    )
    d_scores = (probs * (d_probs - delta[:, :, None])).astype(jnp.bfloat16)
    grad_query = (
        (
            jnp.einsum("hrk,khd->rhd", d_scores, key_heads, preferred_element_type=jnp.float32)
            * scale
        )
        .astype(jnp.bfloat16)
        .reshape(group_rows, columns)
    )
    weights_low = probs.astype(jnp.bfloat16)
    count_rows = group_rows * lax.axis_size("seq")
    key_part = jnp.einsum("hrk,rhd->khd", d_scores, query_heads, preferred_element_type=jnp.float32)
    value_part = jnp.einsum(
        "hrk,rhd->khd", weights_low, grad_heads, preferred_element_type=jnp.float32
    )
    both = lax.psum_scatter(
        jnp.concatenate(
            [key_part.reshape(count_rows, columns), value_part.reshape(count_rows, columns)], 1
        ).astype(jnp.bfloat16),
        "seq",
        scatter_dimension=0,
        tiled=True,
    ).astype(jnp.float32)
    grad_key = (both[:, :columns] * scale).astype(jnp.bfloat16)
    grad_value = both[:, columns:].astype(jnp.bfloat16)
    dnormed = (
        lax.dot_general(grad_query, w_query, CONTRACT_LAST, preferred_element_type=jnp.float32)
        + lax.dot_general(grad_key, w_key, CONTRACT_LAST, preferred_element_type=jnp.float32)
        + lax.dot_general(grad_value, w_value, CONTRACT_LAST, preferred_element_type=jnp.float32)
    )
    normed_grad = lax.psum_scatter(
        dnormed.astype(jnp.bfloat16), "tp", scatter_dimension=1, tiled=True
    ).astype(jnp.float32)
    gain_own = lax.dynamic_slice_in_dim(norm_gain, lax.axis_index("tp") * columns, columns, 0)
    dots = lax.psum(jnp.sum(gain_own[None, :] * normed_grad * wide_in, 1), "tp")
    latent_grad = (
        grad_out.astype(jnp.float32)
        + rinv[:, None] * gain_own[None, :] * normed_grad
        - wide_in * (rinv**3)[:, None] * dots[:, None] / model_width
    )
    return (latent_out, latent_grad)


MESH = pl.DeviceIdType.MESH
LOW = jnp.bfloat16
WIDE = jnp.float32
ROWS_FIRST = (((0,), (0,)), ((), ()))


def tile_of(index, size):
    return pl.ds(pl.multiple_of(index * size, size), size)


def dot(a, b):
    return jnp.dot(a, b, preferred_element_type=WIDE)


def dot_last(a, b):
    return lax.dot_general(a, b, CONTRACT_LAST, preferred_element_type=WIDE)


def to_row(column, lanes):
    n = column.shape[0]
    down = lax.broadcasted_iota(jnp.int32, (n, lanes), 0)
    across = lax.broadcasted_iota(jnp.int32, (n, lanes), 1)
    return jnp.sum(jnp.where(down == across, column, 0.0), 0, keepdims=True)


def to_column(row, n, shift=0):
    lanes = row.shape[1]
    down = lax.broadcasted_iota(jnp.int32, (n, lanes), 0)
    across = lax.broadcasted_iota(jnp.int32, (n, lanes), 1)
    return jnp.sum(jnp.where(down + shift == across, row, 0.0), 1, keepdims=True)


def layer_kernel(
    seq_size,
    tp_size,
    starts_far,
    gain_far,
    encoded_far,
    cotangent_far,
    w_up_far,
    w_query_far,
    w_key_far,
    w_value_far,
    w_out_far,
    out_value,
    out_grad,
    starts,
    gain,
    encoded,
    cotangent,
    w_up,
    w_query,
    w_key,
    w_value,
    w_out,
    lead_out,
    lead_in,
    group,
    wide,
    wide_grad,
    scaled,
    key_bias,
    rinv_column,
    outbox,
    heads,
    value_turned,
    key_turned,
    scores,
    attn_turned,
    share_row,
    key_sum,
    value_sum,
    returns,
    back,
    grad_sum,
    partial,
    pair_in,
    cross_out,
    cross_in,
    dots_out,
    dots_in,
    weight_sem,
    near_sem,
    lead_sem,
    gather_send,
    gather_recv,
    out_send,
    out_recv,
    back_send,
    back_recv,
    pair_send,
    pair_recv,
    cross_send,
    cross_recv,
    dots_send,
    dots_recv,
):
    byte_rows, byte_width = encoded.shape
    shards, cap = starts.shape
    rows, columns = cotangent.shape
    model_width = gain.shape[1]
    patches_total = shards * cap
    mine = lax.axis_index("seq")
    t = lax.axis_index("tp")
    chip, core = t // 2, lax.rem(t, 2)
    shard = mine * tp_size + t
    partner = t + 1 - 2 * core
    across = lax.rem(t + 2, tp_size)
    diagonal = lax.rem(partner + 2, tp_size)
    tile = 2 * HEAD_DIM
    tiles = columns // tile
    scale = HEAD_DIM ** (-0.5)

    def remote(src, dst, send, recv, device):
        return pltpu.make_async_remote_copy(
            src_ref=src,
            dst_ref=dst,
            send_sem=send,
            recv_sem=recv,
            device_id=device,
            device_id_type=MESH,
        )

    barrier = pltpu.get_barrier_semaphore()
    for offset in range(1, tp_size):
        pl.semaphore_signal(
            barrier, inc=1, device_id={"tp": lax.rem(t + offset, tp_size)}, device_id_type=MESH
        )
    for offset in range(1, seq_size):
        pl.semaphore_signal(
            barrier, inc=1, device_id={"seq": lax.rem(mine + offset, seq_size)}, device_id_type=MESH
        )
    has_before = shard > 0
    has_after = shard < shards - 1
    group_first = jnp.logical_and(t == 0, has_before)
    group_last = jnp.logical_and(t == tp_size - 1, has_after)
    shard_before = {
        "seq": jnp.where(t == 0, lax.rem(mine + seq_size - 1, seq_size), mine),
        "tp": lax.rem(t + tp_size - 1, tp_size),
    }
    shard_after = {
        "seq": jnp.where(t == tp_size - 1, lax.rem(mine + 1, seq_size), mine),
        "tp": lax.rem(t + 1, tp_size),
    }

    @pl.when(group_first)
    def _():
        pl.semaphore_signal(barrier, inc=1, device_id=shard_before, device_id_type=MESH)

    @pl.when(group_last)
    def _():
        pl.semaphore_signal(barrier, inc=1, device_id=shard_after, device_id_type=MESH)

    near_copies = [
        pltpu.make_async_copy(starts_far, starts, near_sem.at[0]),
        pltpu.make_async_copy(encoded_far, encoded, near_sem.at[1]),
        pltpu.make_async_copy(cotangent_far, cotangent, near_sem.at[2]),
        pltpu.make_async_copy(gain_far, gain, near_sem.at[3]),
    ]
    for copy in near_copies:
        copy.start()
    pieces = 4

    def weight_copies(i, far, near):
        depth = far.shape[0] // pieces
        for p in range(pieces):
            part = pl.ds(p * depth, depth)
            pltpu.make_async_copy(far.at[part], near.at[part], weight_sem.at[i]).start()

    def weight_wait(i, far, near):
        pltpu.make_async_copy(far, near, weight_sem.at[i]).wait()

    near_copies[0].wait()
    limit = float(byte_rows)
    own = starts[pl.ds(shard, 1), :].astype(WIDE)
    after = starts[pl.ds(jnp.minimum(shard + 1, shards - 1), 1), :].astype(WIDE)
    first = to_column(own, cap)
    slot = lax.broadcasted_iota(jnp.int32, (cap, 1), 0)
    following = to_column(own, cap, 1) + jnp.where(slot == cap - 1, limit, 0.0)
    places = lax.broadcasted_iota(jnp.int32, (cap, byte_rows), 1).astype(WIDE)
    inside = jnp.where((places >= first) & (places < following), 1.0, 0.0).astype(LOW)
    lead_places = lax.broadcasted_iota(jnp.int32, (16, byte_rows), 1).astype(WIDE)
    leading = jnp.where(lead_places < own[:, :1], 1.0, 0.0).astype(LOW)
    near_copies[1].wait()
    weight_copies(0, w_up_far, w_up)
    weight_copies(4, w_out_far, w_out)
    lead_out[...] = dot(leading, encoded[...])[:1]
    sums = dot(inside, encoded[...])

    own_rows = tile_of(mine, rows)
    own_starts = [
        to_column(starts[pl.ds(mine * tp_size + u, 1), :].astype(WIDE), cap)
        for u in range(tp_size)
    ]
    row_valid = jnp.where(jnp.concatenate(own_starts, 0) < limit, 1.0, 0.0)
    near_copies[2].wait()
    wide_grad[t] = jnp.where(row_valid > 0.5, cotangent[...].astype(WIDE), 0.0).astype(LOW)

    neighbours = group_first.astype(jnp.int32) + group_last.astype(jnp.int32)
    pl.semaphore_wait(barrier, tp_size + seq_size - 2 + neighbours)

    lead_copy = remote(lead_out, lead_in, lead_sem.at[0], lead_sem.at[1], shard_before)

    @pl.when(has_before)
    def _():
        lead_copy.start()

    def gather_copy(way, k, kind, piece):
        target = across if way == 0 else partner
        return remote(
            piece, piece, gather_send.at[kind], gather_recv.at[way, k], {"tp": target}
        )

    def gather_start(k, kind, view):
        gather_copy(0, k, kind, view(t)).start()
        gather_copy(1, k, kind, view(t)).start()

    def gather_relay(k, kind, view):
        gather_copy(0, k, kind, view(across)).wait_recv()
        gather_copy(2, k, kind, view(across)).start()

    def gather_finish(k, kind, view, ways=(1, 2)):
        for way in ways:
            gather_copy(way, k, kind, view(partner if way == 1 else diagonal)).wait_recv()

    half_rows = rows // 2
    grad_views = (
        lambda q: wide_grad.at[q, :half_rows],
        lambda q: wide_grad.at[q, half_rows:],
    )
    gather_start(1, 1, grad_views[0])

    group_view = lambda q: group.at[tile_of(q, cap)]
    wide_tile = columns // 2

    def wide_view(batch, j):
        def view(q):
            of_chip = q // 2
            place = of_chip if batch == 0 else 1 - of_chip
            return wide.at[
                q, tile_of(place, half_rows), j * wide_tile : (j + 1) * wide_tile
            ]

        return view

    def wide_chunk(batch, j):
        return 2 + 2 * batch + j

    @pl.when(has_after)
    def _():
        lead_copy.wait_recv()

    joined = jnp.where(
        jnp.logical_and(first < limit, following >= limit), jnp.where(has_after, 1.0, 0.0), 0.0
    )
    sums = sums + joined * jnp.where(has_after, lead_in[...], 0.0)
    sizes = (following - first) * jnp.where(first < limit, 1.0, 0.0) + joined * after[:, :1]
    group[tile_of(t, cap), :] = (sums / jnp.maximum(sizes, 1.0)).astype(LOW)
    gather_start(0, 0, group_view)
    weight_copies(1, w_key_far, w_key)
    weight_copies(2, w_query_far, w_query)
    weight_copies(3, w_value_far, w_value)

    def raise_rows(batch):
        place = tile_of(chip if batch == 0 else 1 - chip, half_rows)
        for j in range(2):
            cut = slice(j * wide_tile, (j + 1) * wide_tile)
            wide[t, place, cut] = dot(group[place, :], w_up[:, cut]).astype(LOW)
            gather_start(wide_chunk(batch, j), 2, wide_view(batch, j))

    gather_finish(0, 0, group_view, (1,))
    weight_wait(0, w_up_far, w_up)
    raise_rows(0)

    far_half = 1 - mine // (seq_size // 2)

    def head_copy(k, h):
        if k >= 6:
            start = half_rows * (7 - k)
            src = outbox.at[3, h, start : start + half_rows]
            place = tile_of(2 * mine + 7 - k, half_rows)
        else:
            a, batch = k // 2, k % 2
            piece = 1 - chip if batch == 0 else chip
            src = outbox.at[a, h, tile_of(piece, half_rows)]
            place = tile_of(2 * mine + piece, half_rows)
        return remote(
            src,
            heads.at[min(k // 2, 3), place],
            out_send.at[k],
            out_recv.at[k],
            {"seq": h},
        )

    def start_head(k, h):
        @pl.when(h != mine)
        def _():
            head_copy(k, h).start()

    def keep_heads(a, h_first, block, start, size):
        for u in range(block.shape[1] // HEAD_DIM):
            h = h_first + u
            part = block[:, u * HEAD_DIM : (u + 1) * HEAD_DIM]

            @pl.when(h == mine)
            def _():
                heads[a, pl.ds(pl.multiple_of(mine * rows + start, size), size), :] = part

            @pl.when(h != mine)
            def _():
                outbox[a, h, pl.ds(pl.multiple_of(start, size), size), :] = part

    def d_attn_tile(upper, jj):
        j = far_half if jj == 0 else 1 - far_half
        start = 0 if upper else half_rows
        acc = jnp.zeros((half_rows, wide_tile), WIDE)
        for q in range(tp_size):
            acc += dot_last(
                wide_grad[q, start : start + half_rows],
                w_out[tile_of(j, wide_tile), q * columns : (q + 1) * columns],
            )
        held = wide_tile // HEAD_DIM
        keep_heads(3, j * held, acc.astype(LOW), start, half_rows)
        if upper:
            for u in range(held):
                start_head(7, j * held + u)

    def d_attn_rows(upper):
        for jj in range(2):
            d_attn_tile(upper, jj)

    def relay_rows(batch):
        for j in range(2):
            gather_relay(wide_chunk(batch, j), 2, wide_view(batch, j))

    def norm_rows(batch):
        place = tile_of(1 - chip if batch == 0 else chip, half_rows)

        def norm_step(q, square):
            piece = wide[q, place].astype(WIDE)
            scaled[q, place] = (piece * gain[:, tile_of(q, columns)]).astype(LOW)
            return square + jnp.sum(piece * piece, 1, keepdims=True)

        square = lax.fori_loop(0, tp_size, norm_step, jnp.zeros((half_rows, 1), WIDE))
        rinv_column[place, :] = lax.rsqrt(square / model_width + EPS)

    def project(a, weight, batch, width):
        piece = 1 - chip if batch == 0 else chip
        place = tile_of(piece, half_rows)
        steps = columns // width
        held = width // HEAD_DIM

        def step(jj, carry):
            j = lax.rem(far_half * (steps // 2) + jj, steps)
            acc = jnp.zeros((half_rows, width), WIDE)
            for q in range(tp_size):
                acc += dot(
                    scaled[q, place], weight[q * columns : (q + 1) * columns, tile_of(j, width)]
                )
            block = (rinv_column[place, :] * acc).astype(LOW)
            keep_heads(a, j * held, block, piece * half_rows, half_rows)
            for u in range(held):
                start_head(2 * a + batch, j * held + u)
            return carry

        lax.fori_loop(0, steps, step, 0)

    gather_relay(1, 1, grad_views[0])
    gather_relay(0, 0, group_view)
    weight_wait(4, w_out_far, w_out)
    gather_finish(1, 1, grad_views[0])
    d_attn_tile(1, 0)
    gather_finish(0, 0, group_view, (2,))
    raise_rows(1)
    near_copies[3].wait()
    relay_rows(0)
    for j in range(2):
        gather_finish(wide_chunk(0, j), 2, wide_view(0, j), (2,))
        gather_finish(wide_chunk(1, j), 2, wide_view(1, j), (1,))
    norm_rows(0)
    weight_wait(1, w_key_far, w_key)
    project(1, w_key, 0, tile)
    d_attn_tile(1, 1)
    relay_rows(1)
    gather_start(6, 1, grad_views[1])
    weight_wait(2, w_query_far, w_query)
    project(0, w_query, 0, wide_tile)
    weight_wait(3, w_value_far, w_value)
    project(2, w_value, 0, wide_tile)
    for j in range(2):
        gather_finish(wide_chunk(0, j), 2, wide_view(0, j), (1,))
        gather_finish(wide_chunk(1, j), 2, wide_view(1, j), (2,))
    norm_rows(1)
    project(1, w_key, 1, wide_tile)
    project(0, w_query, 1, wide_tile)
    gather_relay(6, 1, grad_views[1])
    project(2, w_value, 1, wide_tile)
    gather_finish(6, 1, grad_views[1])

    d_attn_rows(0)

    def heads_arrived(k):
        place = heads.at[min(k // 2, 3), : half_rows * (seq_size - 1)]
        remote(place, place, out_send.at[k], out_recv.at[k], {"seq": mine}).wait_recv()

    def turn(weight):
        def turn_square(q, carry):
            square = weight.at[tile_of(q, columns)]
            square[...] = square[...].T
            return carry

        lax.fori_loop(0, tp_size, turn_square, 0)

    index = lax.broadcasted_iota(jnp.int32, (patches_total, shards), 0)
    lane = lax.broadcasted_iota(jnp.int32, (patches_total, shards), 1)
    owner = jnp.where((index >= lane * cap) & (index < lane * cap + cap), 1.0, 0.0).astype(LOW)
    valid = jnp.where(starts[...].astype(WIDE) < limit, 1.0, 0.0).astype(LOW)
    spread = dot(owner, valid)
    slots = lax.broadcasted_iota(jnp.int32, (patches_total, cap), 1)
    places_in = lax.broadcasted_iota(jnp.int32, (patches_total, cap), 0)
    valid_column = jnp.sum(
        jnp.where(jnp.bitwise_and(places_in, cap - 1) == slots, spread, 0.0), 1, keepdims=True
    )
    key_bias[...] = jnp.broadcast_to((valid_column - 1.0) * -NEG, key_bias.shape)
    for k in (2, 3, 0):
        heads_arrived(k)
    for step in range(seq_size):
        start_head(6, lax.rem(far_half * (seq_size // 2) + step, seq_size))
    turn(w_key)
    heads_arrived(1)

    blocks = patches_total // tile
    own_columns = tile_of(mine, HEAD_DIM)

    def piece_of(k):
        if k < 2:
            return k, 0, rows
        return 2 + k % 2, half_rows * (k // 2 - 1), half_rows

    half_seq = seq_size // 2
    near_half = mine // half_seq

    def return_copy(k, peer):
        a, start, size = piece_of(k)
        return remote(
            returns.at[a, pl.ds(peer * rows + start, size)],
            back.at[a, start : start + size, own_columns],
            back_send.at[k],
            back_recv.at[k, jnp.where(peer // half_seq == near_half, 0, 1)],
            {"seq": peer},
        )

    def send_back(k, i):
        a, start, size = piece_of(k)
        for peer in range(i * tile // rows, (i + 1) * tile // rows):

            @pl.when(peer != mine)
            def _():
                return_copy(k, peer).start()

            @pl.when(peer == mine)
            def _():
                first = peer * rows + start
                back[a, start : start + size, own_columns] = returns[a, first : first + size, :]

    def sent_back(k):
        a, start, size = piece_of(k)
        sent = returns.at[a, : size * (seq_size - 1)]
        remote(sent, sent, back_send.at[k], back_recv.at[k, 0], {"seq": mine}).wait_send()

    def cut_of(i):
        return slice(i * tile, (i + 1) * tile)

    def score_cut(i, j):
        return cut_of(i * (i + 1) // 2 + j)

    for j in range(blocks):
        key_turned[:, cut_of(j)] = heads[1, cut_of(j), :].astype(WIDE).T.astype(LOW)

    def attend(i):
        peak = jnp.full((1, tile), NEG, WIDE)
        for j in range(i + 1):
            score = dot_last(heads[1, cut_of(j), :], heads[0, cut_of(i), :]) * scale
            bias = key_bias[cut_of(j), :]
            score += jnp.concatenate([bias] * (tile // bias.shape[1]), 1)
            if i == j:
                key = lax.broadcasted_iota(jnp.int32, (tile, tile), 0)
                query = lax.broadcasted_iota(jnp.int32, (tile, tile), 1)
                score = jnp.where(key <= query, score, NEG)
            scores[score_cut(i, j), :] = score
            peak = jnp.maximum(peak, jnp.max(score, 0, keepdims=True))
        total = jnp.zeros((1, tile), WIDE)
        for j in range(i + 1):
            expo = jnp.exp(scores[score_cut(i, j), :] - peak)
            scores[score_cut(i, j), :] = expo
            total += jnp.sum(expo, 0, keepdims=True)
        share_row[:, cut_of(i)] = 1.0 / total

    def mix(i):
        mixed = jnp.zeros((HEAD_DIM, tile), WIDE)
        for j in range(i + 1):
            mixed += dot(value_turned[:, cut_of(j)], scores[score_cut(i, j), :].astype(LOW))
        attn = (mixed * share_row[:, cut_of(i)]).astype(LOW).astype(WIDE)
        attn_turned[:, cut_of(i)] = attn
        returns[0, cut_of(i), :] = attn.T.astype(LOW)

    def attend_back(i):
        grad = heads[3, cut_of(i), :]
        delta = jnp.sum(grad.astype(WIDE).T * attn_turned[:, cut_of(i)], 0, keepdims=True)
        share = share_row[:, cut_of(i)]
        query_sum = jnp.zeros((HEAD_DIM, tile), WIDE)
        for j in range(i + 1):
            d_probs = dot_last(heads[2, cut_of(j), :], grad)
            probs = scores[score_cut(i, j), :] * share
            d_scores = (probs * (d_probs - delta)).astype(LOW)
            value_part = dot(probs.astype(LOW), grad)
            key_part = dot(d_scores, heads[0, cut_of(i), :])
            query_sum += dot(key_turned[:, cut_of(j)], d_scores)
            if i < blocks - 1:
                value_part += value_sum[cut_of(j), :]
                key_part += key_sum[cut_of(j), :]
            if i == j:
                returns[2, cut_of(j), :] = value_part.astype(LOW)
                returns[3, cut_of(j), :] = (key_part * scale).astype(LOW)
            else:
                value_sum[cut_of(j), :] = value_part
                key_sum[cut_of(j), :] = key_part
        returns[1, cut_of(i), :] = (query_sum * scale).T.astype(LOW)

    ends = [0] + list(reversed(range(1, blocks)))
    for i in range(blocks):
        attend(i)
    for k in (4, 5):
        heads_arrived(k)
    for j in range(blocks):
        value_turned[:, cut_of(j)] = heads[2, cut_of(j), :].astype(WIDE).T.astype(LOW)
    for i in ends:
        mix(i)
        send_back(0, i)
    heads_arrived(7)
    heads_arrived(6)
    for i in reversed(range(blocks)):
        attend_back(i)
    for i in range(blocks):
        send_back(1, i)
    turn(w_value)
    sent_back(0)
    for k in (2, 3):
        for i in range(blocks):
            send_back(k, i)
    turn(w_query)

    def returns_arrived(k, sides=(0, 1)):
        a, start, size = piece_of(k)
        for side in sides:
            place = returns.at[a, : size * (half_seq - 1 + side)]
            remote(
                place, place, back_send.at[k], back_recv.at[k, side], {"seq": mine}
            ).wait_recv()

    order = (
        (1 - chip) * 2 + (1 - core),
        (1 - chip) * 2 + core,
        chip * 2 + (1 - core),
        chip * 2 + core,
    )
    stages = ((0, slice(0, rows)), (1, slice(0, half_rows)), (1, slice(half_rows, rows)))

    def pair_copy(stage, k):
        a, part = stages[stage]
        return remote(
            partial.at[a, order[2 * k], part],
            pair_in.at[a, k, part],
            pair_send.at[stage],
            pair_recv.at[stage, k],
            {"tp": partner},
        )

    def cross_copy(stage):
        a, part = stages[stage]
        return remote(
            cross_out.at[a, part],
            cross_in.at[a, part],
            cross_send.at[stage],
            cross_recv.at[stage],
            {"tp": across},
        )

    def cross_over(stage):
        a, part = stages[stage]
        pair_copy(stage, 0).wait_recv()
        cross_out[a, part] = (
            partial[a, order[1], part].astype(WIDE) + pair_in[a, 0, part].astype(WIDE)
        ).astype(LOW)
        cross_copy(stage).start()

    def summed(stage):
        a, part = stages[stage]
        pair_copy(stage, 1).wait_recv()
        cross_copy(stage).wait_recv()
        return (
            partial[a, t, part].astype(WIDE)
            + pair_in[a, 1, part].astype(WIDE)
            + cross_in[a, part].astype(WIDE)
        )

    returns_arrived(0)
    for k in range(tp_size):
        quarter = order[k]

        for j in range(2):
            at = tile_of(quarter * 2 + j, wide_tile)
            here = slice(j * wide_tile, (j + 1) * wide_tile)
            partial[0, quarter, :, here] = dot(back[0], w_out[:, at]).astype(LOW)
        if k % 2 == 0:
            pair_copy(0, k // 2).start()
    def dots_copy(half, offset):
        return remote(
            dots_out.at[half],
            dots_in.at[half, offset],
            dots_send.at[half],
            dots_recv.at[half],
            {"tp": lax.rem(t + offset, tp_size)},
        )

    def share_gradient(half, product):
        stage = 1 + half
        part = stages[stage][1]
        dots = jnp.zeros((half_rows, 1), WIDE)
        for k in range(tp_size):
            quarter = order[k]
            for j in range(2):
                at = tile_of(quarter * 2 + j, wide_tile)
                here = slice(j * wide_tile, (j + 1) * wide_tile)
                whole = product(quarter, here)
                partial[1, quarter, part, here] = whole.astype(LOW)
                inner = gain[:, at] * whole * wide[quarter, part, here].astype(WIDE)
                dots += jnp.sum(inner, 1, keepdims=True)
            if k % 2 == 0:
                pair_copy(stage, k // 2).start()
            if k == 2:
                cross_over(stage)
        dots_out[half] = jnp.broadcast_to(to_row(dots, rows), dots_out.shape[1:])
        for offset in range(1, tp_size):
            dots_copy(half, offset).start()
        return dots

    def finish_gradient(half, dots):
        stage = 1 + half
        part = stages[stage][1]
        place = dots_in.at[half, 1:]
        remote(place, place, dots_send.at[half], dots_recv.at[half], {"tp": t}).wait_recv()
        for offset in range(1, tp_size):
            dots += to_column(dots_in[half, offset, :1], half_rows)
        rinv = rinv_column[part, :]
        out_grad[part, :] = (
            wide_grad[t, part].astype(WIDE)
            + rinv * gain[:, tile_of(t, columns)] * summed(stage)
            - wide[t, part].astype(WIDE) * (rinv**3 * dots / model_width)
        )

    half_columns = columns // 2
    for side in range(2):
        returns_arrived(1, (side,))
        which = near_half if side == 0 else 1 - near_half

        def query_step(quarter, carry):
            at = tile_of(quarter * 2 + which, half_columns)
            for j in range(2):
                here = slice(j * wide_tile, (j + 1) * wide_tile)
                more = dot(back[1, :, tile_of(which, half_columns)], w_query[at, here])
                if side == 0:
                    grad_sum[quarter, :, here] = more
                else:
                    grad_sum[quarter, :, here] += more
            return carry

        lax.fori_loop(0, tp_size, query_step, 0, unroll=2)
        sent_back(1 + side)
        for i in range(blocks):
            send_back(4 + side, i)
        if side == 0:
            cross_over(0)

    def half_gradient(half):
        part = stages[1 + half][1]

        def value_step(quarter, carry):
            for j in range(2):
                here = slice(j * wide_tile, (j + 1) * wide_tile)
                turned = w_value[tile_of(quarter, columns), here]
                grad_sum[quarter, part, here] += dot(back[2, part], turned)
            return carry

        def product(quarter, here):
            turned = w_key[tile_of(quarter, columns), here]
            return grad_sum[quarter, part, here] + dot(back[3, part], turned)

        returns_arrived(2 + 2 * half)
        lax.fori_loop(0, tp_size, value_step, 0, unroll=2)
        returns_arrived(3 + 2 * half)
        return share_gradient(half, product)

    upper_dots = half_gradient(0)
    lower_dots = half_gradient(1)
    out_value[...] = jnp.where(
        row_valid > 0.5, wide[t].astype(WIDE) + summed(0), 0.0
    ).astype(LOW)
    finish_gradient(0, upper_dots)
    finish_gradient(1, lower_dots)

    @pl.when(has_before)
    def _():
        lead_copy.wait_send()

    for kind, sent in ((0, group.at[: 3 * cap]), (1, wide_grad.at[:3]), (2, wide.at[:3])):
        gather_copy(0, 0, kind, sent).wait_send()
    for k in range(8):
        sent = outbox.at[min(k // 2, 3), 1:, :half_rows]
        remote(sent, sent, out_send.at[k], out_recv.at[k], {"seq": mine}).wait_send()
    for k in (3, 4, 5):
        sent_back(k)
    for stage in range(len(stages)):
        a, part = stages[stage]
        sent = pair_in.at[a, :, part]
        remote(
            sent, sent, pair_send.at[stage], pair_recv.at[stage, 0], {"tp": partner}
        ).wait_send()
        cross_copy(stage).wait_send()
    for half in range(2):
        sent = dots_in.at[half, 1:]
        remote(sent, sent, dots_send.at[half], dots_recv.at[half], {"tp": t}).wait_send()


def per_device_whole(encoded, starts, w_up, norm_gain, w_query, w_key, w_value, w_out, cotangent):
    seq_size, tp_size = lax.axis_size("seq"), lax.axis_size("tp")
    rows, columns = cotangent.shape
    model_width = norm_gain.shape[0]
    byte_width = encoded.shape[1]
    cap = starts.shape[1]
    total = starts.size
    tile = 2 * HEAD_DIM
    blocks = total // tile
    dma = pltpu.SemaphoreType.DMA
    scratch = [
        pltpu.VMEM(starts.shape, jnp.int32),
        pltpu.VMEM((1, model_width), WIDE),
        pltpu.VMEM(encoded.shape, LOW),
        pltpu.VMEM(cotangent.shape, LOW),
        pltpu.VMEM(w_up.shape, LOW),
        pltpu.VMEM(w_query.shape, LOW),
        pltpu.VMEM(w_key.shape, LOW),
        pltpu.VMEM(w_value.shape, LOW),
        pltpu.VMEM(w_out.shape, LOW),
        pltpu.VMEM((1, byte_width), WIDE),
        pltpu.VMEM((1, byte_width), WIDE),
        pltpu.VMEM((rows, byte_width), LOW),
        pltpu.VMEM((tp_size, rows, columns), LOW),
        pltpu.VMEM((tp_size, rows, columns), LOW),
        pltpu.VMEM((tp_size, rows, columns), LOW),
        pltpu.VMEM((total, 128), WIDE),
        pltpu.VMEM((rows, 1), WIDE),
        pltpu.VMEM((4, seq_size, rows, HEAD_DIM), LOW),
        pltpu.VMEM((4, total, HEAD_DIM), LOW),
        pltpu.VMEM((HEAD_DIM, total), LOW),
        pltpu.VMEM((HEAD_DIM, total), LOW),
        pltpu.VMEM((blocks * (blocks + 1) // 2 * tile, tile), WIDE),
        pltpu.VMEM((HEAD_DIM, total), WIDE),
        pltpu.VMEM((1, total), WIDE),
        pltpu.VMEM((total, HEAD_DIM), WIDE),
        pltpu.VMEM((total, HEAD_DIM), WIDE),
        pltpu.VMEM((4, total, HEAD_DIM), LOW),
        pltpu.VMEM((4, rows, columns), LOW),
        pltpu.VMEM((tp_size, rows, columns), WIDE),
        pltpu.VMEM((2, tp_size, rows, columns), LOW),
        pltpu.VMEM((2, 2, rows, columns), LOW),
        pltpu.VMEM((2, rows, columns), LOW),
        pltpu.VMEM((2, rows, columns), LOW),
        pltpu.VMEM((2, 8, rows), WIDE),
        pltpu.VMEM((2, tp_size, 8, rows), WIDE),
        dma((5,)),
        dma((4,)),
        dma((2,)),
        dma((3,)),
        dma((3, 7)),
        dma((8,)),
        dma((8,)),
        dma((6,)),
        dma((6, 2)),
        dma((3,)),
        dma((3, 2)),
        dma((3,)),
        dma((3,)),
        dma((2,)),
        dma((2,)),
    ]
    near = pl.BlockSpec(memory_space=pltpu.VMEM)
    far = pl.BlockSpec(memory_space=pl.ANY)
    return tuple(
        pl.pallas_call(
            functools.partial(layer_kernel, seq_size, tp_size),
            out_shape=[
                pltpu.VMEM((rows, columns), LOW),
                pltpu.VMEM((rows, columns), WIDE),
            ],
            in_specs=[far] * 9,
            out_specs=[near] * 2,
            scratch_shapes=scratch,
            compiler_params=pltpu.CompilerParams(
                collective_id=0, has_side_effects=True, vmem_limit_bytes=60 * 1024 * 1024
            ),
        )(
            starts,
            norm_gain.reshape(1, model_width),
            encoded,
            cotangent,
            w_up,
            w_query,
            w_key,
            w_value,
            w_out,
        )
    )


def fits_one_kernel(arrays):
    encoded, starts, w_up, norm_gain, w_query, w_key, w_value, w_out, cotangent = arrays
    seq_size, tp_size = lax.axis_size("seq"), lax.axis_size("tp")
    rows, columns = cotangent.shape
    cap = starts.shape[1]
    return (
        tp_size == 4
        and seq_size % 2 == 0
        and columns == seq_size * HEAD_DIM
        and rows == HEAD_DIM
        and rows == tp_size * cap
        and cap & (cap - 1) == 0
        and cap % 16 == 0
        and columns % (4 * HEAD_DIM) == 0
        and norm_gain.shape[0] == tp_size * columns
        and starts.shape[0] == seq_size * tp_size
        and starts.size % (2 * HEAD_DIM) == 0
    )


def solution(mesh):
    in_specs = (
        P(("seq", "tp"), None),
        P(),
        P(None, "tp"),
        P(),
        P(None, "tp"),
        P(None, "tp"),
        P(None, "tp"),
        P("tp", None),
        P("seq", "tp"),
    )
    out_specs = (P("seq", "tp"), P("seq", "tp"))

    def choose(*arrays):
        return (per_device_whole if fits_one_kernel(arrays) else per_device)(*arrays)

    return jax.shard_map(
        choose, mesh=mesh, in_specs=in_specs, out_specs=out_specs, check_vma=False
    )
```

```python
import functools

import jax
import jax.numpy as jnp
from jax import lax
from jax.experimental import pallas as pl
from jax.experimental.pallas import tpu as pltpu
from jax.sharding import PartitionSpec as P

HEAD_DIM = 128


EPS = 1e-05
NEG = -1e30
CONTRACT_LAST = (((1,), (1,)), ((), ()))


def shifted(block, axis, distance):
    devices = range(lax.axis_size(axis))
    route = [(i - distance, i) for i in devices if i - distance in devices]
    return lax.ppermute(block, axis, route)


def per_device(encoded, starts, w_up, norm_gain, w_query, w_key, w_value, w_out, cotangent):
    byte_rows = encoded.shape[0]
    patch_cap = starts.shape[1]
    model_width = norm_gain.shape[0]
    shard = lax.axis_index(("seq", "tp"))
    own_starts = lax.dynamic_slice_in_dim(starts, shard, 1, 0)[0]
    places = jnp.arange(byte_rows, dtype=jnp.int32)
    following = jnp.concatenate([own_starts[1:], jnp.full((1,), byte_rows, jnp.int32)])
    inside = (places[None, :] >= own_starts[:, None]) & (places[None, :] < following[:, None])
    sums = jnp.dot(inside.astype(jnp.bfloat16), encoded, preferred_element_type=jnp.float32)
    sizes = jnp.sum(inside.astype(jnp.float32), 1)
    leading = places[None, :] < own_starts[:1, None]
    lead_sum = jnp.dot(leading.astype(jnp.bfloat16), encoded, preferred_element_type=jnp.float32)
    lead_size = jnp.sum(leading.astype(jnp.float32), 1)
    next_sum, next_size = shifted((lead_sum, lead_size), ("seq", "tp"), -1)
    count = jnp.sum((own_starts < byte_rows).astype(jnp.int32))
    last_slot = (jnp.arange(patch_cap, dtype=jnp.int32) == count - 1).astype(jnp.float32)
    sums = sums + last_slot[:, None] * next_sum
    sizes = sizes + last_slot * next_size
    patches = (sums / jnp.maximum(sizes, 1.0)[:, None]).astype(jnp.bfloat16)
    group = lax.all_gather(patches, "tp", axis=0, tiled=True)
    latent_in = jnp.dot(group, w_up, preferred_element_type=jnp.float32).astype(jnp.bfloat16)
    group_rows, columns = latent_in.shape
    head_count = columns // HEAD_DIM
    wide_piece = lax.all_gather(latent_in, "tp", axis=1, tiled=True).astype(jnp.float32)
    scaled = (wide_piece * norm_gain[None, :]).astype(jnp.bfloat16)
    acc_query = jnp.dot(scaled, w_query, preferred_element_type=jnp.float32)
    acc_key = jnp.dot(scaled, w_key, preferred_element_type=jnp.float32)
    acc_value = jnp.dot(scaled, w_value, preferred_element_type=jnp.float32)
    acc_query, acc_key, acc_value, square = (
        acc_query,
        acc_key,
        acc_value,
        jnp.sum(wide_piece * wide_piece, 1),
    )
    rinv = lax.rsqrt(square / model_width + EPS)
    query = (rinv[:, None] * acc_query).astype(jnp.bfloat16)
    key_rows = (rinv[:, None] * acc_key).astype(jnp.bfloat16)
    value_rows = (rinv[:, None] * acc_value).astype(jnp.bfloat16)
    keys_all, values_all = (
        lax.all_gather(key_rows, "seq", axis=0, tiled=True),
        lax.all_gather(value_rows, "seq", axis=0, tiled=True),
    )
    patches_total = keys_all.shape[0]
    valid_all = (starts < byte_rows).reshape(patches_total)
    row_base = lax.axis_index("seq") * group_rows
    query_index = row_base + jnp.arange(group_rows, dtype=jnp.int32)
    key_index = jnp.arange(patches_total, dtype=jnp.int32)
    query_valid = lax.dynamic_slice_in_dim(valid_all, row_base, group_rows, 0)
    allowed = valid_all[None, :] & (key_index[None, :] <= query_index[:, None])
    scale = HEAD_DIM ** (-0.5)
    query_heads = query.reshape(group_rows, head_count, HEAD_DIM)
    key_heads = keys_all.reshape(patches_total, head_count, HEAD_DIM)
    value_heads = values_all.reshape(patches_total, head_count, HEAD_DIM)
    scores = (
        jnp.einsum("rhd,khd->hrk", query_heads, key_heads, preferred_element_type=jnp.float32)
        * scale
    )
    peak = jnp.max(jnp.where(allowed[None], scores, NEG), 2)
    expo = jnp.where(allowed[None], jnp.exp(scores - peak[:, :, None]), 0.0)
    total = jnp.sum(expo, 2)
    mixed = jnp.einsum(
        "hrk,khd->rhd", expo.astype(jnp.bfloat16), value_heads, preferred_element_type=jnp.float32
    )
    attn = (mixed / total.T[:, :, None]).astype(jnp.bfloat16)
    partial_value = jnp.dot(
        attn.reshape(group_rows, columns), w_out, preferred_element_type=jnp.float32
    )
    head_sum = lax.psum_scatter(
        partial_value.astype(jnp.bfloat16), "tp", scatter_dimension=1, tiled=True
    ).astype(jnp.float32)
    wide_in = latent_in.astype(jnp.float32)
    latent_out = jnp.where(query_valid[:, None], wide_in + head_sum, 0.0).astype(jnp.bfloat16)
    grad_out = jnp.where(query_valid[:, None], cotangent, jnp.zeros_like(cotangent))
    d_attn = lax.dot_general(
        lax.all_gather(grad_out, "tp", axis=1, tiled=True),
        w_out,
        CONTRACT_LAST,
        preferred_element_type=jnp.float32,
    ).astype(jnp.bfloat16)
    grad_heads = d_attn.reshape(group_rows, head_count, HEAD_DIM)
    delta = jnp.sum(grad_heads.astype(jnp.float32) * attn.astype(jnp.float32), 2).T
    probs = expo / total[:, :, None]
    d_probs = jnp.einsum(
        "rhd,khd->hrk", grad_heads, value_heads, preferred_element_type=jnp.float32
    )
    d_scores = (probs * (d_probs - delta[:, :, None])).astype(jnp.bfloat16)
    grad_query = (
        (
            jnp.einsum("hrk,khd->rhd", d_scores, key_heads, preferred_element_type=jnp.float32)
            * scale
        )
        .astype(jnp.bfloat16)
        .reshape(group_rows, columns)
    )
    weights_low = probs.astype(jnp.bfloat16)
    count_rows = group_rows * lax.axis_size("seq")
    key_part = jnp.einsum("hrk,rhd->khd", d_scores, query_heads, preferred_element_type=jnp.float32)
    value_part = jnp.einsum(
        "hrk,rhd->khd", weights_low, grad_heads, preferred_element_type=jnp.float32
    )
    both = lax.psum_scatter(
        jnp.concatenate(
            [key_part.reshape(count_rows, columns), value_part.reshape(count_rows, columns)], 1
        ).astype(jnp.bfloat16),
        "seq",
        scatter_dimension=0,
        tiled=True,
    ).astype(jnp.float32)
    grad_key = (both[:, :columns] * scale).astype(jnp.bfloat16)
    grad_value = both[:, columns:].astype(jnp.bfloat16)
    dnormed = (
        lax.dot_general(grad_query, w_query, CONTRACT_LAST, preferred_element_type=jnp.float32)
        + lax.dot_general(grad_key, w_key, CONTRACT_LAST, preferred_element_type=jnp.float32)
        + lax.dot_general(grad_value, w_value, CONTRACT_LAST, preferred_element_type=jnp.float32)
    )
    normed_grad = lax.psum_scatter(
        dnormed.astype(jnp.bfloat16), "tp", scatter_dimension=1, tiled=True
    ).astype(jnp.float32)
    gain_own = lax.dynamic_slice_in_dim(norm_gain, lax.axis_index("tp") * columns, columns, 0)
    dots = lax.psum(jnp.sum(gain_own[None, :] * normed_grad * wide_in, 1), "tp")
    latent_grad = (
        grad_out.astype(jnp.float32)
        + rinv[:, None] * gain_own[None, :] * normed_grad
        - wide_in * (rinv**3)[:, None] * dots[:, None] / model_width
    )
    return (latent_out, latent_grad)


MESH = pl.DeviceIdType.MESH
LOW = jnp.bfloat16
WIDE = jnp.float32
ROWS_FIRST = (((0,), (0,)), ((), ()))


def tile_of(index, size):
    return pl.ds(pl.multiple_of(index * size, size), size)


def dot(a, b):
    return jnp.dot(a, b, preferred_element_type=WIDE)


def dot_last(a, b):
    return lax.dot_general(a, b, CONTRACT_LAST, preferred_element_type=WIDE)


def to_row(column, lanes):
    n = column.shape[0]
    down = lax.broadcasted_iota(jnp.int32, (n, lanes), 0)
    across = lax.broadcasted_iota(jnp.int32, (n, lanes), 1)
    return jnp.sum(jnp.where(down == across, column, 0.0), 0, keepdims=True)


def to_column(row, n, shift=0):
    lanes = row.shape[1]
    down = lax.broadcasted_iota(jnp.int32, (n, lanes), 0)
    across = lax.broadcasted_iota(jnp.int32, (n, lanes), 1)
    return jnp.sum(jnp.where(down + shift == across, row, 0.0), 1, keepdims=True)


def layer_kernel(
    seq_size,
    tp_size,
    starts_far,
    gain_far,
    encoded_far,
    cotangent_far,
    w_up_far,
    w_query_far,
    w_key_far,
    w_value_far,
    w_out_far,
    out_value,
    out_grad,
    starts,
    gain,
    encoded,
    cotangent,
    w_up,
    w_query,
    w_key,
    w_value,
    w_out,
    lead_out,
    lead_in,
    group,
    wide,
    wide_grad,
    scaled,
    key_bias,
    rinv_column,
    outbox,
    heads,
    value_turned,
    key_turned,
    scores,
    attn_turned,
    share_row,
    key_sum,
    value_sum,
    returns,
    back,
    grad_sum,
    partial,
    pair_in,
    cross_out,
    cross_in,
    dots_out,
    dots_in,
    weight_sem,
    near_sem,
    lead_sem,
    gather_send,
    gather_recv,
    out_send,
    out_recv,
    back_send,
    back_recv,
    pair_send,
    pair_recv,
    cross_send,
    cross_recv,
    dots_send,
    dots_recv,
):
    byte_rows, byte_width = encoded.shape
    shards, cap = starts.shape
    rows, columns = cotangent.shape
    model_width = gain.shape[1]
    patches_total = shards * cap
    mine = lax.axis_index("seq")
    t = lax.axis_index("tp")
    chip, core = t // 2, lax.rem(t, 2)
    shard = mine * tp_size + t
    partner = t + 1 - 2 * core
    across = lax.rem(t + 2, tp_size)
    diagonal = lax.rem(partner + 2, tp_size)
    tile = 2 * HEAD_DIM
    tiles = columns // tile
    scale = HEAD_DIM ** (-0.5)

    def remote(src, dst, send, recv, device):
        return pltpu.make_async_remote_copy(
            src_ref=src,
            dst_ref=dst,
            send_sem=send,
            recv_sem=recv,
            device_id=device,
            device_id_type=MESH,
        )

    barrier = pltpu.get_barrier_semaphore()
    for offset in range(1, tp_size):
        pl.semaphore_signal(
            barrier, inc=1, device_id={"tp": lax.rem(t + offset, tp_size)}, device_id_type=MESH
        )
    for offset in range(1, seq_size):
        pl.semaphore_signal(
            barrier, inc=1, device_id={"seq": lax.rem(mine + offset, seq_size)}, device_id_type=MESH
        )
    has_before = shard > 0
    has_after = shard < shards - 1
    group_first = jnp.logical_and(t == 0, has_before)
    group_last = jnp.logical_and(t == tp_size - 1, has_after)
    shard_before = {
        "seq": jnp.where(t == 0, lax.rem(mine + seq_size - 1, seq_size), mine),
        "tp": lax.rem(t + tp_size - 1, tp_size),
    }
    shard_after = {
        "seq": jnp.where(t == tp_size - 1, lax.rem(mine + 1, seq_size), mine),
        "tp": lax.rem(t + 1, tp_size),
    }

    @pl.when(group_first)
    def _():
        pl.semaphore_signal(barrier, inc=1, device_id=shard_before, device_id_type=MESH)

    @pl.when(group_last)
    def _():
        pl.semaphore_signal(barrier, inc=1, device_id=shard_after, device_id_type=MESH)

    near_copies = [
        pltpu.make_async_copy(starts_far, starts, near_sem.at[0]),
        pltpu.make_async_copy(encoded_far, encoded, near_sem.at[1]),
        pltpu.make_async_copy(cotangent_far, cotangent, near_sem.at[2]),
        pltpu.make_async_copy(gain_far, gain, near_sem.at[3]),
    ]
    for copy in near_copies:
        copy.start()
    pieces = 4

    def weight_copies(i, far, near):
        depth = far.shape[0] // pieces
        for p in range(pieces):
            part = pl.ds(p * depth, depth)
            pltpu.make_async_copy(far.at[part], near.at[part], weight_sem.at[i]).start()

    def weight_wait(i, far, near):
        pltpu.make_async_copy(far, near, weight_sem.at[i]).wait()

    near_copies[0].wait()
    limit = float(byte_rows)
    own = starts[pl.ds(shard, 1), :].astype(WIDE)
    after = starts[pl.ds(jnp.minimum(shard + 1, shards - 1), 1), :].astype(WIDE)
    first = to_column(own, cap)
    slot = lax.broadcasted_iota(jnp.int32, (cap, 1), 0)
    following = to_column(own, cap, 1) + jnp.where(slot == cap - 1, limit, 0.0)
    places = lax.broadcasted_iota(jnp.int32, (cap, byte_rows), 1).astype(WIDE)
    inside = jnp.where((places >= first) & (places < following), 1.0, 0.0).astype(LOW)
    lead_places = lax.broadcasted_iota(jnp.int32, (16, byte_rows), 1).astype(WIDE)
    leading = jnp.where(lead_places < own[:, :1], 1.0, 0.0).astype(LOW)
    near_copies[1].wait()
    weight_copies(0, w_up_far, w_up)
    weight_copies(4, w_out_far, w_out)
    lead_out[...] = dot(leading, encoded[...])[:1]
    sums = dot(inside, encoded[...])

    own_rows = tile_of(mine, rows)
    own_starts = [
        to_column(starts[pl.ds(mine * tp_size + u, 1), :].astype(WIDE), cap)
        for u in range(tp_size)
    ]
    row_valid = jnp.where(jnp.concatenate(own_starts, 0) < limit, 1.0, 0.0)
    near_copies[2].wait()
    wide_grad[t] = jnp.where(row_valid > 0.5, cotangent[...].astype(WIDE), 0.0).astype(LOW)

    neighbours = group_first.astype(jnp.int32) + group_last.astype(jnp.int32)
    pl.semaphore_wait(barrier, tp_size + seq_size - 2 + neighbours)

    lead_copy = remote(lead_out, lead_in, lead_sem.at[0], lead_sem.at[1], shard_before)

    @pl.when(has_before)
    def _():
        lead_copy.start()

    def gather_copy(way, k, kind, piece):
        target = across if way == 0 else partner
        return remote(
            piece, piece, gather_send.at[kind], gather_recv.at[way, k], {"tp": target}
        )

    def gather_start(k, kind, view):
        gather_copy(0, k, kind, view(t)).start()
        gather_copy(1, k, kind, view(t)).start()

    def gather_relay(k, kind, view):
        gather_copy(0, k, kind, view(across)).wait_recv()
        gather_copy(2, k, kind, view(across)).start()

    def gather_finish(k, kind, view, ways=(1, 2)):
        for way in ways:
            gather_copy(way, k, kind, view(partner if way == 1 else diagonal)).wait_recv()

    half_rows = rows // 2
    grad_views = (
        lambda q: wide_grad.at[q, :half_rows],
        lambda q: wide_grad.at[q, half_rows:],
    )
    gather_start(1, 1, grad_views[0])

    group_view = lambda q: group.at[tile_of(q, cap)]
    wide_tile = columns // 2

    def wide_view(batch, j):
        def view(q):
            of_chip = q // 2
            place = of_chip if batch == 0 else 1 - of_chip
            return wide.at[
                q, tile_of(place, half_rows), j * wide_tile : (j + 1) * wide_tile
            ]

        return view

    def wide_chunk(batch, j):
        return 2 + 2 * batch + j

    @pl.when(has_after)
    def _():
        lead_copy.wait_recv()

    joined = jnp.where(
        jnp.logical_and(first < limit, following >= limit), jnp.where(has_after, 1.0, 0.0), 0.0
    )
    sums = sums + joined * jnp.where(has_after, lead_in[...], 0.0)
    sizes = (following - first) * jnp.where(first < limit, 1.0, 0.0) + joined * after[:, :1]
    group[tile_of(t, cap), :] = (sums / jnp.maximum(sizes, 1.0)).astype(LOW)
    gather_start(0, 0, group_view)
    weight_copies(1, w_key_far, w_key)
    weight_copies(2, w_query_far, w_query)
    weight_copies(3, w_value_far, w_value)

    def raise_rows(batch):
        place = tile_of(chip if batch == 0 else 1 - chip, half_rows)
        for j in range(2):
            cut = slice(j * wide_tile, (j + 1) * wide_tile)
            wide[t, place, cut] = dot(group[place, :], w_up[:, cut]).astype(LOW)
            gather_start(wide_chunk(batch, j), 2, wide_view(batch, j))

    gather_finish(0, 0, group_view, (1,))
    weight_wait(0, w_up_far, w_up)
    raise_rows(0)

    far_half = 1 - mine // (seq_size // 2)

    def head_copy(k, h):
        if k >= 6:
            start = half_rows * (7 - k)
            src = outbox.at[3, h, start : start + half_rows]
            place = tile_of(2 * mine + 7 - k, half_rows)
        else:
            a, batch = k // 2, k % 2
            piece = 1 - chip if batch == 0 else chip
            src = outbox.at[a, h, tile_of(piece, half_rows)]
            place = tile_of(2 * mine + piece, half_rows)
        return remote(
            src,
            heads.at[min(k // 2, 3), place],
            out_send.at[k],
            out_recv.at[k],
            {"seq": h},
        )

    def start_head(k, h):
        @pl.when(h != mine)
        def _():
            head_copy(k, h).start()

    def keep_heads(a, h_first, block, start, size):
        for u in range(block.shape[1] // HEAD_DIM):
            h = h_first + u
            part = block[:, u * HEAD_DIM : (u + 1) * HEAD_DIM]

            @pl.when(h == mine)
            def _():
                heads[a, pl.ds(pl.multiple_of(mine * rows + start, size), size), :] = part

            @pl.when(h != mine)
            def _():
                outbox[a, h, pl.ds(pl.multiple_of(start, size), size), :] = part

    def d_attn_tile(upper, jj):
        j = far_half if jj == 0 else 1 - far_half
        start = 0 if upper else half_rows
        acc = jnp.zeros((half_rows, wide_tile), WIDE)
        for q in range(tp_size):
            acc += dot_last(
                wide_grad[q, start : start + half_rows],
                w_out[tile_of(j, wide_tile), q * columns : (q + 1) * columns],
            )
        held = wide_tile // HEAD_DIM
        keep_heads(3, j * held, acc.astype(LOW), start, half_rows)
        if upper:
            for u in range(held):
                start_head(7, j * held + u)

    def d_attn_rows(upper):
        for jj in range(2):
            d_attn_tile(upper, jj)

    def relay_rows(batch):
        for j in range(2):
            gather_relay(wide_chunk(batch, j), 2, wide_view(batch, j))

    def norm_rows(batch):
        place = tile_of(1 - chip if batch == 0 else chip, half_rows)

        def norm_step(q, square):
            piece = wide[q, place].astype(WIDE)
            scaled[q, place] = (piece * gain[:, tile_of(q, columns)]).astype(LOW)
            return square + jnp.sum(piece * piece, 1, keepdims=True)

        square = lax.fori_loop(0, tp_size, norm_step, jnp.zeros((half_rows, 1), WIDE))
        rinv_column[place, :] = lax.rsqrt(square / model_width + EPS)

    def project(a, weight, batch, width):
        piece = 1 - chip if batch == 0 else chip
        place = tile_of(piece, half_rows)
        steps = columns // width
        held = width // HEAD_DIM

        def step(jj, carry):
            j = lax.rem(far_half * (steps // 2) + jj, steps)
            acc = jnp.zeros((half_rows, width), WIDE)
            for q in range(tp_size):
                acc += dot(
                    scaled[q, place], weight[q * columns : (q + 1) * columns, tile_of(j, width)]
                )
            block = (rinv_column[place, :] * acc).astype(LOW)
            keep_heads(a, j * held, block, piece * half_rows, half_rows)
            for u in range(held):
                start_head(2 * a + batch, j * held + u)
            return carry

        lax.fori_loop(0, steps, step, 0)

    gather_relay(1, 1, grad_views[0])
    gather_relay(0, 0, group_view)
    weight_wait(4, w_out_far, w_out)
    gather_finish(1, 1, grad_views[0])
    d_attn_tile(1, 0)
    gather_finish(0, 0, group_view, (2,))
    raise_rows(1)
    near_copies[3].wait()
    relay_rows(0)
    for j in range(2):
        gather_finish(wide_chunk(0, j), 2, wide_view(0, j), (2,))
        gather_finish(wide_chunk(1, j), 2, wide_view(1, j), (1,))
    norm_rows(0)
    weight_wait(1, w_key_far, w_key)
    project(1, w_key, 0, tile)
    d_attn_tile(1, 1)
    relay_rows(1)
    gather_start(6, 1, grad_views[1])
    weight_wait(2, w_query_far, w_query)
    project(0, w_query, 0, wide_tile)
    weight_wait(3, w_value_far, w_value)
    project(2, w_value, 0, wide_tile)
    for j in range(2):
        gather_finish(wide_chunk(0, j), 2, wide_view(0, j), (1,))
        gather_finish(wide_chunk(1, j), 2, wide_view(1, j), (2,))
    norm_rows(1)
    project(1, w_key, 1, wide_tile)
    project(0, w_query, 1, wide_tile)
    gather_relay(6, 1, grad_views[1])
    project(2, w_value, 1, wide_tile)
    gather_finish(6, 1, grad_views[1])

    d_attn_rows(0)

    def heads_arrived(k):
        place = heads.at[min(k // 2, 3), : half_rows * (seq_size - 1)]
        remote(place, place, out_send.at[k], out_recv.at[k], {"seq": mine}).wait_recv()

    def turn(weight):
        def turn_square(q, carry):
            square = weight.at[tile_of(q, columns)]
            square[...] = square[...].T
            return carry

        lax.fori_loop(0, tp_size, turn_square, 0)

    index = lax.broadcasted_iota(jnp.int32, (patches_total, shards), 0)
    lane = lax.broadcasted_iota(jnp.int32, (patches_total, shards), 1)
    owner = jnp.where((index >= lane * cap) & (index < lane * cap + cap), 1.0, 0.0).astype(LOW)
    valid = jnp.where(starts[...].astype(WIDE) < limit, 1.0, 0.0).astype(LOW)
    spread = dot(owner, valid)
    slots = lax.broadcasted_iota(jnp.int32, (patches_total, cap), 1)
    places_in = lax.broadcasted_iota(jnp.int32, (patches_total, cap), 0)
    valid_column = jnp.sum(
        jnp.where(jnp.bitwise_and(places_in, cap - 1) == slots, spread, 0.0), 1, keepdims=True
    )
    key_bias[...] = jnp.broadcast_to((valid_column - 1.0) * -NEG, key_bias.shape)
    for k in (2, 3, 0):
        heads_arrived(k)
    for step in range(seq_size):
        start_head(6, lax.rem(far_half * (seq_size // 2) + step, seq_size))
    turn(w_key)
    heads_arrived(1)

    blocks = patches_total // tile
    own_columns = tile_of(mine, HEAD_DIM)

    def piece_of(k):
        if k < 2:
            return k, 0, rows
        return 2 + k % 2, half_rows * (k // 2 - 1), half_rows

    half_seq = seq_size // 2
    near_half = mine // half_seq

    def return_copy(k, peer):
        a, start, size = piece_of(k)
        return remote(
            returns.at[a, pl.ds(peer * rows + start, size)],
            back.at[a, start : start + size, own_columns],
            back_send.at[k],
            back_recv.at[k, jnp.where(peer // half_seq == near_half, 0, 1)],
            {"seq": peer},
        )

    def send_back(k, i):
        a, start, size = piece_of(k)
        for peer in range(i * tile // rows, (i + 1) * tile // rows):

            @pl.when(peer != mine)
            def _():
                return_copy(k, peer).start()

            @pl.when(peer == mine)
            def _():
                first = peer * rows + start
                back[a, start : start + size, own_columns] = returns[a, first : first + size, :]

    def sent_back(k):
        a, start, size = piece_of(k)
        sent = returns.at[a, : size * (seq_size - 1)]
        remote(sent, sent, back_send.at[k], back_recv.at[k, 0], {"seq": mine}).wait_send()

    def cut_of(i):
        return slice(i * tile, (i + 1) * tile)

    def score_cut(i, j):
        return cut_of(i * (i + 1) // 2 + j)

    for j in range(blocks):
        key_turned[:, cut_of(j)] = heads[1, cut_of(j), :].astype(WIDE).T.astype(LOW)

    def attend(i):
        peak = jnp.full((1, tile), NEG, WIDE)
        for j in range(i + 1):
            score = dot_last(heads[1, cut_of(j), :], heads[0, cut_of(i), :]) * scale
            bias = key_bias[cut_of(j), :]
            score += jnp.concatenate([bias] * (tile // bias.shape[1]), 1)
            if i == j:
                key = lax.broadcasted_iota(jnp.int32, (tile, tile), 0)
                query = lax.broadcasted_iota(jnp.int32, (tile, tile), 1)
                score = jnp.where(key <= query, score, NEG)
            scores[score_cut(i, j), :] = score
            peak = jnp.maximum(peak, jnp.max(score, 0, keepdims=True))
        total = jnp.zeros((1, tile), WIDE)
        for j in range(i + 1):
            expo = jnp.exp(scores[score_cut(i, j), :] - peak)
            scores[score_cut(i, j), :] = expo
            total += jnp.sum(expo, 0, keepdims=True)
        share_row[:, cut_of(i)] = 1.0 / total

    def mix(i):
        mixed = jnp.zeros((HEAD_DIM, tile), WIDE)
        for j in range(i + 1):
            mixed += dot(value_turned[:, cut_of(j)], scores[score_cut(i, j), :].astype(LOW))
        attn = (mixed * share_row[:, cut_of(i)]).astype(LOW).astype(WIDE)
        attn_turned[:, cut_of(i)] = attn
        returns[0, cut_of(i), :] = attn.T.astype(LOW)

    def attend_back(i):
        grad = heads[3, cut_of(i), :]
        delta = jnp.sum(grad.astype(WIDE).T * attn_turned[:, cut_of(i)], 0, keepdims=True)
        share = share_row[:, cut_of(i)]
        query_sum = jnp.zeros((HEAD_DIM, tile), WIDE)
        for j in range(i + 1):
            d_probs = dot_last(heads[2, cut_of(j), :], grad)
            probs = scores[score_cut(i, j), :] * share
            d_scores = (probs * (d_probs - delta)).astype(LOW)
            value_part = dot(probs.astype(LOW), grad)
            key_part = dot(d_scores, heads[0, cut_of(i), :])
            query_sum += dot(key_turned[:, cut_of(j)], d_scores)
            if i < blocks - 1:
                value_part += value_sum[cut_of(j), :]
                key_part += key_sum[cut_of(j), :]
            if i == j:
                returns[2, cut_of(j), :] = value_part.astype(LOW)
                returns[3, cut_of(j), :] = (key_part * scale).astype(LOW)
            else:
                value_sum[cut_of(j), :] = value_part
                key_sum[cut_of(j), :] = key_part
        returns[1, cut_of(i), :] = (query_sum * scale).T.astype(LOW)

    ends = [0] + list(reversed(range(1, blocks)))
    for i in range(blocks):
        attend(i)
    for k in (4, 5):
        heads_arrived(k)
    for j in range(blocks):
        value_turned[:, cut_of(j)] = heads[2, cut_of(j), :].astype(WIDE).T.astype(LOW)
    for i in ends:
        mix(i)
        send_back(0, i)
    heads_arrived(7)
    heads_arrived(6)
    for i in reversed(range(blocks)):
        attend_back(i)
    for i in range(blocks):
        send_back(1, i)
    turn(w_value)
    sent_back(0)
    for k in (2, 3):
        for i in range(blocks):
            send_back(k, i)
    turn(w_query)

    def returns_arrived(k, sides=(0, 1)):
        a, start, size = piece_of(k)
        for side in sides:
            place = returns.at[a, : size * (half_seq - 1 + side)]
            remote(
                place, place, back_send.at[k], back_recv.at[k, side], {"seq": mine}
            ).wait_recv()

    order = (
        (1 - chip) * 2 + (1 - core),
        (1 - chip) * 2 + core,
        chip * 2 + (1 - core),
        chip * 2 + core,
    )
    stages = ((0, slice(0, rows)), (1, slice(0, half_rows)), (1, slice(half_rows, rows)))

    def pair_copy(stage, k):
        a, part = stages[stage]
        return remote(
            partial.at[a, order[2 * k], part],
            pair_in.at[a, k, part],
            pair_send.at[stage],
            pair_recv.at[stage, k],
            {"tp": partner},
        )

    def cross_copy(stage):
        a, part = stages[stage]
        return remote(
            cross_out.at[a, part],
            cross_in.at[a, part],
            cross_send.at[stage],
            cross_recv.at[stage],
            {"tp": across},
        )

    def cross_over(stage):
        a, part = stages[stage]
        pair_copy(stage, 0).wait_recv()
        cross_out[a, part] = (
            partial[a, order[1], part].astype(WIDE) + pair_in[a, 0, part].astype(WIDE)
        ).astype(LOW)
        cross_copy(stage).start()

    def summed(stage):
        a, part = stages[stage]
        pair_copy(stage, 1).wait_recv()
        cross_copy(stage).wait_recv()
        return (
            partial[a, t, part].astype(WIDE)
            + pair_in[a, 1, part].astype(WIDE)
            + cross_in[a, part].astype(WIDE)
        )

    returns_arrived(0)
    for k in range(tp_size):
        quarter = order[k]

        for j in range(2):
            at = tile_of(quarter * 2 + j, wide_tile)
            here = slice(j * wide_tile, (j + 1) * wide_tile)
            partial[0, quarter, :, here] = dot(back[0], w_out[:, at]).astype(LOW)
        if k % 2 == 0:
            pair_copy(0, k // 2).start()
    def dots_copy(half, offset):
        return remote(
            dots_out.at[half],
            dots_in.at[half, offset],
            dots_send.at[half],
            dots_recv.at[half],
            {"tp": lax.rem(t + offset, tp_size)},
        )

    def share_gradient(half, product):
        stage = 1 + half
        part = stages[stage][1]
        dots = jnp.zeros((half_rows, 1), WIDE)
        for k in range(tp_size):
            quarter = order[k]
            for j in range(2):
                at = tile_of(quarter * 2 + j, wide_tile)
                here = slice(j * wide_tile, (j + 1) * wide_tile)
                whole = product(k, here)
                partial[1, quarter, part, here] = whole.astype(LOW)
                inner = gain[:, at] * whole * wide[quarter, part, here].astype(WIDE)
                dots += jnp.sum(inner, 1, keepdims=True)
            if k % 2 == 0:
                pair_copy(stage, k // 2).start()
            if k == 2:
                cross_over(stage)
        dots_out[half] = jnp.broadcast_to(to_row(dots, rows), dots_out.shape[1:])
        for offset in range(1, tp_size):
            dots_copy(half, offset).start()
        return dots

    def finish_gradient(half, dots):
        stage = 1 + half
        part = stages[stage][1]
        place = dots_in.at[half, 1:]
        remote(place, place, dots_send.at[half], dots_recv.at[half], {"tp": t}).wait_recv()
        for offset in range(1, tp_size):
            dots += to_column(dots_in[half, offset, :1], half_rows)
        rinv = rinv_column[part, :]
        out_grad[part, :] = (
            wide_grad[t, part].astype(WIDE)
            + rinv * gain[:, tile_of(t, columns)] * summed(stage)
            - wide[t, part].astype(WIDE) * (rinv**3 * dots / model_width)
        )

    half_columns = columns // 2
    for side in range(2):
        returns_arrived(1, (side,))
        which = near_half if side == 0 else 1 - near_half

        def query_step(quarter, carry):
            at = tile_of(quarter * 2 + which, half_columns)
            for j in range(2):
                here = slice(j * wide_tile, (j + 1) * wide_tile)
                more = dot(back[1, :, tile_of(which, half_columns)], w_query[at, here])
                if side == 0:
                    grad_sum[quarter, :, here] = more
                else:
                    grad_sum[quarter, :, here] += more
            return carry

        lax.fori_loop(0, tp_size, query_step, 0, unroll=2)
        sent_back(1 + side)
        for i in range(blocks):
            send_back(4 + side, i)
        if side == 0:
            cross_over(0)

    def half_gradient(half):
        part = stages[1 + half][1]

        def value_product(quarter, here):
            return dot(back[2, part], w_value[tile_of(quarter, columns), here])

        def product(k, here):
            quarter = order[k]
            whole = grad_sum[quarter, part, here]
            if k >= 2:
                whole += value_product(quarter, here)
            return whole + dot(back[3, part], w_key[tile_of(quarter, columns), here])

        returns_arrived(2 + 2 * half)
        for k in range(2):
            for j in range(2):
                here = slice(j * wide_tile, (j + 1) * wide_tile)
                grad_sum[order[k], part, here] += value_product(order[k], here)
        returns_arrived(3 + 2 * half)
        return share_gradient(half, product)

    upper_dots = half_gradient(0)
    lower_dots = half_gradient(1)
    out_value[...] = jnp.where(
        row_valid > 0.5, wide[t].astype(WIDE) + summed(0), 0.0
    ).astype(LOW)
    finish_gradient(0, upper_dots)
    finish_gradient(1, lower_dots)

    @pl.when(has_before)
    def _():
        lead_copy.wait_send()

    for kind, sent in ((0, group.at[: 3 * cap]), (1, wide_grad.at[:3]), (2, wide.at[:3])):
        gather_copy(0, 0, kind, sent).wait_send()
    for k in range(8):
        sent = outbox.at[min(k // 2, 3), 1:, :half_rows]
        remote(sent, sent, out_send.at[k], out_recv.at[k], {"seq": mine}).wait_send()
    for k in (3, 4, 5):
        sent_back(k)
    for stage in range(len(stages)):
        a, part = stages[stage]
        sent = pair_in.at[a, :, part]
        remote(
            sent, sent, pair_send.at[stage], pair_recv.at[stage, 0], {"tp": partner}
        ).wait_send()
        cross_copy(stage).wait_send()
    for half in range(2):
        sent = dots_in.at[half, 1:]
        remote(sent, sent, dots_send.at[half], dots_recv.at[half], {"tp": t}).wait_send()


def per_device_whole(encoded, starts, w_up, norm_gain, w_query, w_key, w_value, w_out, cotangent):
    seq_size, tp_size = lax.axis_size("seq"), lax.axis_size("tp")
    rows, columns = cotangent.shape
    model_width = norm_gain.shape[0]
    byte_width = encoded.shape[1]
    cap = starts.shape[1]
    total = starts.size
    tile = 2 * HEAD_DIM
    blocks = total // tile
    dma = pltpu.SemaphoreType.DMA
    scratch = [
        pltpu.VMEM(starts.shape, jnp.int32),
        pltpu.VMEM((1, model_width), WIDE),
        pltpu.VMEM(encoded.shape, LOW),
        pltpu.VMEM(cotangent.shape, LOW),
        pltpu.VMEM(w_up.shape, LOW),
        pltpu.VMEM(w_query.shape, LOW),
        pltpu.VMEM(w_key.shape, LOW),
        pltpu.VMEM(w_value.shape, LOW),
        pltpu.VMEM(w_out.shape, LOW),
        pltpu.VMEM((1, byte_width), WIDE),
        pltpu.VMEM((1, byte_width), WIDE),
        pltpu.VMEM((rows, byte_width), LOW),
        pltpu.VMEM((tp_size, rows, columns), LOW),
        pltpu.VMEM((tp_size, rows, columns), LOW),
        pltpu.VMEM((tp_size, rows, columns), LOW),
        pltpu.VMEM((total, 128), WIDE),
        pltpu.VMEM((rows, 1), WIDE),
        pltpu.VMEM((4, seq_size, rows, HEAD_DIM), LOW),
        pltpu.VMEM((4, total, HEAD_DIM), LOW),
        pltpu.VMEM((HEAD_DIM, total), LOW),
        pltpu.VMEM((HEAD_DIM, total), LOW),
        pltpu.VMEM((blocks * (blocks + 1) // 2 * tile, tile), WIDE),
        pltpu.VMEM((HEAD_DIM, total), WIDE),
        pltpu.VMEM((1, total), WIDE),
        pltpu.VMEM((total, HEAD_DIM), WIDE),
        pltpu.VMEM((total, HEAD_DIM), WIDE),
        pltpu.VMEM((4, total, HEAD_DIM), LOW),
        pltpu.VMEM((4, rows, columns), LOW),
        pltpu.VMEM((tp_size, rows, columns), WIDE),
        pltpu.VMEM((2, tp_size, rows, columns), LOW),
        pltpu.VMEM((2, 2, rows, columns), LOW),
        pltpu.VMEM((2, rows, columns), LOW),
        pltpu.VMEM((2, rows, columns), LOW),
        pltpu.VMEM((2, 8, rows), WIDE),
        pltpu.VMEM((2, tp_size, 8, rows), WIDE),
        dma((5,)),
        dma((4,)),
        dma((2,)),
        dma((3,)),
        dma((3, 7)),
        dma((8,)),
        dma((8,)),
        dma((6,)),
        dma((6, 2)),
        dma((3,)),
        dma((3, 2)),
        dma((3,)),
        dma((3,)),
        dma((2,)),
        dma((2,)),
    ]
    near = pl.BlockSpec(memory_space=pltpu.VMEM)
    far = pl.BlockSpec(memory_space=pl.ANY)
    return tuple(
        pl.pallas_call(
            functools.partial(layer_kernel, seq_size, tp_size),
            out_shape=[
                pltpu.VMEM((rows, columns), LOW),
                pltpu.VMEM((rows, columns), WIDE),
            ],
            in_specs=[far] * 9,
            out_specs=[near] * 2,
            scratch_shapes=scratch,
            compiler_params=pltpu.CompilerParams(
                collective_id=0, has_side_effects=True, vmem_limit_bytes=60 * 1024 * 1024
            ),
        )(
            starts,
            norm_gain.reshape(1, model_width),
            encoded,
            cotangent,
            w_up,
            w_query,
            w_key,
            w_value,
            w_out,
        )
    )


def fits_one_kernel(arrays):
    encoded, starts, w_up, norm_gain, w_query, w_key, w_value, w_out, cotangent = arrays
    seq_size, tp_size = lax.axis_size("seq"), lax.axis_size("tp")
    rows, columns = cotangent.shape
    cap = starts.shape[1]
    return (
        tp_size == 4
        and seq_size % 2 == 0
        and columns == seq_size * HEAD_DIM
        and rows == HEAD_DIM
        and rows == tp_size * cap
        and cap & (cap - 1) == 0
        and cap % 16 == 0
        and columns % (4 * HEAD_DIM) == 0
        and norm_gain.shape[0] == tp_size * columns
        and starts.shape[0] == seq_size * tp_size
        and starts.size % (2 * HEAD_DIM) == 0
    )


def solution(mesh):
    in_specs = (
        P(("seq", "tp"), None),
        P(),
        P(None, "tp"),
        P(),
        P(None, "tp"),
        P(None, "tp"),
        P(None, "tp"),
        P("tp", None),
        P("seq", "tp"),
    )
    out_specs = (P("seq", "tp"), P("seq", "tp"))

    def choose(*arrays):
        return (per_device_whole if fits_one_kernel(arrays) else per_device)(*arrays)

    return jax.shard_map(
        choose, mesh=mesh, in_specs=in_specs, out_specs=out_specs, check_vma=False
    )
```

```python
import functools

import jax
import jax.numpy as jnp
from jax import lax
from jax.experimental import pallas as pl
from jax.experimental.pallas import tpu as pltpu
from jax.sharding import PartitionSpec as P

HEAD_DIM = 128


EPS = 1e-05
NEG = -1e30
CONTRACT_LAST = (((1,), (1,)), ((), ()))


def shifted(block, axis, distance):
    devices = range(lax.axis_size(axis))
    route = [(i - distance, i) for i in devices if i - distance in devices]
    return lax.ppermute(block, axis, route)


def per_device(encoded, starts, w_up, norm_gain, w_query, w_key, w_value, w_out, cotangent):
    byte_rows = encoded.shape[0]
    patch_cap = starts.shape[1]
    model_width = norm_gain.shape[0]
    shard = lax.axis_index(("seq", "tp"))
    own_starts = lax.dynamic_slice_in_dim(starts, shard, 1, 0)[0]
    places = jnp.arange(byte_rows, dtype=jnp.int32)
    following = jnp.concatenate([own_starts[1:], jnp.full((1,), byte_rows, jnp.int32)])
    inside = (places[None, :] >= own_starts[:, None]) & (places[None, :] < following[:, None])
    sums = jnp.dot(inside.astype(jnp.bfloat16), encoded, preferred_element_type=jnp.float32)
    sizes = jnp.sum(inside.astype(jnp.float32), 1)
    leading = places[None, :] < own_starts[:1, None]
    lead_sum = jnp.dot(leading.astype(jnp.bfloat16), encoded, preferred_element_type=jnp.float32)
    lead_size = jnp.sum(leading.astype(jnp.float32), 1)
    next_sum, next_size = shifted((lead_sum, lead_size), ("seq", "tp"), -1)
    count = jnp.sum((own_starts < byte_rows).astype(jnp.int32))
    last_slot = (jnp.arange(patch_cap, dtype=jnp.int32) == count - 1).astype(jnp.float32)
    sums = sums + last_slot[:, None] * next_sum
    sizes = sizes + last_slot * next_size
    patches = (sums / jnp.maximum(sizes, 1.0)[:, None]).astype(jnp.bfloat16)
    group = lax.all_gather(patches, "tp", axis=0, tiled=True)
    latent_in = jnp.dot(group, w_up, preferred_element_type=jnp.float32).astype(jnp.bfloat16)
    group_rows, columns = latent_in.shape
    head_count = columns // HEAD_DIM
    wide_piece = lax.all_gather(latent_in, "tp", axis=1, tiled=True).astype(jnp.float32)
    scaled = (wide_piece * norm_gain[None, :]).astype(jnp.bfloat16)
    acc_query = jnp.dot(scaled, w_query, preferred_element_type=jnp.float32)
    acc_key = jnp.dot(scaled, w_key, preferred_element_type=jnp.float32)
    acc_value = jnp.dot(scaled, w_value, preferred_element_type=jnp.float32)
    acc_query, acc_key, acc_value, square = (
        acc_query,
        acc_key,
        acc_value,
        jnp.sum(wide_piece * wide_piece, 1),
    )
    rinv = lax.rsqrt(square / model_width + EPS)
    query = (rinv[:, None] * acc_query).astype(jnp.bfloat16)
    key_rows = (rinv[:, None] * acc_key).astype(jnp.bfloat16)
    value_rows = (rinv[:, None] * acc_value).astype(jnp.bfloat16)
    keys_all, values_all = (
        lax.all_gather(key_rows, "seq", axis=0, tiled=True),
        lax.all_gather(value_rows, "seq", axis=0, tiled=True),
    )
    patches_total = keys_all.shape[0]
    valid_all = (starts < byte_rows).reshape(patches_total)
    row_base = lax.axis_index("seq") * group_rows
    query_index = row_base + jnp.arange(group_rows, dtype=jnp.int32)
    key_index = jnp.arange(patches_total, dtype=jnp.int32)
    query_valid = lax.dynamic_slice_in_dim(valid_all, row_base, group_rows, 0)
    allowed = valid_all[None, :] & (key_index[None, :] <= query_index[:, None])
    scale = HEAD_DIM ** (-0.5)
    query_heads = query.reshape(group_rows, head_count, HEAD_DIM)
    key_heads = keys_all.reshape(patches_total, head_count, HEAD_DIM)
    value_heads = values_all.reshape(patches_total, head_count, HEAD_DIM)
    scores = (
        jnp.einsum("rhd,khd->hrk", query_heads, key_heads, preferred_element_type=jnp.float32)
        * scale
    )
    peak = jnp.max(jnp.where(allowed[None], scores, NEG), 2)
    expo = jnp.where(allowed[None], jnp.exp(scores - peak[:, :, None]), 0.0)
    total = jnp.sum(expo, 2)
    mixed = jnp.einsum(
        "hrk,khd->rhd", expo.astype(jnp.bfloat16), value_heads, preferred_element_type=jnp.float32
    )
    attn = (mixed / total.T[:, :, None]).astype(jnp.bfloat16)
    partial_value = jnp.dot(
        attn.reshape(group_rows, columns), w_out, preferred_element_type=jnp.float32
    )
    head_sum = lax.psum_scatter(
        partial_value.astype(jnp.bfloat16), "tp", scatter_dimension=1, tiled=True
    ).astype(jnp.float32)
    wide_in = latent_in.astype(jnp.float32)
    latent_out = jnp.where(query_valid[:, None], wide_in + head_sum, 0.0).astype(jnp.bfloat16)
    grad_out = jnp.where(query_valid[:, None], cotangent, jnp.zeros_like(cotangent))
    d_attn = lax.dot_general(
        lax.all_gather(grad_out, "tp", axis=1, tiled=True),
        w_out,
        CONTRACT_LAST,
        preferred_element_type=jnp.float32,
    ).astype(jnp.bfloat16)
    grad_heads = d_attn.reshape(group_rows, head_count, HEAD_DIM)
    delta = jnp.sum(grad_heads.astype(jnp.float32) * attn.astype(jnp.float32), 2).T
    probs = expo / total[:, :, None]
    d_probs = jnp.einsum(
        "rhd,khd->hrk", grad_heads, value_heads, preferred_element_type=jnp.float32
    )
    d_scores = (probs * (d_probs - delta[:, :, None])).astype(jnp.bfloat16)
    grad_query = (
        (
            jnp.einsum("hrk,khd->rhd", d_scores, key_heads, preferred_element_type=jnp.float32)
            * scale
        )
        .astype(jnp.bfloat16)
        .reshape(group_rows, columns)
    )
    weights_low = probs.astype(jnp.bfloat16)
    count_rows = group_rows * lax.axis_size("seq")
    key_part = jnp.einsum("hrk,rhd->khd", d_scores, query_heads, preferred_element_type=jnp.float32)
    value_part = jnp.einsum(
        "hrk,rhd->khd", weights_low, grad_heads, preferred_element_type=jnp.float32
    )
    both = lax.psum_scatter(
        jnp.concatenate(
            [key_part.reshape(count_rows, columns), value_part.reshape(count_rows, columns)], 1
        ).astype(jnp.bfloat16),
        "seq",
        scatter_dimension=0,
        tiled=True,
    ).astype(jnp.float32)
    grad_key = (both[:, :columns] * scale).astype(jnp.bfloat16)
    grad_value = both[:, columns:].astype(jnp.bfloat16)
    dnormed = (
        lax.dot_general(grad_query, w_query, CONTRACT_LAST, preferred_element_type=jnp.float32)
        + lax.dot_general(grad_key, w_key, CONTRACT_LAST, preferred_element_type=jnp.float32)
        + lax.dot_general(grad_value, w_value, CONTRACT_LAST, preferred_element_type=jnp.float32)
    )
    normed_grad = lax.psum_scatter(
        dnormed.astype(jnp.bfloat16), "tp", scatter_dimension=1, tiled=True
    ).astype(jnp.float32)
    gain_own = lax.dynamic_slice_in_dim(norm_gain, lax.axis_index("tp") * columns, columns, 0)
    dots = lax.psum(jnp.sum(gain_own[None, :] * normed_grad * wide_in, 1), "tp")
    latent_grad = (
        grad_out.astype(jnp.float32)
        + rinv[:, None] * gain_own[None, :] * normed_grad
        - wide_in * (rinv**3)[:, None] * dots[:, None] / model_width
    )
    return (latent_out, latent_grad)


MESH = pl.DeviceIdType.MESH
LOW = jnp.bfloat16
WIDE = jnp.float32
ROWS_FIRST = (((0,), (0,)), ((), ()))


def tile_of(index, size):
    return pl.ds(pl.multiple_of(index * size, size), size)


def dot(a, b):
    return jnp.dot(a, b, preferred_element_type=WIDE)


def dot_last(a, b):
    return lax.dot_general(a, b, CONTRACT_LAST, preferred_element_type=WIDE)


def to_row(column, lanes):
    n = column.shape[0]
    down = lax.broadcasted_iota(jnp.int32, (n, lanes), 0)
    across = lax.broadcasted_iota(jnp.int32, (n, lanes), 1)
    return jnp.sum(jnp.where(down == across, column, 0.0), 0, keepdims=True)


def to_column(row, n, shift=0):
    lanes = row.shape[1]
    down = lax.broadcasted_iota(jnp.int32, (n, lanes), 0)
    across = lax.broadcasted_iota(jnp.int32, (n, lanes), 1)
    return jnp.sum(jnp.where(down + shift == across, row, 0.0), 1, keepdims=True)


def layer_kernel(
    seq_size,
    tp_size,
    starts_far,
    gain_far,
    encoded_far,
    cotangent_far,
    w_up_far,
    w_query_far,
    w_key_far,
    w_value_far,
    w_out_far,
    out_value,
    out_grad,
    starts,
    gain,
    encoded,
    cotangent,
    w_up,
    w_query,
    w_key,
    w_value,
    w_out,
    lead_out,
    lead_in,
    group,
    wide,
    wide_grad,
    scaled,
    key_bias,
    rinv_column,
    outbox,
    heads,
    value_turned,
    key_turned,
    scores,
    attn_turned,
    share_row,
    key_sum,
    value_sum,
    returns,
    back,
    grad_sum,
    partial,
    pair_in,
    cross_out,
    cross_in,
    dots_out,
    dots_in,
    weight_sem,
    near_sem,
    lead_sem,
    gather_send,
    gather_recv,
    out_send,
    out_recv,
    back_send,
    back_recv,
    pair_send,
    pair_recv,
    cross_send,
    cross_recv,
    dots_send,
    dots_recv,
):
    byte_rows, byte_width = encoded.shape
    shards, cap = starts.shape
    rows, columns = cotangent.shape
    model_width = gain.shape[1]
    patches_total = shards * cap
    mine = lax.axis_index("seq")
    t = lax.axis_index("tp")
    chip, core = t // 2, lax.rem(t, 2)
    shard = mine * tp_size + t
    partner = t + 1 - 2 * core
    across = lax.rem(t + 2, tp_size)
    diagonal = lax.rem(partner + 2, tp_size)
    tile = 2 * HEAD_DIM
    tiles = columns // tile
    scale = HEAD_DIM ** (-0.5)

    def remote(src, dst, send, recv, device):
        return pltpu.make_async_remote_copy(
            src_ref=src,
            dst_ref=dst,
            send_sem=send,
            recv_sem=recv,
            device_id=device,
            device_id_type=MESH,
        )

    barrier = pltpu.get_barrier_semaphore()
    for offset in range(1, tp_size):
        pl.semaphore_signal(
            barrier, inc=1, device_id={"tp": lax.rem(t + offset, tp_size)}, device_id_type=MESH
        )
    for offset in range(1, seq_size):
        pl.semaphore_signal(
            barrier, inc=1, device_id={"seq": lax.rem(mine + offset, seq_size)}, device_id_type=MESH
        )
    has_before = shard > 0
    has_after = shard < shards - 1
    group_first = jnp.logical_and(t == 0, has_before)
    group_last = jnp.logical_and(t == tp_size - 1, has_after)
    shard_before = {
        "seq": jnp.where(t == 0, lax.rem(mine + seq_size - 1, seq_size), mine),
        "tp": lax.rem(t + tp_size - 1, tp_size),
    }
    shard_after = {
        "seq": jnp.where(t == tp_size - 1, lax.rem(mine + 1, seq_size), mine),
        "tp": lax.rem(t + 1, tp_size),
    }

    @pl.when(group_first)
    def _():
        pl.semaphore_signal(barrier, inc=1, device_id=shard_before, device_id_type=MESH)

    @pl.when(group_last)
    def _():
        pl.semaphore_signal(barrier, inc=1, device_id=shard_after, device_id_type=MESH)

    near_copies = [
        pltpu.make_async_copy(starts_far, starts, near_sem.at[0]),
        pltpu.make_async_copy(encoded_far, encoded, near_sem.at[1]),
        pltpu.make_async_copy(cotangent_far, cotangent, near_sem.at[2]),
        pltpu.make_async_copy(gain_far, gain, near_sem.at[3]),
    ]
    for copy in near_copies:
        copy.start()
    pieces = 4

    def weight_copies(i, far, near):
        depth = far.shape[0] // pieces
        for p in range(pieces):
            part = pl.ds(p * depth, depth)
            pltpu.make_async_copy(far.at[part], near.at[part], weight_sem.at[i]).start()

    def weight_wait(i, far, near):
        pltpu.make_async_copy(far, near, weight_sem.at[i]).wait()

    near_copies[0].wait()
    limit = float(byte_rows)
    own = starts[pl.ds(shard, 1), :].astype(WIDE)
    after = starts[pl.ds(jnp.minimum(shard + 1, shards - 1), 1), :].astype(WIDE)
    first = to_column(own, cap)
    slot = lax.broadcasted_iota(jnp.int32, (cap, 1), 0)
    following = to_column(own, cap, 1) + jnp.where(slot == cap - 1, limit, 0.0)
    places = lax.broadcasted_iota(jnp.int32, (cap, byte_rows), 1).astype(WIDE)
    inside = jnp.where((places >= first) & (places < following), 1.0, 0.0).astype(LOW)
    lead_places = lax.broadcasted_iota(jnp.int32, (16, byte_rows), 1).astype(WIDE)
    leading = jnp.where(lead_places < own[:, :1], 1.0, 0.0).astype(LOW)
    near_copies[1].wait()
    weight_copies(0, w_up_far, w_up)
    weight_copies(4, w_out_far, w_out)
    lead_out[...] = dot(leading, encoded[...])[:1]
    sums = dot(inside, encoded[...])

    own_rows = tile_of(mine, rows)
    own_starts = [
        to_column(starts[pl.ds(mine * tp_size + u, 1), :].astype(WIDE), cap)
        for u in range(tp_size)
    ]
    row_valid = jnp.where(jnp.concatenate(own_starts, 0) < limit, 1.0, 0.0)
    near_copies[2].wait()
    wide_grad[t] = jnp.where(row_valid > 0.5, cotangent[...].astype(WIDE), 0.0).astype(LOW)

    neighbours = group_first.astype(jnp.int32) + group_last.astype(jnp.int32)
    pl.semaphore_wait(barrier, tp_size + seq_size - 2 + neighbours)

    lead_copy = remote(lead_out, lead_in, lead_sem.at[0], lead_sem.at[1], shard_before)

    @pl.when(has_before)
    def _():
        lead_copy.start()

    def gather_copy(way, k, kind, piece):
        target = across if way == 0 else partner
        return remote(
            piece, piece, gather_send.at[kind], gather_recv.at[way, k], {"tp": target}
        )

    def gather_start(k, kind, view):
        gather_copy(0, k, kind, view(t)).start()
        gather_copy(1, k, kind, view(t)).start()

    def gather_relay(k, kind, view):
        gather_copy(0, k, kind, view(across)).wait_recv()
        gather_copy(2, k, kind, view(across)).start()

    def gather_finish(k, kind, view, ways=(1, 2)):
        for way in ways:
            gather_copy(way, k, kind, view(partner if way == 1 else diagonal)).wait_recv()

    half_rows = rows // 2
    grad_views = (
        lambda q: wide_grad.at[q, :half_rows],
        lambda q: wide_grad.at[q, half_rows:],
    )
    gather_start(1, 1, grad_views[0])

    group_view = lambda q: group.at[tile_of(q, cap)]
    wide_tile = columns // 2

    def wide_view(batch, j):
        def view(q):
            of_chip = q // 2
            place = of_chip if batch == 0 else 1 - of_chip
            return wide.at[
                q, tile_of(place, half_rows), j * wide_tile : (j + 1) * wide_tile
            ]

        return view

    def wide_chunk(batch, j):
        return 2 + 2 * batch + j

    @pl.when(has_after)
    def _():
        lead_copy.wait_recv()

    joined = jnp.where(
        jnp.logical_and(first < limit, following >= limit), jnp.where(has_after, 1.0, 0.0), 0.0
    )
    sums = sums + joined * jnp.where(has_after, lead_in[...], 0.0)
    sizes = (following - first) * jnp.where(first < limit, 1.0, 0.0) + joined * after[:, :1]
    group[tile_of(t, cap), :] = (sums / jnp.maximum(sizes, 1.0)).astype(LOW)
    gather_start(0, 0, group_view)
    weight_copies(1, w_key_far, w_key)
    weight_copies(2, w_query_far, w_query)
    weight_copies(3, w_value_far, w_value)

    def raise_rows(batch):
        place = tile_of(chip if batch == 0 else 1 - chip, half_rows)
        for j in range(2):
            cut = slice(j * wide_tile, (j + 1) * wide_tile)
            wide[t, place, cut] = dot(group[place, :], w_up[:, cut]).astype(LOW)
            gather_start(wide_chunk(batch, j), 2, wide_view(batch, j))

    gather_finish(0, 0, group_view, (1,))
    weight_wait(0, w_up_far, w_up)
    raise_rows(0)

    far_half = 1 - mine // (seq_size // 2)

    def head_copy(k, h):
        if k >= 6:
            start = half_rows * (7 - k)
            src = outbox.at[3, h, start : start + half_rows]
            place = tile_of(2 * mine + 7 - k, half_rows)
        else:
            a, batch = k // 2, k % 2
            piece = 1 - chip if batch == 0 else chip
            src = outbox.at[a, h, tile_of(piece, half_rows)]
            place = tile_of(2 * mine + piece, half_rows)
        return remote(
            src,
            heads.at[min(k // 2, 3), place],
            out_send.at[k],
            out_recv.at[k],
            {"seq": h},
        )

    def start_head(k, h):
        @pl.when(h != mine)
        def _():
            head_copy(k, h).start()

    def keep_heads(a, h_first, block, start, size):
        for u in range(block.shape[1] // HEAD_DIM):
            h = h_first + u
            part = block[:, u * HEAD_DIM : (u + 1) * HEAD_DIM]

            @pl.when(h == mine)
            def _():
                heads[a, pl.ds(pl.multiple_of(mine * rows + start, size), size), :] = part

            @pl.when(h != mine)
            def _():
                outbox[a, h, pl.ds(pl.multiple_of(start, size), size), :] = part

    def d_attn_tile(upper, jj):
        j = far_half if jj == 0 else 1 - far_half
        start = 0 if upper else half_rows
        acc = jnp.zeros((half_rows, wide_tile), WIDE)
        for q in range(tp_size):
            acc += dot_last(
                wide_grad[q, start : start + half_rows],
                w_out[tile_of(j, wide_tile), q * columns : (q + 1) * columns],
            )
        held = wide_tile // HEAD_DIM
        keep_heads(3, j * held, acc.astype(LOW), start, half_rows)
        if upper:
            for u in range(held):
                start_head(7, j * held + u)

    def d_attn_rows(upper):
        for jj in range(2):
            d_attn_tile(upper, jj)

    def relay_rows(batch):
        for j in range(2):
            gather_relay(wide_chunk(batch, j), 2, wide_view(batch, j))

    def norm_rows(batch):
        place = tile_of(1 - chip if batch == 0 else chip, half_rows)

        def norm_step(q, square):
            piece = wide[q, place].astype(WIDE)
            scaled[q, place] = (piece * gain[:, tile_of(q, columns)]).astype(LOW)
            return square + jnp.sum(piece * piece, 1, keepdims=True)

        square = lax.fori_loop(0, tp_size, norm_step, jnp.zeros((half_rows, 1), WIDE))
        rinv_column[place, :] = lax.rsqrt(square / model_width + EPS)

    def project(a, weight, batch, width):
        piece = 1 - chip if batch == 0 else chip
        place = tile_of(piece, half_rows)
        steps = columns // width
        held = width // HEAD_DIM

        def step(jj, carry):
            j = lax.rem(far_half * (steps // 2) + jj, steps)
            acc = jnp.zeros((half_rows, width), WIDE)
            for q in range(tp_size):
                acc += dot(
                    scaled[q, place], weight[q * columns : (q + 1) * columns, tile_of(j, width)]
                )
            block = (rinv_column[place, :] * acc).astype(LOW)
            keep_heads(a, j * held, block, piece * half_rows, half_rows)
            for u in range(held):
                start_head(2 * a + batch, j * held + u)
            return carry

        lax.fori_loop(0, steps, step, 0)

    gather_relay(1, 1, grad_views[0])
    gather_relay(0, 0, group_view)
    weight_wait(4, w_out_far, w_out)
    gather_finish(1, 1, grad_views[0])
    d_attn_tile(1, 0)
    gather_finish(0, 0, group_view, (2,))
    raise_rows(1)
    near_copies[3].wait()
    relay_rows(0)
    for j in range(2):
        gather_finish(wide_chunk(0, j), 2, wide_view(0, j), (2,))
        gather_finish(wide_chunk(1, j), 2, wide_view(1, j), (1,))
    norm_rows(0)
    weight_wait(1, w_key_far, w_key)
    project(1, w_key, 0, tile)
    relay_rows(1)
    gather_start(6, 1, grad_views[1])
    weight_wait(2, w_query_far, w_query)
    project(0, w_query, 0, wide_tile)
    weight_wait(3, w_value_far, w_value)
    project(2, w_value, 0, wide_tile)
    for j in range(2):
        gather_finish(wide_chunk(0, j), 2, wide_view(0, j), (1,))
        gather_finish(wide_chunk(1, j), 2, wide_view(1, j), (2,))
    norm_rows(1)
    project(1, w_key, 1, wide_tile)
    project(0, w_query, 1, wide_tile)
    gather_relay(6, 1, grad_views[1])
    project(2, w_value, 1, wide_tile)
    gather_finish(6, 1, grad_views[1])

    d_attn_tile(1, 1)
    d_attn_rows(0)

    def heads_arrived(k):
        place = heads.at[min(k // 2, 3), : half_rows * (seq_size - 1)]
        remote(place, place, out_send.at[k], out_recv.at[k], {"seq": mine}).wait_recv()

    def turn(weight):
        def turn_square(q, carry):
            square = weight.at[tile_of(q, columns)]
            square[...] = square[...].T
            return carry

        lax.fori_loop(0, tp_size, turn_square, 0)

    index = lax.broadcasted_iota(jnp.int32, (patches_total, shards), 0)
    lane = lax.broadcasted_iota(jnp.int32, (patches_total, shards), 1)
    owner = jnp.where((index >= lane * cap) & (index < lane * cap + cap), 1.0, 0.0).astype(LOW)
    valid = jnp.where(starts[...].astype(WIDE) < limit, 1.0, 0.0).astype(LOW)
    spread = dot(owner, valid)
    slots = lax.broadcasted_iota(jnp.int32, (patches_total, cap), 1)
    places_in = lax.broadcasted_iota(jnp.int32, (patches_total, cap), 0)
    valid_column = jnp.sum(
        jnp.where(jnp.bitwise_and(places_in, cap - 1) == slots, spread, 0.0), 1, keepdims=True
    )
    key_bias[...] = jnp.broadcast_to((valid_column - 1.0) * -NEG, key_bias.shape)
    for k in (2, 3, 0):
        heads_arrived(k)
    for step in range(seq_size):
        start_head(6, lax.rem(far_half * (seq_size // 2) + step, seq_size))
    turn(w_key)
    heads_arrived(1)

    blocks = patches_total // tile
    own_columns = tile_of(mine, HEAD_DIM)

    def piece_of(k):
        if k < 2:
            return k, 0, rows
        return 2 + k % 2, half_rows * (k // 2 - 1), half_rows

    half_seq = seq_size // 2
    near_half = mine // half_seq

    def return_copy(k, peer):
        a, start, size = piece_of(k)
        return remote(
            returns.at[a, pl.ds(peer * rows + start, size)],
            back.at[a, start : start + size, own_columns],
            back_send.at[k],
            back_recv.at[k, jnp.where(peer // half_seq == near_half, 0, 1)],
            {"seq": peer},
        )

    def send_back(k, i):
        a, start, size = piece_of(k)
        for peer in range(i * tile // rows, (i + 1) * tile // rows):

            @pl.when(peer != mine)
            def _():
                return_copy(k, peer).start()

            @pl.when(peer == mine)
            def _():
                first = peer * rows + start
                back[a, start : start + size, own_columns] = returns[a, first : first + size, :]

    def sent_back(k):
        a, start, size = piece_of(k)
        sent = returns.at[a, : size * (seq_size - 1)]
        remote(sent, sent, back_send.at[k], back_recv.at[k, 0], {"seq": mine}).wait_send()

    def cut_of(i):
        return slice(i * tile, (i + 1) * tile)

    def score_cut(i, j):
        return cut_of(i * (i + 1) // 2 + j)

    for j in range(blocks):
        key_turned[:, cut_of(j)] = heads[1, cut_of(j), :].astype(WIDE).T.astype(LOW)

    def attend(i):
        peak = jnp.full((1, tile), NEG, WIDE)
        for j in range(i + 1):
            score = dot_last(heads[1, cut_of(j), :], heads[0, cut_of(i), :]) * scale
            bias = key_bias[cut_of(j), :]
            score += jnp.concatenate([bias] * (tile // bias.shape[1]), 1)
            if i == j:
                key = lax.broadcasted_iota(jnp.int32, (tile, tile), 0)
                query = lax.broadcasted_iota(jnp.int32, (tile, tile), 1)
                score = jnp.where(key <= query, score, NEG)
            scores[score_cut(i, j), :] = score
            peak = jnp.maximum(peak, jnp.max(score, 0, keepdims=True))
        total = jnp.zeros((1, tile), WIDE)
        for j in range(i + 1):
            expo = jnp.exp(scores[score_cut(i, j), :] - peak)
            scores[score_cut(i, j), :] = expo
            total += jnp.sum(expo, 0, keepdims=True)
        share_row[:, cut_of(i)] = 1.0 / total

    def mix(i):
        mixed = jnp.zeros((HEAD_DIM, tile), WIDE)
        for j in range(i + 1):
            mixed += dot(value_turned[:, cut_of(j)], scores[score_cut(i, j), :].astype(LOW))
        attn = (mixed * share_row[:, cut_of(i)]).astype(LOW).astype(WIDE)
        attn_turned[:, cut_of(i)] = attn
        returns[0, cut_of(i), :] = attn.T.astype(LOW)

    def attend_back(i):
        grad = heads[3, cut_of(i), :]
        delta = jnp.sum(grad.astype(WIDE).T * attn_turned[:, cut_of(i)], 0, keepdims=True)
        share = share_row[:, cut_of(i)]
        query_sum = jnp.zeros((HEAD_DIM, tile), WIDE)
        for j in range(i + 1):
            d_probs = dot_last(heads[2, cut_of(j), :], grad)
            probs = scores[score_cut(i, j), :] * share
            d_scores = (probs * (d_probs - delta)).astype(LOW)
            value_part = dot(probs.astype(LOW), grad)
            key_part = dot(d_scores, heads[0, cut_of(i), :])
            query_sum += dot(key_turned[:, cut_of(j)], d_scores)
            if i < blocks - 1:
                value_part += value_sum[cut_of(j), :]
                key_part += key_sum[cut_of(j), :]
            if i == j:
                returns[2, cut_of(j), :] = value_part.astype(LOW)
                returns[3, cut_of(j), :] = (key_part * scale).astype(LOW)
            else:
                value_sum[cut_of(j), :] = value_part
                key_sum[cut_of(j), :] = key_part
        returns[1, cut_of(i), :] = (query_sum * scale).T.astype(LOW)

    ends = [0] + list(reversed(range(1, blocks)))
    for i in range(blocks):
        attend(i)
    for k in (4, 5):
        heads_arrived(k)
    for j in range(blocks):
        value_turned[:, cut_of(j)] = heads[2, cut_of(j), :].astype(WIDE).T.astype(LOW)
    for i in ends:
        mix(i)
        send_back(0, i)
    heads_arrived(7)
    heads_arrived(6)
    for i in reversed(range(blocks)):
        attend_back(i)
    for i in range(blocks):
        send_back(1, i)
    turn(w_value)
    sent_back(0)
    for k in (2, 3):
        for i in range(blocks):
            send_back(k, i)
    turn(w_query)

    def returns_arrived(k, sides=(0, 1)):
        a, start, size = piece_of(k)
        for side in sides:
            place = returns.at[a, : size * (half_seq - 1 + side)]
            remote(
                place, place, back_send.at[k], back_recv.at[k, side], {"seq": mine}
            ).wait_recv()

    order = (
        (1 - chip) * 2 + (1 - core),
        (1 - chip) * 2 + core,
        chip * 2 + (1 - core),
        chip * 2 + core,
    )
    stages = ((0, slice(0, rows)), (1, slice(0, half_rows)), (1, slice(half_rows, rows)))

    def pair_copy(stage, k):
        a, part = stages[stage]
        return remote(
            partial.at[a, order[2 * k], part],
            pair_in.at[a, k, part],
            pair_send.at[stage],
            pair_recv.at[stage, k],
            {"tp": partner},
        )

    def cross_copy(stage):
        a, part = stages[stage]
        return remote(
            cross_out.at[a, part],
            cross_in.at[a, part],
            cross_send.at[stage],
            cross_recv.at[stage],
            {"tp": across},
        )

    def cross_over(stage):
        a, part = stages[stage]
        pair_copy(stage, 0).wait_recv()
        cross_out[a, part] = (
            partial[a, order[1], part].astype(WIDE) + pair_in[a, 0, part].astype(WIDE)
        ).astype(LOW)
        cross_copy(stage).start()

    def summed(stage):
        a, part = stages[stage]
        pair_copy(stage, 1).wait_recv()
        cross_copy(stage).wait_recv()
        return (
            partial[a, t, part].astype(WIDE)
            + pair_in[a, 1, part].astype(WIDE)
            + cross_in[a, part].astype(WIDE)
        )

    returns_arrived(0)
    for k in range(tp_size):
        quarter = order[k]

        for j in range(2):
            at = tile_of(quarter * 2 + j, wide_tile)
            here = slice(j * wide_tile, (j + 1) * wide_tile)
            partial[0, quarter, :, here] = dot(back[0], w_out[:, at]).astype(LOW)
        if k % 2 == 0:
            pair_copy(0, k // 2).start()
    def dots_copy(half, offset):
        return remote(
            dots_out.at[half],
            dots_in.at[half, offset],
            dots_send.at[half],
            dots_recv.at[half],
            {"tp": lax.rem(t + offset, tp_size)},
        )

    def share_gradient(half, product):
        stage = 1 + half
        part = stages[stage][1]
        dots = jnp.zeros((half_rows, 1), WIDE)
        for k in range(tp_size):
            quarter = order[k]
            for j in range(2):
                at = tile_of(quarter * 2 + j, wide_tile)
                here = slice(j * wide_tile, (j + 1) * wide_tile)
                whole = product(k, here)
                partial[1, quarter, part, here] = whole.astype(LOW)
                inner = gain[:, at] * whole * wide[quarter, part, here].astype(WIDE)
                dots += jnp.sum(inner, 1, keepdims=True)
            if k % 2 == 0:
                pair_copy(stage, k // 2).start()
            if k == 2:
                cross_over(stage)
        dots_out[half] = jnp.broadcast_to(to_row(dots, rows), dots_out.shape[1:])
        for offset in range(1, tp_size):
            dots_copy(half, offset).start()
        return dots

    def finish_gradient(half, dots):
        stage = 1 + half
        part = stages[stage][1]
        place = dots_in.at[half, 1:]
        remote(place, place, dots_send.at[half], dots_recv.at[half], {"tp": t}).wait_recv()
        for offset in range(1, tp_size):
            dots += to_column(dots_in[half, offset, :1], half_rows)
        rinv = rinv_column[part, :]
        out_grad[part, :] = (
            wide_grad[t, part].astype(WIDE)
            + rinv * gain[:, tile_of(t, columns)] * summed(stage)
            - wide[t, part].astype(WIDE) * (rinv**3 * dots / model_width)
        )

    half_columns = columns // 2
    for side in range(2):
        returns_arrived(1, (side,))
        which = near_half if side == 0 else 1 - near_half

        def query_step(quarter, carry):
            at = tile_of(quarter * 2 + which, half_columns)
            for j in range(2):
                here = slice(j * wide_tile, (j + 1) * wide_tile)
                more = dot(back[1, :, tile_of(which, half_columns)], w_query[at, here])
                if side == 0:
                    grad_sum[quarter, :, here] = more
                else:
                    grad_sum[quarter, :, here] += more
            return carry

        lax.fori_loop(0, tp_size, query_step, 0, unroll=2)
        sent_back(1 + side)
        for i in range(blocks):
            send_back(4 + side, i)
        if side == 0:
            cross_over(0)

    def half_gradient(half):
        part = stages[1 + half][1]

        def value_product(quarter, here):
            return dot(back[2, part], w_value[tile_of(quarter, columns), here])

        def product(k, here):
            quarter = order[k]
            whole = grad_sum[quarter, part, here]
            if k >= 2:
                whole += value_product(quarter, here)
            return whole + dot(back[3, part], w_key[tile_of(quarter, columns), here])

        returns_arrived(2 + 2 * half)
        for k in range(2):
            for j in range(2):
                here = slice(j * wide_tile, (j + 1) * wide_tile)
                grad_sum[order[k], part, here] += value_product(order[k], here)
        returns_arrived(3 + 2 * half)
        return share_gradient(half, product)

    upper_dots = half_gradient(0)
    lower_dots = half_gradient(1)
    out_value[...] = jnp.where(
        row_valid > 0.5, wide[t].astype(WIDE) + summed(0), 0.0
    ).astype(LOW)
    finish_gradient(0, upper_dots)
    finish_gradient(1, lower_dots)

    @pl.when(has_before)
    def _():
        lead_copy.wait_send()

    for kind, sent in ((0, group.at[: 3 * cap]), (1, wide_grad.at[:3]), (2, wide.at[:3])):
        gather_copy(0, 0, kind, sent).wait_send()
    for k in range(8):
        sent = outbox.at[min(k // 2, 3), 1:, :half_rows]
        remote(sent, sent, out_send.at[k], out_recv.at[k], {"seq": mine}).wait_send()
    for k in (3, 4, 5):
        sent_back(k)
    for stage in range(len(stages)):
        a, part = stages[stage]
        sent = pair_in.at[a, :, part]
        remote(
            sent, sent, pair_send.at[stage], pair_recv.at[stage, 0], {"tp": partner}
        ).wait_send()
        cross_copy(stage).wait_send()
    for half in range(2):
        sent = dots_in.at[half, 1:]
        remote(sent, sent, dots_send.at[half], dots_recv.at[half], {"tp": t}).wait_send()


def per_device_whole(encoded, starts, w_up, norm_gain, w_query, w_key, w_value, w_out, cotangent):
    seq_size, tp_size = lax.axis_size("seq"), lax.axis_size("tp")
    rows, columns = cotangent.shape
    model_width = norm_gain.shape[0]
    byte_width = encoded.shape[1]
    cap = starts.shape[1]
    total = starts.size
    tile = 2 * HEAD_DIM
    blocks = total // tile
    dma = pltpu.SemaphoreType.DMA
    scratch = [
        pltpu.VMEM(starts.shape, jnp.int32),
        pltpu.VMEM((1, model_width), WIDE),
        pltpu.VMEM(encoded.shape, LOW),
        pltpu.VMEM(cotangent.shape, LOW),
        pltpu.VMEM(w_up.shape, LOW),
        pltpu.VMEM(w_query.shape, LOW),
        pltpu.VMEM(w_key.shape, LOW),
        pltpu.VMEM(w_value.shape, LOW),
        pltpu.VMEM(w_out.shape, LOW),
        pltpu.VMEM((1, byte_width), WIDE),
        pltpu.VMEM((1, byte_width), WIDE),
        pltpu.VMEM((rows, byte_width), LOW),
        pltpu.VMEM((tp_size, rows, columns), LOW),
        pltpu.VMEM((tp_size, rows, columns), LOW),
        pltpu.VMEM((tp_size, rows, columns), LOW),
        pltpu.VMEM((total, 128), WIDE),
        pltpu.VMEM((rows, 1), WIDE),
        pltpu.VMEM((4, seq_size, rows, HEAD_DIM), LOW),
        pltpu.VMEM((4, total, HEAD_DIM), LOW),
        pltpu.VMEM((HEAD_DIM, total), LOW),
        pltpu.VMEM((HEAD_DIM, total), LOW),
        pltpu.VMEM((blocks * (blocks + 1) // 2 * tile, tile), WIDE),
        pltpu.VMEM((HEAD_DIM, total), WIDE),
        pltpu.VMEM((1, total), WIDE),
        pltpu.VMEM((total, HEAD_DIM), WIDE),
        pltpu.VMEM((total, HEAD_DIM), WIDE),
        pltpu.VMEM((4, total, HEAD_DIM), LOW),
        pltpu.VMEM((4, rows, columns), LOW),
        pltpu.VMEM((tp_size, rows, columns), WIDE),
        pltpu.VMEM((2, tp_size, rows, columns), LOW),
        pltpu.VMEM((2, 2, rows, columns), LOW),
        pltpu.VMEM((2, rows, columns), LOW),
        pltpu.VMEM((2, rows, columns), LOW),
        pltpu.VMEM((2, 8, rows), WIDE),
        pltpu.VMEM((2, tp_size, 8, rows), WIDE),
        dma((5,)),
        dma((4,)),
        dma((2,)),
        dma((3,)),
        dma((3, 7)),
        dma((8,)),
        dma((8,)),
        dma((6,)),
        dma((6, 2)),
        dma((3,)),
        dma((3, 2)),
        dma((3,)),
        dma((3,)),
        dma((2,)),
        dma((2,)),
    ]
    near = pl.BlockSpec(memory_space=pltpu.VMEM)
    far = pl.BlockSpec(memory_space=pl.ANY)
    return tuple(
        pl.pallas_call(
            functools.partial(layer_kernel, seq_size, tp_size),
            out_shape=[
                pltpu.VMEM((rows, columns), LOW),
                pltpu.VMEM((rows, columns), WIDE),
            ],
            in_specs=[far] * 9,
            out_specs=[near] * 2,
            scratch_shapes=scratch,
            compiler_params=pltpu.CompilerParams(
                collective_id=0, has_side_effects=True, vmem_limit_bytes=60 * 1024 * 1024
            ),
        )(
            starts,
            norm_gain.reshape(1, model_width),
            encoded,
            cotangent,
            w_up,
            w_query,
            w_key,
            w_value,
            w_out,
        )
    )


def fits_one_kernel(arrays):
    encoded, starts, w_up, norm_gain, w_query, w_key, w_value, w_out, cotangent = arrays
    seq_size, tp_size = lax.axis_size("seq"), lax.axis_size("tp")
    rows, columns = cotangent.shape
    cap = starts.shape[1]
    return (
        tp_size == 4
        and seq_size % 2 == 0
        and columns == seq_size * HEAD_DIM
        and rows == HEAD_DIM
        and rows == tp_size * cap
        and cap & (cap - 1) == 0
        and cap % 16 == 0
        and columns % (4 * HEAD_DIM) == 0
        and norm_gain.shape[0] == tp_size * columns
        and starts.shape[0] == seq_size * tp_size
        and starts.size % (2 * HEAD_DIM) == 0
    )


def solution(mesh):
    in_specs = (
        P(("seq", "tp"), None),
        P(),
        P(None, "tp"),
        P(),
        P(None, "tp"),
        P(None, "tp"),
        P(None, "tp"),
        P("tp", None),
        P("seq", "tp"),
    )
    out_specs = (P("seq", "tp"), P("seq", "tp"))

    def choose(*arrays):
        return (per_device_whole if fits_one_kernel(arrays) else per_device)(*arrays)

    return jax.shard_map(
        choose, mesh=mesh, in_specs=in_specs, out_specs=out_specs, check_vma=False
    )
```
